128 devices in a mesh: gx: 4 (over x), gy: 4 (over y), gz: 8 (over z, core).
Axes of the slice: x: 4, y: 4, z: 4, core: 2. Of those that a mesh axis runs over, the one named last changes fastest.
Arguments:
- positions: float32 [4096, 3, 256], P(('gx', 'gy', 'gz')), may hold values from 0 to 32, as said below
- smoothing: float32 [4096, 256], P(('gx', 'gy', 'gz')), may hold values from 0.35 to 2
- velocity: float32 [4096, 3, 256], P(('gx', 'gy', 'gz')), may hold values from -0.3 to 0.3
- counts: int32 [4096], P(('gx', 'gy', 'gz')), may hold values from 32 to 256
- plan_before: int32 [4096], P(('gx', 'gy', 'gz')), may hold values from 0 to 4095, as said below
- neighbours: int32 [4096, 8], P(('gx', 'gy', 'gz')), may hold values from 0 to 4095, as said below
- plan_after: int32 [4096], P(('gx', 'gy', 'gz')), may hold values from 0 to 4095, as said below
Outputs:
- new_positions: float32 [4096, 3, 256], P(('gx', 'gy', 'gz'))
- new_velocity: float32 [4096, 3, 256], P(('gx', 'gy', 'gz'))
- density: float32 [4096, 256], P(('gx', 'gy', 'gz'))
The draws below stay inside these ranges and needn't reach their ends.
Inputs may be any that keep to these rules, and one draw needn't show every extreme that they name: `plan_before`: a permutation: each value once. The cells that device d holds (c // 32 = d) go to exactly 16 different devices (place // 32), exactly 2 cells to each. `plan_after`: a permutation of the places after plan_before, with the same property: the cells of one device go to exactly 16 devices, 2 to each. Every entry of row a lies on the device a // 32 or on one of its six face neighbours in the grid of devices (index = (gx * size of gy + gy) * size of gz + gz), which closes into a loop along each axis; entries may repeat and may name a itself. `positions`: coordinates inside the periodic box of the steps.
All inputs are finite; a program needn't handle non-finite values.
Results may differ from the reference program's by a relative error of at most 0.0003.
Values sent between devices are 32-bit elements; how exact they have to be, the bound alone decides.
A program may use at most 64 MiB of HBM per device.

```python
import math
import jax
import jax.numpy as jnp
from jax import lax

P_SIZE = 256
CD = 32
CELLS = 4096
CAP = 2
N_GX = 4
N_GY = 4
N_GZ = 8


def shuffle_slots(row_key):
    return jax.random.permutation(row_key, CD).astype(jnp.int32)


def plan_draw(key):
    devices = N_GX * N_GY * N_GZ
    rounds = CD // CAP
    keys = jax.random.split(key, 5)
    offsets = jax.random.permutation(keys[0], devices).astype(jnp.int32)[:rounds]
    outer = jax.random.permutation(keys[1], devices).astype(jnp.int32)
    inner = jax.random.permutation(keys[2], devices).astype(jnp.int32)
    spread = jax.random.permutation(keys[3], CD).astype(jnp.int32)
    within = jax.vmap(shuffle_slots)(jax.random.split(keys[4], devices))
    target_dev = outer[(inner[:, None] + offsets[None, :]) % devices]
    target_slots = jnp.repeat(target_dev, CAP, axis=1)
    value = target_slots * CD + spread[None, :]
    source = jnp.arange(devices, dtype=jnp.int32)[:, None] * CD + within
    plan = jnp.zeros((devices * CD,), jnp.int32)
    return plan.at[source.reshape(-1)].set(value.reshape(-1).astype(jnp.int32))


def layout_draw(key):
    devices = N_GX * N_GY * N_GZ
    local_of_slot = jax.vmap(shuffle_slots)(jax.random.split(key, devices))
    slot_of_local = jnp.zeros((devices, CD), jnp.int32).at[jnp.arange(devices, dtype=jnp.int32)[:, None], local_of_slot].set(jnp.broadcast_to(jnp.arange(CD, dtype=jnp.int32)[None, :], (devices, CD)))
    return (local_of_slot, slot_of_local)


def place_coords(local_of_slot):
    devices = N_GX * N_GY * N_GZ
    places = jnp.arange(devices * CD, dtype=jnp.int32)
    owner = places // CD
    local = local_of_slot.reshape(-1)
    coord_x = owner // (N_GY * N_GZ) * (CD // 4) + local // 4
    coord_y = owner // N_GZ % N_GY * 2 + local // 2 % 2
    coord_z = owner % N_GZ * 2 + local % 2
    return (coord_x, coord_y, coord_z)


def draw_plan_before(key, part):
    return plan_draw(jax.random.fold_in(key, 11))


def draw_plan_after(key, part):
    return plan_draw(jax.random.fold_in(key, 12))


def draw_neighbours(key, part):
    local_of_slot, slot_of_local = layout_draw(jax.random.fold_in(key, 14))
    coord_x, coord_y, coord_z = place_coords(local_of_slot)
    box_x, box_y, box_z = (CD // 4 * N_GX, 2 * N_GY, 2 * N_GZ)
    columns = []
    for step_x, step_y, step_z in ((-1, 0, 0), (1, 0, 0), (-2, 0, 0), (2, 0, 0), (0, -1, 0), (0, 1, 0), (0, 0, -1), (0, 0, 1)):
        near_x = (coord_x + step_x) % box_x
        near_y = (coord_y + step_y) % box_y
        near_z = (coord_z + step_z) % box_z
        near_dev = (near_x // (CD // 4) * N_GY + near_y // 2) * N_GZ + near_z // 2
        near_local = near_x % (CD // 4) * 4 + near_y % 2 * 2 + near_z % 2
        columns.append(near_dev * CD + slot_of_local[near_dev, near_local])
    return jnp.stack(columns, axis=1).astype(jnp.int32)


def draw_positions(key, part):
    devices = N_GX * N_GY * N_GZ
    plan = plan_draw(jax.random.fold_in(key, 11))
    local_of_slot, slot_of_local = layout_draw(jax.random.fold_in(key, 14))
    coord_x, coord_y, coord_z = place_coords(local_of_slot)
    centre = jnp.stack([coord_x, coord_y, coord_z], axis=1).astype(jnp.float32)[plan]
    inside = jax.random.uniform(jax.random.fold_in(key, 15), (devices * CD, 3, P_SIZE), jnp.float32)
    return (centre[:, :, None] + inside).astype(jnp.float32)


def with_ends(array, rng, low, top_value):
    longest = array.shape.index(max(array.shape))
    spots = []
    for shift in (0, 1):
        where = [jax.random.randint(jax.random.fold_in(rng, axis), (), 0, length) for axis, length in enumerate(array.shape)]
        where[longest] = (where[longest] + shift) % array.shape[longest]
        spots.append(tuple(where))
    return array.at[spots[0]].set(low).at[spots[1]].set(top_value)


def block_levels(stream_key, dims, shards, smallest, top_value):
    level, own = 1.0, jax.random.fold_in(stream_key, 6)
    for position, blocks in shards:
        steps = jnp.exp(jax.random.uniform(jax.random.fold_in(own, position), (blocks,), jnp.float32, smallest / len(shards), top_value / len(shards)))
        level = level * jnp.repeat(steps, dims[position] // blocks).reshape([-1 if axis == position else 1 for axis in range(len(dims))])
    return level


def noise(key, dims, width, bound, shards=(), kind=jnp.bfloat16):
    drawn = jax.random.normal(key, dims, jnp.float32) * width
    if len(shards) > 0:
        drawn = block_levels(key, dims, shards, -0.22, 0.18) * drawn
    return jnp.clip(drawn, min=-bound, max=bound).astype(kind)


def setup_inputs(seed: int = 0) -> dict:
    splits = jax.random.split(jax.random.key(seed), 8)
    positions = draw_positions(jax.random.fold_in(splits[7], 71), 0)
    smoothing = jnp.clip(jnp.exp(math.log(2.0) - 1.7429693 * jax.random.uniform(splits[1], (CELLS, P_SIZE), jnp.float32) ** block_levels(splits[1], (CELLS, P_SIZE), ((0, 128),), -0.2, 0.2)), 0.35, 2.0)
    velocity = noise(splits[2], (CELLS, 3, P_SIZE), 0.05, 0.3, ((0, 128),), jnp.float32)
    counts = with_ends(jax.random.randint(splits[3], (CELLS,), P_SIZE // 8, P_SIZE + 1), jax.random.fold_in(splits[3], 1), P_SIZE // 8, P_SIZE).astype(jnp.int32)
    plan_before = draw_plan_before(jax.random.fold_in(splits[7], 71), 0)
    neighbours = draw_neighbours(jax.random.fold_in(splits[7], 71), 0)
    plan_after = draw_plan_after(jax.random.fold_in(splits[7], 71), 0)
    return dict(positions=positions, smoothing=smoothing, velocity=velocity, counts=counts, plan_before=plan_before, neighbours=neighbours, plan_after=plan_after)


time_step = 0.1


def pair_offsets(own_pos, near_pos, box):
    offsets = []
    for component in range(3):
        length = box[component]
        raw = own_pos[:, component, :, None, None] - near_pos[:, None, :, component, :]
        offsets.append(jnp.mod(raw + 0.5 * length, length) - 0.5 * length)
    return offsets


def live_mask(near_count, particles):
    ladder = jnp.arange(particles).astype(jnp.float32)
    return (ladder[None, None, :] < near_count[:, :, None]).astype(jnp.float32)


def density_group(own_pos, own_h, near_pos, near_count, box):
    particles = own_pos.shape[-1]
    part_mass = 1.0 / (near_pos.shape[1] * particles)
    offsets = pair_offsets(own_pos, near_pos, box)
    dist_sq = offsets[0] * offsets[0] + offsets[1] * offsets[1] + offsets[2] * offsets[2]
    inv_area = 1.0 / (own_h * own_h)
    kernel = jnp.exp(-dist_sq * inv_area[:, :, None, None])
    weights = live_mask(near_count, particles)[:, None, :, :]
    total = jnp.sum(kernel * weights, axis=(2, 3))
    return part_mass * (1.0 + total) / (own_h * own_h * own_h)


def accel_group(own_pos, own_h, own_rho, near_pos, near_count, near_rho, box):
    particles = own_pos.shape[-1]
    part_mass = 1.0 / (near_pos.shape[1] * particles)
    offsets = pair_offsets(own_pos, near_pos, box)
    dist_sq = offsets[0] * offsets[0] + offsets[1] * offsets[1] + offsets[2] * offsets[2]
    inv_area = 1.0 / (own_h * own_h)
    kernel = jnp.exp(-dist_sq * inv_area[:, :, None, None])
    weights = live_mask(near_count, particles)
    pair_weight = kernel * (weights / near_rho)[:, None, :, :] + kernel * weights[:, None, :, :] * (1.0 / own_rho)[:, :, None, None]
    scale_term = 2.0 * part_mass / (own_h * own_h * own_h * own_h * own_h)
    parts = [jnp.sum(pair_weight * offsets[component], axis=(2, 3)) * scale_term for component in range(3)]
    return jnp.stack(parts, axis=1)


def place_rows(values, plan):
    return jnp.zeros_like(values).at[plan].set(values)


def reference(positions, smoothing, velocity, counts, plan_before, neighbours, plan_after):
    cell_total = positions.shape[0]
    particles = positions.shape[-1]
    box = (float(CD // 4 * N_GX), float(2 * N_GY), float(2 * N_GZ))
    placed_pos = place_rows(positions, plan_before)
    placed_h = place_rows(smoothing, plan_before)
    placed_vel = place_rows(velocity, plan_before)
    placed_count = place_rows(counts.astype(jnp.float32), plan_before)
    group_ids = jnp.arange(cell_total, dtype=jnp.int32).reshape(-1, 4)

    def partners(ids):
        return jnp.concatenate([ids[:, None], neighbours[ids]], axis=1)

    def density_step(ids):
        near_ids = partners(ids)
        return density_group(placed_pos[ids], placed_h[ids], placed_pos[near_ids], placed_count[near_ids], box)

    rho = lax.map(density_step, group_ids).reshape(cell_total, particles)

    def accel_step(ids):
        near_ids = partners(ids)
        return accel_group(placed_pos[ids], placed_h[ids], rho[ids], placed_pos[near_ids], placed_count[near_ids], rho[near_ids], box)

    accel = lax.map(accel_step, group_ids).reshape(cell_total, 3, particles)
    kicked = placed_vel + time_step * accel
    drifted = placed_pos + time_step * kicked
    return place_rows(drifted, plan_after), place_rows(kicked, plan_after), place_rows(rho, plan_after)
```

```python
import functools
import math

import jax
import jax.numpy as jnp
from jax import lax
from jax.experimental import pallas as pl
from jax.experimental.pallas import tpu as pltpu
from jax.sharding import PartitionSpec as P

time_step = 0.1
LANES = 128
AXES = ("gx", "gy", "gz")

def split_up(array, dim, peers):
    before, after = (array.shape[:dim], array.shape[dim + 1 :])
    return jnp.moveaxis(array.reshape(*before, peers, -1, *after), dim, 0)


def joined_along(parts, dim):
    shape = list(parts.shape[1:])
    shape[dim] *= parts.shape[0]
    return jnp.moveaxis(parts, 0, dim).reshape(shape)


def one_exchange(array, axis, axes, splits, concats):
    sizes = [lax.axis_size(a) for a in axes]
    parts = split_up(array, splits[0], sizes[0])
    parts = jnp.moveaxis(split_up(parts, splits[1] + 1, sizes[1]), 0, 1)
    inside = parts.shape[2:]
    parts = parts.reshape(-1, *inside)
    parts = lax.all_to_all(parts, axis, split_axis=0, concat_axis=0, tiled=True)
    parts = joined_along(parts.reshape(*sizes, *inside), concats[0] + 1)
    return joined_along(parts, concats[1])


def relocate(fields, plan):
    cell_count = plan.shape[0]
    devices = lax.axis_size("gx") * lax.axis_size("gy") * lax.axis_size("gz")
    capacity = max(2, cell_count // devices)
    target = plan // cell_count
    ladder = jnp.arange(cell_count, dtype=jnp.int32)
    earlier = (target[:, None] == target[None, :]) & (ladder[None, :] < ladder[:, None])
    slot_rank = jnp.sum(earlier.astype(jnp.int32), axis=1)
    send_slot = target * capacity + slot_rank
    buffer_rows = devices * capacity
    arrival = (plan % cell_count).astype(jnp.float32)
    marker = jnp.full((buffer_rows,), -1.0, jnp.float32).at[send_slot].set(arrival)
    packed = tuple(
        (
            jnp.zeros((buffer_rows,) + field.shape[1:], jnp.float32).at[send_slot].set(field)
            for field in fields
        )
    ) + (marker,)
    count_x = lax.axis_size("gx")
    sectioned = tuple(
        (item.reshape((count_x, devices // count_x, capacity) + item.shape[1:]) for item in packed)
    )
    received = jax.tree.map(
        lambda part: one_exchange(part, ("gx", "gy", "gz"), ("gx", ("gy", "gz")), (0, 1), (0, 1)),
        sectioned,
    )
    flat = tuple(
        (item.reshape((buffer_rows,) + source.shape[1:]) for item, source in zip(received, packed))
    )
    landing = flat[-1]
    place_index = jnp.where(landing >= 0.0, landing, float(cell_count)).astype(jnp.int32)
    placed = []
    for item in flat[:-1]:
        holder = jnp.zeros((cell_count,) + item.shape[1:], jnp.float32)
        placed.append(holder.at[place_index].set(item, mode="drop"))
    return tuple(placed)


def neighbour_steps():
    return [(axis, step) for axis in AXES for step in (-1, 1)]


def halo_table(own):
    blocks = [own]
    for axis, step in neighbour_steps():
        peers = lax.axis_size(axis)
        blocks.append(lax.ppermute(own, axis, [((i + step) % peers, i) for i in range(peers)]))
    return jnp.concatenate(blocks, axis=0)


def near_table(neighbours, cell_count):
    sizes = {axis: lax.axis_size(axis) for axis in AXES}
    here = {axis: lax.axis_index(axis) for axis in AXES}
    owner = neighbours // cell_count
    block = jnp.zeros_like(owner)
    for number, (axis, step) in enumerate(neighbour_steps(), 1):
        there = dict(here)
        there[axis] = (here[axis] + step) % sizes[axis]
        device = (there["gx"] * sizes["gy"] + there["gy"]) * sizes["gz"] + there["gz"]
        block = jnp.where(owner == device, number, block)
    near = block * cell_count + neighbours % cell_count
    own = jnp.arange(cell_count, dtype=jnp.int32)[:, None]
    return jnp.concatenate([own, near], axis=1).reshape(-1)


def fixed_point(pos, box):
    parts = []
    for component in range(3):
        scaled = pos[:, component] * (2.0**32 / box[component])
        scaled = jnp.where(scaled >= 2.0**31, scaled - 2.0**32, scaled)
        parts.append(scaled.astype(jnp.int32))
    parts = jnp.stack(parts, axis=1)
    return jnp.pad(parts, ((0, 0), (0, 5), (0, 0)))


def gather_live(cell, near_ref, count_ref, pairs, partners):
    lane = lax.broadcasted_iota(jnp.int32, (8, LANES), 1)
    fill = jnp.int32(0)
    for partner in range(partners):
        b = near_ref[cell * partners + partner]
        live = count_ref[b]
        shift = fill & (LANES - 1)
        chunk = fill >> 7
        kept = lane < shift
        for table_ref, list_ref in pairs:
            first = pltpu.roll(table_ref[b, :, 0:LANES], shift, 1)
            second = pltpu.roll(table_ref[b, :, LANES : 2 * LANES], shift, 1)
            list_ref[chunk] = jnp.where(kept, list_ref[chunk], first)
            list_ref[chunk + 1] = jnp.where(kept, first, second)
            list_ref[chunk + 2] = second
        fill = fill + live
    return fill


def as_column(row):
    halves = []
    for half in range(2):
        part = row[:, half * LANES : (half + 1) * LANES]
        halves.append(jnp.broadcast_to(part, (LANES, LANES)).T)
    return halves


def store_column(ref, row):
    for half, block in enumerate(as_column(row)):
        ref[half * LANES : (half + 1) * LANES, :] = block


def row_sums(acc):
    ones = jnp.ones((8, LANES), jnp.float32)
    sums = lax.dot_general(
        ones, acc, (((1,), (1,)), ((), ())),
        precision=lax.Precision.HIGHEST, preferred_element_type=jnp.float32,
    )
    return sums[0:1, :]


def spread(list_ref, chunk, row):
    return jnp.broadcast_to(list_ref[chunk, row : row + 1, :], (8, LANES))


def offsets(i_refs, rows, others, shifts):
    parts = []
    for ref, other, shift in zip(i_refs, others, shifts):
        diff = ref[rows, :] - other
        if shift:
            diff = diff >> shift
        parts.append(diff.astype(jnp.float32))
    return parts


def density_kernel(partners, mass, unit, shifts, near_ref, count_ref, table_ref, h_ref, rho_ref,
                   list_ref, xi_ref, yi_ref, zi_ref, ci_ref, acc_ref):
    cells, particles = h_ref.shape[0], h_ref.shape[2]
    blocks = particles // 8
    i_refs = (xi_ref, yi_ref, zi_ref)
    lane = lax.broadcasted_iota(jnp.int32, (8, LANES), 1)
    factor = -math.log2(math.e) * unit * unit

    def one_cell(cell, carry):
        total = gather_live(cell, near_ref, count_ref, ((table_ref, list_ref),), partners)
        for component in range(3):
            store_column(i_refs[component], table_ref[cell, component : component + 1, :])
        h = h_ref[cell]
        store_column(ci_ref, factor / (h * h))
        last = (total - 1) >> 7

        def weights(chunk, others, block):
            rows = pl.ds(block * 8, 8)
            dx, dy, dz = offsets(i_refs, rows, others, shifts)
            return rows, jnp.exp2((dx * dx + dy * dy + dz * dz) * ci_ref[rows, :])

        others = [spread(list_ref, last, row) for row in range(3)]
        alive = lane < total - last * LANES
        for block in range(blocks):
            rows, w = weights(last, others, block)
            acc_ref[rows, :] = jnp.where(alive, w, 0.0)

        def one_chunk(chunk, inner):
            near = [spread(list_ref, chunk, row) for row in range(3)]
            for block in range(blocks):
                rows, w = weights(chunk, near, block)
                acc_ref[rows, :] += w
            return inner

        lax.fori_loop(0, last, one_chunk, 0)
        rho_ref[cell] = mass * (1.0 + row_sums(acc_ref[...])) / (h * h * h)
        return carry

    lax.fori_loop(0, cells, one_cell, 0)


def accel_kernel(partners, mass, unit, shifts, near_ref, count_ref, table_ref, inverse_ref, h_ref,
                 pos_ref, vel_ref, drifted_ref, kicked_ref,
                 list_ref, inverse_list_ref, xi_ref, yi_ref, zi_ref, ci_ref, ai_ref,
                 ax_ref, ay_ref, az_ref):
    cells, particles = h_ref.shape[0], h_ref.shape[2]
    blocks = particles // 8
    i_refs = (xi_ref, yi_ref, zi_ref)
    acc_refs = (ax_ref, ay_ref, az_ref)
    lane = lax.broadcasted_iota(jnp.int32, (8, LANES), 1)
    factor = -math.log2(math.e) * unit * unit

    def one_cell(cell, carry):
        total = gather_live(
            cell, near_ref, count_ref,
            ((table_ref, list_ref), (inverse_ref, inverse_list_ref)), partners,
        )
        for component in range(3):
            store_column(i_refs[component], table_ref[cell, component : component + 1, :])
        h = h_ref[cell]
        store_column(ci_ref, factor / (h * h))
        store_column(ai_ref, inverse_ref[cell, 0:1, :])
        last = (total - 1) >> 7

        def terms(others, other_inverse, block):
            rows = pl.ds(block * 8, 8)
            parts = offsets(i_refs, rows, others, shifts)
            dx, dy, dz = parts
            w = jnp.exp2((dx * dx + dy * dy + dz * dz) * ci_ref[rows, :])
            return rows, parts, w * (ai_ref[rows, :] + other_inverse)

        others = [spread(list_ref, last, row) for row in range(3)]
        other_inverse = spread(inverse_list_ref, last, 0)
        alive = lane < total - last * LANES
        for block in range(blocks):
            rows, parts, pair = terms(others, other_inverse, block)
            pair = jnp.where(alive, pair, 0.0)
            for acc_ref, part in zip(acc_refs, parts):
                acc_ref[rows, :] = pair * part

        def one_chunk(chunk, inner):
            near = [spread(list_ref, chunk, row) for row in range(3)]
            near_inverse = spread(inverse_list_ref, chunk, 0)
            for block in range(blocks):
                rows, parts, pair = terms(near, near_inverse, block)
                for acc_ref, part in zip(acc_refs, parts):
                    acc_ref[rows, :] += pair * part
            return inner

        lax.fori_loop(0, last, one_chunk, 0)
        scale = (time_step * 2.0 * mass * unit) / (h * h * h * h * h)
        for component, acc_ref in enumerate(acc_refs):
            row = slice(component, component + 1)
            kicked = vel_ref[cell, row, :] + row_sums(acc_ref[...]) * scale
            kicked_ref[cell, row, :] = kicked
            drifted_ref[cell, row, :] = pos_ref[cell, row, :] + time_step * kicked
        return carry

    lax.fori_loop(0, cells, one_cell, 0)


def shards(positions, smoothing, velocity, counts, plan_before, neighbours, plan_after):
    cell_count = positions.shape[0]
    particles = positions.shape[-1]
    partners = neighbours.shape[1] + 1
    box = (
        float(cell_count // 4 * lax.axis_size("gx")),
        float(2 * lax.axis_size("gy")),
        float(2 * lax.axis_size("gz")),
    )
    longest = max(box)
    shifts = tuple(int(round(math.log2(longest / length))) for length in box)
    unit = longest / 2.0**32
    mass = 1.0 / (partners * particles)
    placed_pos, placed_h, placed_vel, placed_count = relocate(
        (positions, smoothing, velocity, counts.astype(jnp.float32)), plan_before
    )
    near = near_table(neighbours, cell_count)
    table = fixed_point(halo_table(placed_pos), box)
    table_count = halo_table(placed_count).astype(jnp.int32)
    own_h = placed_h.reshape(cell_count, 1, particles)

    smem = pl.BlockSpec(memory_space=pltpu.SMEM)
    vmem = pl.BlockSpec(memory_space=pltpu.VMEM)
    chunks = partners * particles // LANES + 1
    square = (particles, LANES)
    columns = [pltpu.VMEM(square, jnp.int32)] * 3
    rho = pl.pallas_call(
        functools.partial(density_kernel, partners, mass, unit, shifts),
        out_shape=jax.ShapeDtypeStruct((cell_count, 1, particles), jnp.float32),
        in_specs=[smem, smem, vmem, vmem],
        out_specs=vmem,
        scratch_shapes=[pltpu.VMEM((chunks, 8, LANES), jnp.int32)] + columns
        + [pltpu.VMEM(square, jnp.float32)] * 2,
    )(near, table_count, table, own_h)

    inverse = 1.0 / halo_table(rho)
    inverse = jnp.broadcast_to(inverse, (inverse.shape[0], 8, particles))
    drifted, kicked = pl.pallas_call(
        functools.partial(accel_kernel, partners, mass, unit, shifts),
        out_shape=[jax.ShapeDtypeStruct(placed_pos.shape, jnp.float32)] * 2,
        in_specs=[smem, smem, vmem, vmem, vmem, vmem, vmem],
        out_specs=[vmem, vmem],
        scratch_shapes=[
            pltpu.VMEM((chunks, 8, LANES), jnp.int32),
            pltpu.VMEM((chunks, 8, LANES), jnp.float32),
        ]
        + columns
        + [pltpu.VMEM(square, jnp.float32)] * 5,
    )(near, table_count, table, inverse, own_h, placed_pos, placed_vel)
    final_pos, final_vel, final_rho = relocate(
        (drifted, kicked, rho.reshape(cell_count, particles)), plan_after
    )
    return (final_pos, final_vel, final_rho)


def solution(mesh):
    in_specs = (
        P(("gx", "gy", "gz"), None, None),
        P(("gx", "gy", "gz"), None),
        P(("gx", "gy", "gz"), None, None),
        P(("gx", "gy", "gz")),
        P(("gx", "gy", "gz")),
        P(("gx", "gy", "gz"), None),
        P(("gx", "gy", "gz")),
    )
    out_specs = (
        P(("gx", "gy", "gz"), None, None),
        P(("gx", "gy", "gz"), None, None),
        P(("gx", "gy", "gz"), None),
    )
    return jax.shard_map(shards, mesh=mesh, in_specs=in_specs, out_specs=out_specs, check_vma=False)
```

```python
import functools
import math

import jax
import jax.numpy as jnp
from jax import lax
from jax.experimental import pallas as pl
from jax.experimental.pallas import tpu as pltpu
from jax.sharding import PartitionSpec as P

time_step = 0.1
LANES = 128
AXES = ("gx", "gy", "gz")
MESH = pl.DeviceIdType.MESH

def neighbour_steps():
    return [(axis, step) for axis in AXES for step in (-1, 1)]


def slots_of(plan, cell_count, devices):
    target = plan // cell_count
    ladder = jnp.arange(cell_count, dtype=jnp.int32)
    earlier = (target[:, None] == target[None, :]) & (ladder[None, :] < ladder[:, None])
    rank = jnp.sum(earlier.astype(jnp.int32), axis=1)
    slot = target * 2 + rank
    every = jnp.arange(devices * 2, dtype=jnp.int32)
    cell = jnp.sum(jnp.where(slot[None, :] == every[:, None], ladder[None, :], 0), axis=1)
    return plan * 2 + rank, cell


def near_table(neighbours, cell_count):
    sizes = {axis: lax.axis_size(axis) for axis in AXES}
    here = {axis: lax.axis_index(axis) for axis in AXES}
    owner = neighbours // cell_count
    block = jnp.zeros_like(owner)
    for number, (axis, step) in enumerate(neighbour_steps(), 1):
        there = dict(here)
        there[axis] = (here[axis] + step) % sizes[axis]
        device = (there["gx"] * sizes["gy"] + there["gy"]) * sizes["gz"] + there["gz"]
        block = jnp.where(owner == device, number, block)
    near = block * cell_count + neighbours % cell_count
    own = jnp.arange(cell_count, dtype=jnp.int32)[:, None]
    return jnp.concatenate([own, near], axis=1).reshape(-1)


def exchange(sizes, pairs, send_sems, recv_sems):
    count_x, count_y, count_z = sizes
    devices = count_x * count_y * count_z
    here = [lax.axis_index(axis) for axis in AXES]
    me = (here[0] * count_y + here[1]) * count_z + here[2]

    def send(step, carry):
        there_x = lax.rem(here[0] + lax.div(step, count_y * count_z), count_x)
        there_y = lax.rem(here[1] + lax.rem(lax.div(step, count_z), count_y), count_y)
        there_z = lax.rem(here[2] + lax.rem(step, count_z), count_z)
        there = (there_x * count_y + there_y) * count_z + there_z
        for number, (source, target, whole) in enumerate(pairs):
            pltpu.make_async_remote_copy(
                src_ref=source if whole else source.at[there],
                dst_ref=target.at[me],
                send_sem=send_sems.at[number],
                recv_sem=recv_sems.at[number],
                device_id=(there_x, there_y, there_z),
                device_id_type=MESH,
            ).start()
        return carry

    lax.fori_loop(1, devices, send, 0)
    for source, target, whole in pairs:
        target[me] = source[...] if whole else source[me]
    for number, (source, target, whole) in enumerate(pairs):
        most = target.at[pl.ds(0, devices - 1)]
        arrived = pltpu.make_async_remote_copy(
            src_ref=most, dst_ref=most, send_sem=send_sems.at[number],
            recv_sem=recv_sems.at[number], device_id=tuple(here), device_id_type=MESH,
        )
        arrived.wait_send()
        arrived.wait_recv()


def fill_blocks(cell_ref, q_ref, v_ref, sendq_ref, sendv_ref):
    def one(d, carry):
        first, second = cell_ref[2 * d], cell_ref[2 * d + 1]
        sendq_ref[d, 0] = q_ref[first]
        sendq_ref[d, 1] = q_ref[second]
        low, high = v_ref[first], v_ref[second]
        sendv_ref[d, 0] = low[0:4]
        sendv_ref[d, 1, 0:2] = low[4:6]
        sendv_ref[d, 1, 2:4] = high[0:2]
        sendv_ref[d, 2] = high[2:6]
        return carry

    lax.fori_loop(0, sendq_ref.shape[0], one, 0)


def velocity_rows(recvv_ref, slot):
    block, odd = slot >> 1, (slot & 1) == 1
    first, middle, last = recvv_ref[block, 0], recvv_ref[block, 1], recvv_ref[block, 2]
    even_rows = jnp.concatenate([first, middle[0:2]], axis=0)
    odd_rows = jnp.concatenate([middle[2:4], last], axis=0)
    rows = jnp.where(odd, odd_rows, even_rows)
    return rows[0:3], rows[3:6]


def first_exchange_kernel(sizes, cell_ref, meta_ref, pos_ref, h_ref, vel_ref,
                          recvq_ref, recvv_ref, metas_ref,
                          q_ref, v_ref, sendq_ref, sendv_ref, send_sems, recv_sems):
    for cell in range(pos_ref.shape[0]):
        for half in range(2):
            lanes = slice(half * LANES, (half + 1) * LANES)
            q_ref[cell, 4 * half : 4 * half + 3] = pos_ref[cell, :, lanes]
            q_ref[cell, 4 * half + 3 : 4 * half + 4] = h_ref[cell : cell + 1, lanes]
            v_ref[cell, 3 * half : 3 * half + 3] = vel_ref[cell, :, lanes]
    fill_blocks(cell_ref, q_ref, v_ref, sendq_ref, sendv_ref)
    exchange(
        sizes,
        ((meta_ref, metas_ref, True), (sendq_ref, recvq_ref, False), (sendv_ref, recvv_ref, False)),
        send_sems, recv_sems,
    )


def last_exchange_kernel(sizes, cell_ref, q_ref, v_ref, recvq_ref, recvv_ref,
                         sendq_ref, sendv_ref, send_sems, recv_sems):
    fill_blocks(cell_ref, q_ref, v_ref, sendq_ref, sendv_ref)
    exchange(
        sizes, ((sendq_ref, recvq_ref, False), (sendv_ref, recvv_ref, False)), send_sems, recv_sems
    )


def halo(sizes, own, table_ref, send_sems, recv_sems):
    here = [lax.axis_index(axis) for axis in AXES]
    copies = []
    for number, (axis, step) in enumerate(neighbour_steps()):
        there = list(here)
        dim = AXES.index(axis)
        there[dim] = lax.rem(here[dim] + sizes[dim] - step, sizes[dim])
        copies.append(
            pltpu.make_async_remote_copy(
                src_ref=own, dst_ref=table_ref.at[number + 1], send_sem=send_sems.at[number],
                recv_sem=recv_sems.at[number], device_id=tuple(there), device_id_type=MESH,
            )
        )
        copies[-1].start()
    return copies


def cell_halo_kernel(sizes, slot_ref, recvq_ref, table_ref, send_sems, recv_sems):
    for place in range(table_ref.shape[1]):
        table_ref[0, place] = recvq_ref[slot_ref[place]]
    for copy in halo(sizes, table_ref.at[0], table_ref, send_sems, recv_sems):
        copy.wait()


def rho_halo_kernel(sizes, rho_ref, table_ref, send_sems, recv_sems):
    copies = halo(sizes, rho_ref, table_ref, send_sems, recv_sems)
    table_ref[0] = rho_ref[...]
    for copy in copies:
        copy.wait()


def unpack_kernel(slot_ref, recvq_ref, recvv_ref, pos_ref, vel_ref, rho_ref):
    for place in range(pos_ref.shape[0]):
        slot = slot_ref[place]
        rows = recvq_ref[slot]
        velocity = velocity_rows(recvv_ref, slot)
        for half in range(2):
            lanes = slice(half * LANES, (half + 1) * LANES)
            pos_ref[place, :, lanes] = rows[4 * half : 4 * half + 3]
            rho_ref[place : place + 1, lanes] = rows[4 * half + 3 : 4 * half + 4]
            vel_ref[place, :, lanes] = velocity[half]


def fixed_point(table_ref, fixed_ref, box):
    row = lax.broadcasted_iota(jnp.int32, (8, LANES), 0) & 3
    scale = jnp.full((8, LANES), 2.0**32 / box[2], jnp.float32)
    scale = jnp.where(row == 0, 2.0**32 / box[0], jnp.where(row == 1, 2.0**32 / box[1], scale))
    scale = jnp.where(row == 3, 1.0, scale)
    cells = table_ref.shape[1]

    def one(cell, carry):
        for block in range(table_ref.shape[0]):
            scaled = table_ref[block, cell] * scale
            scaled = jnp.where(scaled >= 2.0**31, scaled - 2.0**32, scaled)
            fixed_ref[block * cells + cell] = scaled.astype(jnp.int32)
        return carry

    lax.fori_loop(0, cells, one, 0)


def gather_live(cell, near_ref, count_ref, pairs, partners):
    fill = jnp.int32(0)
    for partner in range(partners):
        b = near_ref[cell * partners + partner]
        live = count_ref[b]
        shift = fill & (LANES - 1)
        chunk = fill >> 7
        for table_ref, list_ref in pairs:
            rows = list_ref.shape[1]
            kept = lax.broadcasted_iota(jnp.int32, (rows, LANES), 1) < shift
            rolled = pltpu.roll(table_ref[b], shift, 1)
            first, second = rolled[0:rows], rolled[rows : 2 * rows]
            list_ref[chunk] = jnp.where(kept, list_ref[chunk], first)
            list_ref[chunk + 1] = jnp.where(kept, first, second)
            list_ref[chunk + 2] = second
        fill = fill + live
    return fill


def store_column(ref, halves):
    for half, part in enumerate(halves):
        ref[half * LANES : (half + 1) * LANES, :] = jnp.broadcast_to(part, (LANES, LANES)).T


def halves_of(ref, cell, row):
    step = ref.shape[1] // 2
    return [ref[cell, row + half * step : row + half * step + 1, :] for half in range(2)]


def row_sums(acc):
    ones = jnp.ones((8, LANES), jnp.float32)
    sums = lax.dot_general(
        ones, acc, (((1,), (1,)), ((), ())),
        precision=lax.Precision.HIGHEST, preferred_element_type=jnp.float32,
    )
    return [sums[0:1, 0:LANES], sums[0:1, LANES : 2 * LANES]]


def spread(list_ref, chunk, row):
    return jnp.broadcast_to(list_ref[chunk, row : row + 1, :], (8, LANES))


def offsets(i_refs, rows, others, shifts):
    parts = []
    for ref, other, shift in zip(i_refs, others, shifts):
        diff = ref[rows, :] - other
        if shift:
            diff = diff >> shift
        parts.append(diff.astype(jnp.float32))
    return parts


def density_kernel(partners, mass, unit, shifts, box, near_ref, count_ref, table_ref, rho_ref,
                   fixed_ref, list_ref, xi_ref, yi_ref, zi_ref, ci_ref, acc_ref):
    cells, particles = table_ref.shape[1], 2 * LANES
    blocks = particles // 8
    i_refs = (xi_ref, yi_ref, zi_ref)
    lane = lax.broadcasted_iota(jnp.int32, (8, LANES), 1)
    factor = -math.log2(math.e) * unit * unit
    fixed_point(table_ref, fixed_ref, box)

    def one_cell(cell, carry):
        total = gather_live(cell, near_ref, count_ref, ((fixed_ref, list_ref),), partners)
        for component in range(3):
            store_column(i_refs[component], halves_of(fixed_ref, cell, component))
        h = halves_of(table_ref.at[0], cell, 3)
        store_column(ci_ref, [factor / (part * part) for part in h])
        last = (total - 1) >> 7

        def weights(chunk, others, block):
            rows = pl.ds(block * 8, 8)
            dx, dy, dz = offsets(i_refs, rows, others, shifts)
            return rows, jnp.exp2((dx * dx + dy * dy + dz * dz) * ci_ref[rows, :])

        others = [spread(list_ref, last, row) for row in range(3)]
        alive = lane < total - last * LANES
        for block in range(blocks):
            rows, w = weights(last, others, block)
            acc_ref[rows, :] = jnp.where(alive, w, 0.0)

        def one_chunk(chunk, inner):
            near = [spread(list_ref, chunk, row) for row in range(3)]
            for block in range(blocks):
                rows, w = weights(chunk, near, block)
                acc_ref[rows, :] += w
            return inner

        lax.fori_loop(0, last, one_chunk, 0)
        for half, (part, total_half) in enumerate(zip(h, row_sums(acc_ref[...]))):
            rho_ref[cell, half : half + 1] = mass * (1.0 + total_half) / (part * part * part)
        return carry

    lax.fori_loop(0, cells, one_cell, 0)


def accel_kernel(partners, mass, unit, shifts, box, near_ref, count_ref, slot_ref, table_ref, rho_ref,
                 recvv_ref, q_ref, v_ref,
                 fixed_ref, inverse_ref, list_ref, inverse_list_ref, xi_ref, yi_ref, zi_ref, ci_ref, ai_ref,
                 ax_ref, ay_ref, az_ref):
    cells, particles = table_ref.shape[1], 2 * LANES
    blocks = particles // 8
    i_refs = (xi_ref, yi_ref, zi_ref)
    acc_refs = (ax_ref, ay_ref, az_ref)
    lane = lax.broadcasted_iota(jnp.int32, (8, LANES), 1)
    factor = -math.log2(math.e) * unit * unit
    fixed_point(table_ref, fixed_ref, box)

    def invert(cell, carry):
        for block in range(rho_ref.shape[0]):
            inverse_ref[block * cells + cell] = 1.0 / rho_ref[block, cell]
        return carry

    lax.fori_loop(0, cells, invert, 0)

    def one_cell(cell, carry):
        total = gather_live(
            cell, near_ref, count_ref,
            ((fixed_ref, list_ref), (inverse_ref, inverse_list_ref)), partners,
        )
        for component in range(3):
            store_column(i_refs[component], halves_of(fixed_ref, cell, component))
        h = halves_of(table_ref.at[0], cell, 3)
        store_column(ci_ref, [factor / (part * part) for part in h])
        store_column(ai_ref, halves_of(inverse_ref, cell, 0))
        last = (total - 1) >> 7

        def terms(others, other_inverse, block):
            rows = pl.ds(block * 8, 8)
            parts = offsets(i_refs, rows, others, shifts)
            dx, dy, dz = parts
            w = jnp.exp2((dx * dx + dy * dy + dz * dz) * ci_ref[rows, :])
            return rows, parts, w * (ai_ref[rows, :] + other_inverse)

        others = [spread(list_ref, last, row) for row in range(3)]
        other_inverse = spread(inverse_list_ref, last, 0)
        alive = lane < total - last * LANES
        for block in range(blocks):
            rows, parts, pair = terms(others, other_inverse, block)
            pair = jnp.where(alive, pair, 0.0)
            for acc_ref, part in zip(acc_refs, parts):
                acc_ref[rows, :] = pair * part

        def one_chunk(chunk, inner):
            near = [spread(list_ref, chunk, row) for row in range(3)]
            near_inverse = spread(inverse_list_ref, chunk, 0)
            for block in range(blocks):
                rows, parts, pair = terms(near, near_inverse, block)
                for acc_ref, part in zip(acc_refs, parts):
                    acc_ref[rows, :] += pair * part
            return inner

        lax.fori_loop(0, last, one_chunk, 0)
        scale = [(time_step * 2.0 * mass * unit) / (part * part * part * part * part) for part in h]
        velocity = velocity_rows(recvv_ref, slot_ref[cell])
        for component, acc_ref in enumerate(acc_refs):
            sums = row_sums(acc_ref[...])
            for half in range(2):
                kicked = velocity[half][component : component + 1] + sums[half] * scale[half]
                v_ref[cell, 3 * half + component : 3 * half + component + 1] = kicked
                row = slice(4 * half + component, 4 * half + component + 1)
                q_ref[cell, row] = table_ref[0, cell, row] + time_step * kicked
        for half in range(2):
            row = slice(4 * half + 3, 4 * half + 4)
            q_ref[cell, row] = rho_ref[0, cell, half : half + 1]
        return carry

    lax.fori_loop(0, cells, one_cell, 0)


def shards(positions, smoothing, velocity, counts, plan_before, neighbours, plan_after):
    cell_count = positions.shape[0]
    particles = positions.shape[-1]
    partners = neighbours.shape[1] + 1
    sizes = tuple(lax.axis_size(axis) for axis in AXES)
    devices = sizes[0] * sizes[1] * sizes[2]
    box = (float(cell_count // 4 * sizes[0]), float(2 * sizes[1]), float(2 * sizes[2]))
    longest = max(box)
    shifts = tuple(int(round(math.log2(longest / length))) for length in box)
    unit = longest / 2.0**32
    mass = 1.0 / (partners * particles)

    smem = pl.BlockSpec(memory_space=pltpu.SMEM)
    vmem = pl.BlockSpec(memory_space=pltpu.VMEM)
    f32 = lambda *shape: jax.ShapeDtypeStruct(shape, jnp.float32)
    effects = pltpu.CompilerParams(has_side_effects=True)
    sems = lambda count: [pltpu.SemaphoreType.DMA((count,))] * 2
    blocks_q, blocks_v = (devices, 2, 8, LANES), (devices, 3, 4, LANES)
    sends = [pltpu.VMEM(blocks_q, jnp.float32), pltpu.VMEM(blocks_v, jnp.float32)]
    cells8 = pltpu.VMEM((cell_count, 8, LANES), jnp.float32)

    key_before, cell_before = slots_of(plan_before, cell_count, devices)
    key_after, cell_after = slots_of(plan_after, cell_count, devices)
    meta = jnp.concatenate([key_before, key_after, counts, jnp.zeros_like(counts)])[None, :]
    recv_q, recv_v, metas = pl.pallas_call(
        functools.partial(first_exchange_kernel, sizes),
        out_shape=[f32(*blocks_q), f32(*blocks_v), jax.ShapeDtypeStruct((devices, 1, LANES), jnp.int32)],
        in_specs=[smem, vmem, vmem, vmem, vmem],
        out_specs=[vmem] * 3,
        scratch_shapes=[cells8, cells8] + sends + sems(3),
        compiler_params=effects,
        name="first_exchange",
    )(cell_before, meta, positions, smoothing, velocity)

    here = [lax.axis_index(axis) for axis in AXES]
    blocks = [tuple(here)]
    for axis, step in neighbour_steps():
        there = list(here)
        dim = AXES.index(axis)
        there[dim] = (here[dim] + step) % sizes[dim]
        blocks.append(tuple(there))
    first_place = jnp.stack([((x * sizes[1] + y) * sizes[2] + z) * cell_count for x, y, z in blocks])
    local = jnp.arange(cell_count, dtype=jnp.int32)
    place = (first_place[:, None] + local[None, :]).reshape(-1)
    keys, keys_after = metas[:, 0, 0:cell_count], metas[:, 0, cell_count : 2 * cell_count]
    all_counts = metas[:, 0, 2 * cell_count : 3 * cell_count]
    source = 2 * jnp.arange(devices, dtype=jnp.int32)[None, :, None]

    def pick(keys, places, values):
        hit = (keys >> 1)[None] == places[:, None, None]
        return jnp.sum(jnp.where(hit, values, 0), axis=(1, 2))

    own_place = place[:cell_count]
    table_count = pick(keys, place, all_counts[None])
    slot_before = pick(keys, own_place, (keys & 1)[None] + source)
    slot_after = pick(keys_after, own_place, (keys_after & 1)[None] + source)
    near = near_table(neighbours, cell_count)

    table = pl.pallas_call(
        functools.partial(cell_halo_kernel, sizes),
        out_shape=f32(7, cell_count, 8, LANES),
        in_specs=[smem, vmem],
        out_specs=vmem,
        scratch_shapes=sems(6),
        compiler_params=effects,
        name="cell_halo",
    )(slot_before, recv_q.reshape(2 * devices, 8, LANES))

    chunks = partners * particles // LANES + 1
    square = (particles, LANES)
    columns = [pltpu.VMEM(square, jnp.int32)] * 3
    fixed = pltpu.VMEM((7 * cell_count, 8, LANES), jnp.int32)
    rho = pl.pallas_call(
        functools.partial(density_kernel, partners, mass, unit, shifts, box),
        out_shape=f32(cell_count, 2, LANES),
        in_specs=[smem, smem, vmem],
        out_specs=vmem,
        scratch_shapes=[fixed, pltpu.VMEM((chunks, 4, LANES), jnp.int32)] + columns
        + [pltpu.VMEM(square, jnp.float32)] * 2,
        name="density",
    )(near, table_count, table)

    table_rho = pl.pallas_call(
        functools.partial(rho_halo_kernel, sizes),
        out_shape=f32(7, cell_count, 2, LANES),
        in_specs=[vmem],
        out_specs=vmem,
        scratch_shapes=sems(6),
        compiler_params=effects,
        name="rho_halo",
    )(rho)

    out_q, out_v = pl.pallas_call(
        functools.partial(accel_kernel, partners, mass, unit, shifts, box),
        out_shape=[f32(cell_count, 8, LANES)] * 2,
        in_specs=[smem, smem, smem, vmem, vmem, vmem],
        out_specs=[vmem, vmem],
        scratch_shapes=[
            fixed,
            pltpu.VMEM((7 * cell_count, 2, LANES), jnp.float32),
            pltpu.VMEM((chunks, 4, LANES), jnp.int32),
            pltpu.VMEM((chunks, 1, LANES), jnp.float32),
        ]
        + columns
        + [pltpu.VMEM(square, jnp.float32)] * 5,
        name="accel",
    )(near, table_count, slot_before, table, table_rho, recv_v)

    last_q, last_v = pl.pallas_call(
        functools.partial(last_exchange_kernel, sizes),
        out_shape=[f32(*blocks_q), f32(*blocks_v)],
        in_specs=[smem, vmem, vmem],
        out_specs=[vmem] * 2,
        scratch_shapes=sends + sems(2),
        compiler_params=effects,
        name="last_exchange",
    )(cell_after, out_q, out_v)
    return pl.pallas_call(
        unpack_kernel,
        out_shape=[f32(*positions.shape), f32(*velocity.shape), f32(*smoothing.shape)],
        in_specs=[smem, vmem, vmem],
        out_specs=[vmem] * 3,
        name="unpack",
    )(slot_after, last_q.reshape(2 * devices, 8, LANES), last_v)


def solution(mesh):
    in_specs = (
        P(("gx", "gy", "gz"), None, None),
        P(("gx", "gy", "gz"), None),
        P(("gx", "gy", "gz"), None, None),
        P(("gx", "gy", "gz")),
        P(("gx", "gy", "gz")),
        P(("gx", "gy", "gz"), None),
        P(("gx", "gy", "gz")),
    )
    out_specs = (
        P(("gx", "gy", "gz"), None, None),
        P(("gx", "gy", "gz"), None, None),
        P(("gx", "gy", "gz"), None),
    )
    return jax.shard_map(shards, mesh=mesh, in_specs=in_specs, out_specs=out_specs, check_vma=False)
```

```python
import functools
import math

import jax
import jax.numpy as jnp
from jax import lax
from jax.experimental import pallas as pl
from jax.experimental.pallas import tpu as pltpu
from jax.sharding import PartitionSpec as P

time_step = 0.1
LANES = 128
AXES = ("gx", "gy", "gz")
MESH = pl.DeviceIdType.MESH

def neighbour_steps():
    return [(axis, step) for axis in AXES for step in (-1, 1)]


def slots_of(plans, cell_count, devices):
    target = plans // cell_count
    ladder = jnp.arange(cell_count, dtype=jnp.int32)
    earlier = (target[:, :, None] == target[:, None, :]) & (ladder[None, :] < ladder[:, None])
    rank = jnp.sum(earlier.astype(jnp.int32), axis=2)
    slot = target * 2 + rank
    every = jnp.arange(devices * 2, dtype=jnp.int32)
    hit = slot[:, None, :] == every[None, :, None]
    return plans * 2 + rank, jnp.sum(jnp.where(hit, ladder, 0), axis=2)


def near_table(neighbours, cell_count):
    sizes = {axis: lax.axis_size(axis) for axis in AXES}
    here = {axis: lax.axis_index(axis) for axis in AXES}
    owner = neighbours // cell_count
    block = jnp.zeros_like(owner)
    for number, (axis, step) in enumerate(neighbour_steps(), 1):
        there = dict(here)
        there[axis] = (here[axis] + step) % sizes[axis]
        device = (there["gx"] * sizes["gy"] + there["gy"]) * sizes["gz"] + there["gz"]
        block = jnp.where(owner == device, number, block)
    near = block * cell_count + neighbours % cell_count
    own = jnp.arange(cell_count, dtype=jnp.int32)[:, None]
    return jnp.concatenate([own, near], axis=1).reshape(-1)


def peer_offsets(sizes):
    count_x, count_y, count_z = sizes
    steps = [(x, y, z) for x in range(count_x) for y in range(count_y) for z in range(count_z)][1:]

    def hops(step):
        x, y, z = step
        chips = count_z // 2
        return min(x, count_x - x) + min(y, count_y - y) + min(z // 2, chips - z // 2)

    return sorted(steps, key=lambda step: -hops(step))


def shifted(here, step, sizes):
    return tuple(lax.rem(h + d, n) if d else h for h, d, n in zip(here, step, sizes))


def flat(place, sizes):
    return (place[0] * sizes[1] + place[1]) * sizes[2] + place[2]


def greet(peers):
    barrier = pltpu.get_barrier_semaphore()
    for peer in peers:
        pl.semaphore_signal(barrier, inc=1, device_id=peer, device_id_type=MESH)
    return barrier, len(peers)


def exchange(sizes, fill, pairs, send_sems, recv_sems):
    here = [lax.axis_index(axis) for axis in AXES]
    me = flat(here, sizes)
    peers = [shifted(here, step, sizes) for step in peer_offsets(sizes)]
    barrier, signals = greet(peers)
    fill()
    pl.semaphore_wait(barrier, signals)
    for number, (source, target, whole) in enumerate(pairs):
        for there in peers:
            pltpu.make_async_remote_copy(
                src_ref=source if whole else source.at[flat(there, sizes)],
                dst_ref=target.at[me],
                send_sem=send_sems.at[number],
                recv_sem=recv_sems.at[number],
                device_id=there,
                device_id_type=MESH,
            ).start()
    for source, target, whole in pairs:
        target[me] = source[...] if whole else source[me]
    for number, (source, target, whole) in enumerate(pairs):
        most = target.at[pl.ds(0, signals)]
        arrived = pltpu.make_async_remote_copy(
            src_ref=most, dst_ref=most, send_sem=send_sems.at[number],
            recv_sem=recv_sems.at[number], device_id=tuple(here), device_id_type=MESH,
        )
        arrived.wait_send()
        arrived.wait_recv()


def fill_blocks(cell_ref, q_ref, v_ref, send_ref):
    def one(d, carry):
        first, second = cell_ref[2 * d], cell_ref[2 * d + 1]
        for number, cell in enumerate((first, second)):
            rows = q_ref[cell]
            send_ref[d, 2 * number] = rows[0:4]
            send_ref[d, 2 * number + 1] = rows[4:8]
        low, high = v_ref[first], v_ref[second]
        send_ref[d, 4] = low[0:4]
        send_ref[d, 5, 0:2] = low[4:6]
        send_ref[d, 5, 2:4] = high[0:2]
        send_ref[d, 6] = high[2:6]
        return carry

    lax.fori_loop(0, send_ref.shape[0], one, 0)


def cell_rows(recv_ref, slot):
    block, odd = slot >> 1, slot & 1
    return [recv_ref[block, 2 * odd + half] for half in range(2)]


def velocity_rows(recv_ref, slot):
    block, odd = slot >> 1, (slot & 1) == 1
    first, middle, last = recv_ref[block, 4], recv_ref[block, 5], recv_ref[block, 6]
    even_rows = jnp.concatenate([first, middle[0:2]], axis=0)
    odd_rows = jnp.concatenate([middle[2:4], last], axis=0)
    rows = jnp.where(odd, odd_rows, even_rows)
    return rows[0:3], rows[3:6]


def first_exchange_kernel(sizes, cell_ref, meta_ref, pos_ref, h_ref, vel_ref, recv_ref, metas_ref,
                          q_ref, v_ref, send_ref, send_sems, recv_sems):
    def fill():
        for cell in range(pos_ref.shape[1]):
            for half in range(2):
                lanes = slice(half * LANES, (half + 1) * LANES)
                for component in range(3):
                    q_ref[cell, 4 * half + component] = pos_ref[component, cell, lanes]
                    v_ref[cell, 3 * half + component] = vel_ref[component, cell, lanes]
                q_ref[cell, 4 * half + 3] = h_ref[cell, lanes]
        fill_blocks(cell_ref, q_ref, v_ref, send_ref)

    pairs = ((meta_ref, metas_ref, True), (send_ref, recv_ref, False))
    exchange(sizes, fill, pairs, send_sems, recv_sems)


def last_exchange_kernel(sizes, cell_ref, q_ref, v_ref, recv_ref, send_ref, send_sems, recv_sems):
    def fill():
        fill_blocks(cell_ref, q_ref, v_ref, send_ref)

    exchange(sizes, fill, ((send_ref, recv_ref, False),), send_sems, recv_sems)


def halo(sizes, fill, pairs, send_sems, recv_sems):
    here = [lax.axis_index(axis) for axis in AXES]
    peers = []
    for axis, step in neighbour_steps():
        there = [0] * 3
        there[AXES.index(axis)] = (-step) % sizes[AXES.index(axis)]
        peers.append(shifted(here, there, sizes))
    barrier, signals = greet(peers)
    fill()
    pl.semaphore_wait(barrier, signals)
    copies = []
    for which, (source, target) in enumerate(pairs):
        for number, there in enumerate(peers):
            copies.append(
                pltpu.make_async_remote_copy(
                    src_ref=source, dst_ref=target.at[number + 1],
                    send_sem=send_sems.at[which, number], recv_sem=recv_sems.at[which, number],
                    device_id=there, device_id_type=MESH,
                )
            )
            copies[-1].start()
    for copy in copies:
        copy.wait()


def cell_halo_kernel(sizes, slot_ref, count_ref, recv_ref, table_ref, counts_ref, send_sems, recv_sems):
    def fill():
        counts_ref[0] = count_ref[...]
        for place in range(table_ref.shape[1]):
            low, high = cell_rows(recv_ref, slot_ref[place])
            table_ref[0, place, 0:4] = low
            table_ref[0, place, 4:8] = high

    pairs = ((count_ref, counts_ref), (table_ref.at[0], table_ref))
    halo(sizes, fill, pairs, send_sems, recv_sems)


def rho_halo_kernel(sizes, rho_ref, table_ref, send_sems, recv_sems):
    def fill():
        table_ref[0] = rho_ref[...]

    halo(sizes, fill, ((rho_ref, table_ref),), send_sems, recv_sems)


def unpack_kernel(slot_ref, recv_ref, pos_ref, vel_ref, rho_ref):
    for place in range(pos_ref.shape[1]):
        slot = slot_ref[place]
        rows = cell_rows(recv_ref, slot)
        velocity = velocity_rows(recv_ref, slot)
        for half in range(2):
            lanes = slice(half * LANES, (half + 1) * LANES)
            for component in range(3):
                pos_ref[component, place, lanes] = rows[half][component]
                vel_ref[component, place, lanes] = velocity[half][component]
            rho_ref[place, lanes] = rows[half][3]


def fixed_point(table_ref, fixed_ref, box):
    row = lax.broadcasted_iota(jnp.int32, (8, LANES), 0) & 3
    scale = jnp.full((8, LANES), 2.0**32 / box[2], jnp.float32)
    scale = jnp.where(row == 0, 2.0**32 / box[0], jnp.where(row == 1, 2.0**32 / box[1], scale))
    scale = jnp.where(row == 3, 1.0, scale)
    cells = table_ref.shape[1]

    def one(cell, carry):
        for block in range(table_ref.shape[0]):
            scaled = table_ref[block, cell] * scale
            scaled = jnp.where(scaled >= 2.0**31, scaled - 2.0**32, scaled)
            fixed_ref[block * cells + cell] = scaled.astype(jnp.int32)
        return carry

    lax.fori_loop(0, cells, one, 0)


def gather_live(cell, near_ref, count_ref, pairs, partners):
    fill = jnp.int32(0)
    for partner in range(partners):
        b = near_ref[cell * partners + partner]
        live = count_ref[b]
        shift = fill & (LANES - 1)
        chunk = fill >> 7
        for table_ref, list_ref in pairs:
            rows = list_ref.shape[1]
            kept = lax.broadcasted_iota(jnp.int32, (rows, LANES), 1) < shift
            rolled = pltpu.roll(table_ref[b], shift, 1)
            first, second = rolled[0:rows], rolled[rows : 2 * rows]
            list_ref[chunk] = jnp.where(kept, list_ref[chunk], first)
            list_ref[chunk + 1] = jnp.where(kept, first, second)
            list_ref[chunk + 2] = second
        fill = fill + live
    return fill


def store_column(ref, halves):
    for half, part in enumerate(halves):
        ref[half * LANES : (half + 1) * LANES, :] = jnp.broadcast_to(part, (LANES, LANES)).T


def halves_of(ref, cell, row):
    step = ref.shape[1] // 2
    return [ref[cell, row + half * step : row + half * step + 1, :] for half in range(2)]


def row_sums(acc):
    ones = jnp.ones((8, LANES), jnp.float32)
    sums = lax.dot_general(
        ones, acc, (((1,), (1,)), ((), ())),
        precision=lax.Precision.HIGHEST, preferred_element_type=jnp.float32,
    )
    return [sums[0:1, 0:LANES], sums[0:1, LANES : 2 * LANES]]


def spread(list_ref, chunk, row):
    return jnp.broadcast_to(list_ref[chunk, row : row + 1, :], (8, LANES))


def offsets(i_refs, rows, others, shifts):
    parts = []
    for ref, other, shift in zip(i_refs, others, shifts):
        diff = ref[rows, :] - other
        if shift:
            diff = diff >> shift
        parts.append(diff.astype(jnp.float32))
    return parts


def density_kernel(partners, mass, unit, shifts, box, near_ref, count_ref, table_ref, rho_ref,
                   fixed_ref, list_ref, xi_ref, yi_ref, zi_ref, ci_ref, acc_ref):
    cells, particles = table_ref.shape[1], 2 * LANES
    blocks = particles // 8
    i_refs = (xi_ref, yi_ref, zi_ref)
    lane = lax.broadcasted_iota(jnp.int32, (8, LANES), 1)
    factor = -math.log2(math.e) * unit * unit
    fixed_point(table_ref, fixed_ref, box)

    def one_cell(cell, carry):
        total = gather_live(cell, near_ref, count_ref, ((fixed_ref, list_ref),), partners)
        for component in range(3):
            store_column(i_refs[component], halves_of(fixed_ref, cell, component))
        h = halves_of(table_ref.at[0], cell, 3)
        store_column(ci_ref, [factor / (part * part) for part in h])
        last = (total - 1) >> 7

        def weights(chunk, others, block):
            rows = pl.ds(block * 8, 8)
            dx, dy, dz = offsets(i_refs, rows, others, shifts)
            return rows, jnp.exp2((dx * dx + dy * dy + dz * dz) * ci_ref[rows, :])

        others = [spread(list_ref, last, row) for row in range(3)]
        alive = lane < total - last * LANES
        for block in range(blocks):
            rows, w = weights(last, others, block)
            acc_ref[rows, :] = jnp.where(alive, w, 0.0)

        def one_chunk(chunk, inner):
            near = [spread(list_ref, chunk, row) for row in range(3)]
            for block in range(blocks):
                rows, w = weights(chunk, near, block)
                acc_ref[rows, :] += w
            return inner

        lax.fori_loop(0, last, one_chunk, 0)
        for half, (part, total_half) in enumerate(zip(h, row_sums(acc_ref[...]))):
            rho_ref[cell, half : half + 1] = mass * (1.0 + total_half) / (part * part * part)
        return carry

    lax.fori_loop(0, cells, one_cell, 0)


def accel_kernel(partners, mass, unit, shifts, box, near_ref, count_ref, slot_ref, table_ref, rho_ref,
                 recv_ref, q_ref, v_ref,
                 fixed_ref, inverse_ref, list_ref, inverse_list_ref, xi_ref, yi_ref, zi_ref, ci_ref, ai_ref,
                 ax_ref, ay_ref, az_ref):
    cells, particles = table_ref.shape[1], 2 * LANES
    blocks = particles // 8
    i_refs = (xi_ref, yi_ref, zi_ref)
    acc_refs = (ax_ref, ay_ref, az_ref)
    lane = lax.broadcasted_iota(jnp.int32, (8, LANES), 1)
    factor = -math.log2(math.e) * unit * unit
    fixed_point(table_ref, fixed_ref, box)

    def invert(cell, carry):
        for block in range(rho_ref.shape[0]):
            inverse_ref[block * cells + cell] = 1.0 / rho_ref[block, cell]
        return carry

    lax.fori_loop(0, cells, invert, 0)

    def one_cell(cell, carry):
        total = gather_live(
            cell, near_ref, count_ref,
            ((fixed_ref, list_ref), (inverse_ref, inverse_list_ref)), partners,
        )
        for component in range(3):
            store_column(i_refs[component], halves_of(fixed_ref, cell, component))
        h = halves_of(table_ref.at[0], cell, 3)
        store_column(ci_ref, [factor / (part * part) for part in h])
        store_column(ai_ref, halves_of(inverse_ref, cell, 0))
        last = (total - 1) >> 7

        def terms(others, other_inverse, block):
            rows = pl.ds(block * 8, 8)
            parts = offsets(i_refs, rows, others, shifts)
            dx, dy, dz = parts
            w = jnp.exp2((dx * dx + dy * dy + dz * dz) * ci_ref[rows, :])
            return rows, parts, w * (ai_ref[rows, :] + other_inverse)

        others = [spread(list_ref, last, row) for row in range(3)]
        other_inverse = spread(inverse_list_ref, last, 0)
        alive = lane < total - last * LANES
        for block in range(blocks):
            rows, parts, pair = terms(others, other_inverse, block)
            pair = jnp.where(alive, pair, 0.0)
            for acc_ref, part in zip(acc_refs, parts):
                acc_ref[rows, :] = pair * part

        def one_chunk(chunk, inner):
            near = [spread(list_ref, chunk, row) for row in range(3)]
            near_inverse = spread(inverse_list_ref, chunk, 0)
            for block in range(blocks):
                rows, parts, pair = terms(near, near_inverse, block)
                for acc_ref, part in zip(acc_refs, parts):
                    acc_ref[rows, :] += pair * part
            return inner

        lax.fori_loop(0, last, one_chunk, 0)
        scale = [(time_step * 2.0 * mass * unit) / (part * part * part * part * part) for part in h]
        velocity = velocity_rows(recv_ref, slot_ref[cell])
        for component, acc_ref in enumerate(acc_refs):
            sums = row_sums(acc_ref[...])
            for half in range(2):
                kicked = velocity[half][component : component + 1] + sums[half] * scale[half]
                v_ref[cell, 3 * half + component : 3 * half + component + 1] = kicked
                row = slice(4 * half + component, 4 * half + component + 1)
                q_ref[cell, row] = table_ref[0, cell, row] + time_step * kicked
        for half in range(2):
            row = slice(4 * half + 3, 4 * half + 4)
            q_ref[cell, row] = rho_ref[0, cell, half : half + 1]
        return carry

    lax.fori_loop(0, cells, one_cell, 0)


def shards(positions, smoothing, velocity, counts, plan_before, neighbours, plan_after):
    cell_count = positions.shape[0]
    particles = positions.shape[-1]
    partners = neighbours.shape[1] + 1
    sizes = tuple(lax.axis_size(axis) for axis in AXES)
    devices = sizes[0] * sizes[1] * sizes[2]
    box = (float(cell_count // 4 * sizes[0]), float(2 * sizes[1]), float(2 * sizes[2]))
    longest = max(box)
    shifts = tuple(int(round(math.log2(longest / length))) for length in box)
    unit = longest / 2.0**32
    mass = 1.0 / (partners * particles)

    smem = pl.BlockSpec(memory_space=pltpu.SMEM)
    vmem = pl.BlockSpec(memory_space=pltpu.VMEM)
    f32 = lambda *shape: jax.ShapeDtypeStruct(shape, jnp.float32)
    effects = lambda number: pltpu.CompilerParams(has_side_effects=True, collective_id=number)
    sems = lambda *count: [pltpu.SemaphoreType.DMA(count)] * 2
    blocks = (devices, 7, 4, LANES)
    cells8 = pltpu.VMEM((cell_count, 8, LANES), jnp.float32)

    keys, cells = slots_of(jnp.stack([plan_before, plan_after]), cell_count, devices)
    meta = jnp.concatenate([keys.reshape(-1), counts, jnp.zeros_like(counts)])[None, :]
    recv, metas = pl.pallas_call(
        functools.partial(first_exchange_kernel, sizes),
        out_shape=[f32(*blocks), jax.ShapeDtypeStruct((devices, 1, LANES), jnp.int32)],
        in_specs=[smem, vmem, vmem, vmem, vmem],
        out_specs=[vmem] * 2,
        scratch_shapes=[cells8, cells8, pltpu.VMEM(blocks, jnp.float32)] + sems(2),
        compiler_params=effects(0),
        name="first_exchange",
    )(cells[0], meta, jnp.transpose(positions, (1, 0, 2)), smoothing, jnp.transpose(velocity, (1, 0, 2)))

    here = [lax.axis_index(axis) for axis in AXES]
    place = flat(here, sizes) * cell_count + jnp.arange(cell_count, dtype=jnp.int32)
    metas = metas[:, 0, :]
    keys_before, keys_after = metas[:, 0:cell_count], metas[:, cell_count : 2 * cell_count]
    all_counts = metas[:, 2 * cell_count : 3 * cell_count]
    source = 2 * jnp.arange(devices, dtype=jnp.int32)[:, None]

    def pick(keys, values):
        hit = (keys >> 1)[None] == place[:, None, None]
        return jnp.sum(jnp.where(hit, values[None], 0), axis=(1, 2))

    slot_count = pick(keys_before, (keys_before & 1) + source + all_counts * (2 * devices))
    slot_before, own_count = slot_count % (2 * devices), slot_count // (2 * devices)
    slot_after = pick(keys_after, (keys_after & 1) + source)
    near = near_table(neighbours, cell_count)

    table, table_count = pl.pallas_call(
        functools.partial(cell_halo_kernel, sizes),
        out_shape=[f32(7, cell_count, 8, LANES), jax.ShapeDtypeStruct((7, 1, LANES), jnp.int32)],
        in_specs=[smem, vmem, vmem],
        out_specs=[vmem, vmem],
        scratch_shapes=sems(2, 6),
        compiler_params=effects(1),
        name="cell_halo",
    )(slot_before, jnp.pad(own_count, (0, LANES - cell_count))[None, :], recv)
    table_count = table_count[:, 0, :cell_count].reshape(-1)

    chunks = partners * particles // LANES + 1
    square = (particles, LANES)
    columns = [pltpu.VMEM(square, jnp.int32)] * 3
    fixed = pltpu.VMEM((7 * cell_count, 8, LANES), jnp.int32)
    rho = pl.pallas_call(
        functools.partial(density_kernel, partners, mass, unit, shifts, box),
        out_shape=f32(cell_count, 2, LANES),
        in_specs=[smem, smem, vmem],
        out_specs=vmem,
        scratch_shapes=[fixed, pltpu.VMEM((chunks, 4, LANES), jnp.int32)] + columns
        + [pltpu.VMEM(square, jnp.float32)] * 2,
        name="density",
    )(near, table_count, table)

    table_rho = pl.pallas_call(
        functools.partial(rho_halo_kernel, sizes),
        out_shape=f32(7, cell_count, 2, LANES),
        in_specs=[vmem],
        out_specs=vmem,
        scratch_shapes=sems(1, 6),
        compiler_params=effects(2),
        name="rho_halo",
    )(rho)

    out_q, out_v = pl.pallas_call(
        functools.partial(accel_kernel, partners, mass, unit, shifts, box),
        out_shape=[f32(cell_count, 8, LANES)] * 2,
        in_specs=[smem, smem, smem, vmem, vmem, vmem],
        out_specs=[vmem, vmem],
        scratch_shapes=[
            fixed,
            pltpu.VMEM((7 * cell_count, 2, LANES), jnp.float32),
            pltpu.VMEM((chunks, 4, LANES), jnp.int32),
            pltpu.VMEM((chunks, 1, LANES), jnp.float32),
        ]
        + columns
        + [pltpu.VMEM(square, jnp.float32)] * 5,
        name="accel",
    )(near, table_count, slot_before, table, table_rho, recv)

    last = pl.pallas_call(
        functools.partial(last_exchange_kernel, sizes),
        out_shape=f32(*blocks),
        in_specs=[smem, vmem, vmem],
        out_specs=vmem,
        scratch_shapes=[pltpu.VMEM(blocks, jnp.float32)] + sems(1),
        compiler_params=effects(3),
        name="last_exchange",
    )(cells[1], out_q, out_v)
    new_pos, new_vel, new_rho = pl.pallas_call(
        unpack_kernel,
        out_shape=[f32(3, cell_count, particles)] * 2 + [f32(cell_count, particles)],
        in_specs=[smem, vmem],
        out_specs=[vmem] * 3,
        name="unpack",
    )(slot_after, last)
    return jnp.transpose(new_pos, (1, 0, 2)), jnp.transpose(new_vel, (1, 0, 2)), new_rho


def solution(mesh):
    in_specs = (
        P(("gx", "gy", "gz"), None, None),
        P(("gx", "gy", "gz"), None),
        P(("gx", "gy", "gz"), None, None),
        P(("gx", "gy", "gz")),
        P(("gx", "gy", "gz")),
        P(("gx", "gy", "gz"), None),
        P(("gx", "gy", "gz")),
    )
    out_specs = (
        P(("gx", "gy", "gz"), None, None),
        P(("gx", "gy", "gz"), None, None),
        P(("gx", "gy", "gz"), None),
    )
    return jax.shard_map(shards, mesh=mesh, in_specs=in_specs, out_specs=out_specs, check_vma=False)
```

```python
import functools
import math

import jax
import jax.numpy as jnp
from jax import lax
from jax.experimental import pallas as pl
from jax.experimental.pallas import tpu as pltpu
from jax.sharding import PartitionSpec as P

time_step = 0.1
LANES = 128
AXES = ("gx", "gy", "gz")
MESH = pl.DeviceIdType.MESH

def neighbour_steps():
    return [(axis, step) for axis in AXES for step in (-1, 1)]


def slots_of(plans, cell_count, devices):
    target = plans // cell_count
    ladder = jnp.arange(cell_count, dtype=jnp.int32)
    earlier = (target[:, :, None] == target[:, None, :]) & (ladder[None, :] < ladder[:, None])
    rank = jnp.sum(earlier.astype(jnp.int32), axis=2)
    slot = target * 2 + rank
    every = jnp.arange(devices * 2, dtype=jnp.int32)
    hit = slot[:, None, :] == every[None, :, None]
    return plans * 2 + rank, jnp.sum(jnp.where(hit, ladder, 0), axis=2)


def near_table(neighbours, cell_count):
    sizes = {axis: lax.axis_size(axis) for axis in AXES}
    here = {axis: lax.axis_index(axis) for axis in AXES}
    owner = neighbours // cell_count
    block = jnp.zeros_like(owner)
    for number, (axis, step) in enumerate(neighbour_steps(), 1):
        there = dict(here)
        there[axis] = (here[axis] + step) % sizes[axis]
        device = (there["gx"] * sizes["gy"] + there["gy"]) * sizes["gz"] + there["gz"]
        block = jnp.where(owner == device, number, block)
    near = block * cell_count + neighbours % cell_count
    own = jnp.arange(cell_count, dtype=jnp.int32)[:, None]
    return jnp.concatenate([own, near], axis=1).reshape(-1)


def peer_offsets(sizes):
    count_x, count_y, count_z = sizes
    steps = [(x, y, z) for x in range(count_x) for y in range(count_y) for z in range(count_z)][1:]

    def hops(step):
        x, y, z = step
        chips = count_z // 2
        return min(x, count_x - x) + min(y, count_y - y) + min(z // 2, chips - z // 2)

    return sorted(steps, key=lambda step: -hops(step))


def shifted(here, step, sizes):
    return tuple(lax.rem(h + d, n) if d else h for h, d, n in zip(here, step, sizes))


def flat(place, sizes):
    return (place[0] * sizes[1] + place[1]) * sizes[2] + place[2]


def greet(peers):
    barrier = pltpu.get_barrier_semaphore()
    for peer in peers:
        pl.semaphore_signal(barrier, inc=1, device_id=peer, device_id_type=MESH)
    return barrier, len(peers)


def exchange(sizes, fill, pairs, send_sems, recv_sems):
    here = [lax.axis_index(axis) for axis in AXES]
    me = flat(here, sizes)
    peers = [shifted(here, step, sizes) for step in peer_offsets(sizes)]
    barrier, signals = greet(peers)
    fill()
    pl.semaphore_wait(barrier, signals)
    for number, (source, target, whole) in enumerate(pairs):
        for there in peers:
            pltpu.make_async_remote_copy(
                src_ref=source if whole else source.at[flat(there, sizes)],
                dst_ref=target.at[me],
                send_sem=send_sems.at[number],
                recv_sem=recv_sems.at[number],
                device_id=there,
                device_id_type=MESH,
            ).start()
    for source, target, whole in pairs:
        target[me] = source[...] if whole else source[me]
    for number, (source, target, whole) in enumerate(pairs):
        most = target.at[pl.ds(0, signals)]
        arrived = pltpu.make_async_remote_copy(
            src_ref=most, dst_ref=most, send_sem=send_sems.at[number],
            recv_sem=recv_sems.at[number], device_id=tuple(here), device_id_type=MESH,
        )
        arrived.wait_send()
        arrived.wait_recv()


def fill_blocks(cell_ref, q_ref, v_ref, send_ref):
    def one(d, carry):
        first, second = cell_ref[2 * d], cell_ref[2 * d + 1]
        for number, cell in enumerate((first, second)):
            rows = q_ref[cell]
            send_ref[d, 2 * number] = rows[0:4]
            send_ref[d, 2 * number + 1] = rows[4:8]
        low, high = v_ref[first], v_ref[second]
        send_ref[d, 4] = low[0:4]
        send_ref[d, 5, 0:2] = low[4:6]
        send_ref[d, 5, 2:4] = high[0:2]
        send_ref[d, 6] = high[2:6]
        return carry

    lax.fori_loop(0, send_ref.shape[0], one, 0)


def cell_rows(recv_ref, slot):
    block, odd = slot >> 1, slot & 1
    return [recv_ref[block, 2 * odd + half] for half in range(2)]


def velocity_rows(recv_ref, slot):
    block, odd = slot >> 1, (slot & 1) == 1
    first, middle, last = recv_ref[block, 4], recv_ref[block, 5], recv_ref[block, 6]
    even_rows = jnp.concatenate([first, middle[0:2]], axis=0)
    odd_rows = jnp.concatenate([middle[2:4], last], axis=0)
    rows = jnp.where(odd, odd_rows, even_rows)
    return rows[0:3], rows[3:6]


def first_exchange_kernel(sizes, cell_ref, meta_ref, pos_ref, h_ref, vel_ref, recv_ref, metas_ref,
                          q_ref, v_ref, send_ref, send_sems, recv_sems):
    def fill():
        for cell in range(pos_ref.shape[1]):
            for half in range(2):
                lanes = slice(half * LANES, (half + 1) * LANES)
                for component in range(3):
                    q_ref[cell, 4 * half + component] = pos_ref[component, cell, lanes]
                    v_ref[cell, 3 * half + component] = vel_ref[component, cell, lanes]
                q_ref[cell, 4 * half + 3] = h_ref[cell, lanes]
        fill_blocks(cell_ref, q_ref, v_ref, send_ref)

    pairs = ((meta_ref, metas_ref, True), (send_ref, recv_ref, False))
    exchange(sizes, fill, pairs, send_sems, recv_sems)


def last_exchange_kernel(sizes, cell_ref, q_ref, v_ref, recv_ref, send_ref, send_sems, recv_sems):
    def fill():
        fill_blocks(cell_ref, q_ref, v_ref, send_ref)

    exchange(sizes, fill, ((send_ref, recv_ref, False),), send_sems, recv_sems)


def halo(sizes, fill, pairs, send_sems, recv_sems):
    here = [lax.axis_index(axis) for axis in AXES]
    peers = []
    for axis, step in neighbour_steps():
        there = [0] * 3
        there[AXES.index(axis)] = (-step) % sizes[AXES.index(axis)]
        peers.append(shifted(here, there, sizes))
    barrier, signals = greet(peers)
    fill()
    pl.semaphore_wait(barrier, signals)
    copies = []
    for which, (source, target) in enumerate(pairs):
        for number, there in enumerate(peers):
            copies.append(
                pltpu.make_async_remote_copy(
                    src_ref=source, dst_ref=target.at[number + 1],
                    send_sem=send_sems.at[which, number], recv_sem=recv_sems.at[which, number],
                    device_id=there, device_id_type=MESH,
                )
            )
            copies[-1].start()
    for copy in copies:
        copy.wait()


def cell_halo_kernel(sizes, slot_ref, count_ref, recv_ref, table_ref, counts_ref, send_sems, recv_sems):
    def fill():
        counts_ref[0] = count_ref[...]
        for place in range(table_ref.shape[1]):
            low, high = cell_rows(recv_ref, slot_ref[place])
            table_ref[0, place, 0:4] = low
            table_ref[0, place, 4:8] = high

    pairs = ((count_ref, counts_ref), (table_ref.at[0], table_ref))
    halo(sizes, fill, pairs, send_sems, recv_sems)


def rho_halo_kernel(sizes, rho_ref, table_ref, send_sems, recv_sems):
    def fill():
        table_ref[0] = rho_ref[...]

    halo(sizes, fill, ((rho_ref, table_ref),), send_sems, recv_sems)


def unpack_kernel(slot_ref, recv_ref, pos_ref, vel_ref, rho_ref):
    for place in range(pos_ref.shape[1]):
        slot = slot_ref[place]
        rows = cell_rows(recv_ref, slot)
        velocity = velocity_rows(recv_ref, slot)
        for half in range(2):
            lanes = slice(half * LANES, (half + 1) * LANES)
            for component in range(3):
                pos_ref[component, place, lanes] = rows[half][component]
                vel_ref[component, place, lanes] = velocity[half][component]
            rho_ref[place, lanes] = rows[half][3]


def fixed_point(table_ref, fixed_ref, box):
    row = lax.broadcasted_iota(jnp.int32, (8, LANES), 0) & 3
    scale = jnp.full((8, LANES), 2.0**32 / box[2], jnp.float32)
    scale = jnp.where(row == 0, 2.0**32 / box[0], jnp.where(row == 1, 2.0**32 / box[1], scale))
    scale = jnp.where(row == 3, 1.0, scale)
    cells = table_ref.shape[1]

    def one(cell, carry):
        for block in range(table_ref.shape[0]):
            scaled = table_ref[block, cell] * scale
            scaled = jnp.where(scaled >= 2.0**31, scaled - 2.0**32, scaled)
            fixed_ref[block * cells + cell] = scaled.astype(jnp.int32)
        return carry

    lax.fori_loop(0, cells, one, 0)


def gather_live(cell, near_ref, count_ref, pairs, partners):
    fill = jnp.int32(0)
    for partner in range(partners):
        b = near_ref[cell * partners + partner]
        live = count_ref[b]
        shift = fill & (LANES - 1)
        chunk = fill >> 7
        for table_ref, list_ref in pairs:
            rows = list_ref.shape[1]
            kept = lax.broadcasted_iota(jnp.int32, (rows, LANES), 1) < shift
            rolled = pltpu.roll(table_ref[b], shift, 1)
            first, second = rolled[0:rows], rolled[rows : 2 * rows]
            list_ref[chunk] = jnp.where(kept, list_ref[chunk], first)
            list_ref[chunk + 1] = jnp.where(kept, first, second)
            list_ref[chunk + 2] = second
        fill = fill + live
    return fill


def store_column(ref, halves):
    for half, part in enumerate(halves):
        ref[half * LANES : (half + 1) * LANES, :] = jnp.broadcast_to(part, (LANES, LANES)).T


def halves_of(ref, cell, row):
    step = ref.shape[1] // 2
    return [ref[cell, row + half * step : row + half * step + 1, :] for half in range(2)]


def row_sums(acc):
    ones = jnp.ones((8, LANES), jnp.float32)
    sums = lax.dot_general(
        ones, acc, (((1,), (1,)), ((), ())),
        precision=lax.Precision.HIGHEST, preferred_element_type=jnp.float32,
    )
    return [sums[0:1, 0:LANES], sums[0:1, LANES : 2 * LANES]]


def spread(list_ref, chunk, row):
    return jnp.broadcast_to(list_ref[chunk, row : row + 1, :], (8, LANES))


def offsets(i_refs, rows, others, shifts):
    parts = []
    for ref, other, shift in zip(i_refs, others, shifts):
        diff = ref[rows, :] - other
        if shift:
            diff = diff >> shift
        parts.append(diff.astype(jnp.float32))
    return parts


def by_row(values):
    row = lax.broadcasted_iota(jnp.int32, (8, LANES), 0) & 3
    out = jnp.full((8, LANES), values[3], jnp.float32)
    for number in range(3):
        out = jnp.where(row == number, jnp.float32(values[number]), out)
    return out


def bounds(table_ref, low_ref, high_ref):
    blocks, cells = table_ref.shape[0], table_ref.shape[1]

    def one(cell, carry):
        for block in range(blocks):
            rows = table_ref[block, cell]
            low = jnp.broadcast_to(jnp.min(rows, axis=1, keepdims=True), (8, LANES))
            high = jnp.broadcast_to(jnp.max(rows, axis=1, keepdims=True), (8, LANES))
            low_ref[block * cells + cell] = jnp.minimum(low, pltpu.roll(low, 4, 0))
            high_ref[block * cells + cell] = jnp.maximum(high, pltpu.roll(high, 4, 0))
        return carry

    lax.fori_loop(0, cells, one, 0)


def middle(low, high):
    return jnp.floor(low + high + 0.5) * 0.5


def image(low_a, high_a, low_b, high_b, lengths):
    return jnp.floor((low_a - high_b) / lengths + 0.5) * lengths


def sum_of_xyz(rows):
    return pltpu.roll(rows, 1, 0) + pltpu.roll(rows, 2, 0) + pltpu.roll(rows, 3, 0)


def one_image(cells, partners, box, near_ref, low_ref, high_ref):
    lengths = by_row(box + (1.0,))
    half = lengths * (0.5 * (1.0 - 2.0**-16))
    coordinate = (lax.broadcasted_iota(jnp.int32, (8, LANES), 0) & 3) < 3
    limit = 256.0 / math.log2(math.e)

    def one(cell, good):
        low_a, high_a = low_ref[cell], high_ref[cell]
        origin = middle(low_a, high_a)
        for partner in range(partners):
            b = near_ref[cell * partners + partner]
            low_b, high_b = low_ref[b], high_ref[b]
            shift = image(low_a, high_a, low_b, high_b, lengths)
            fits = (high_a - low_b - shift < half) & (low_a - high_b - shift > -half)
            moved = shift - origin
            reach = jnp.maximum(jnp.abs(low_b + moved), jnp.abs(high_b + moved))
            small = sum_of_xyz(reach * reach) <= limit * low_a * low_a
            fine = jnp.where(coordinate, jnp.where(fits, 1.0, 0.0), jnp.where(small, 1.0, 0.0))
            good = jnp.minimum(good, fine)
        return good

    good = lax.fori_loop(0, cells, one, jnp.ones((8, LANES), jnp.float32))
    return jnp.min(good) > 0.5


def three_parts(value):
    first = value.astype(jnp.bfloat16).astype(jnp.float32)
    value = value - first
    second = value.astype(jnp.bfloat16).astype(jnp.float32)
    return first, second, value - second


def joined(upper, lower, half):
    top = lax.broadcasted_iota(jnp.int32, (8, LANES), 0) < 4
    if half == 0:
        return jnp.where(top, upper, pltpu.roll(lower, 4, 0))
    return jnp.where(top, pltpu.roll(upper, 4, 0), lower)


def own_factors(rows, origin, own_ref):
    row = lax.broadcasted_iota(jnp.int32, (8, LANES), 0)
    centred = rows - origin
    c = -math.log2(math.e) / (rows * rows)
    c = jnp.where(row < 4, jnp.broadcast_to(c[3:4], (8, LANES)), jnp.broadcast_to(c[7:8], (8, LANES)))
    p1, p2, p3 = three_parts(jnp.where((row & 3) == 3, c, -2.0 * c * centred))
    squares = three_parts(c * sum_of_xyz(centred * centred))
    for half in range(2):
        last = jnp.where(row == 3, 1.0, 0.0)
        for number, part in enumerate(squares):
            moved = pltpu.roll(part, (number + 5 - 4 * half) % 8, 0)
            last = jnp.where(row == number, moved, last)
        groups = [joined(p1, p1, half), joined(p1, p2, half), joined(p2, p3, half), last]
        block = jnp.concatenate(groups, axis=0).T
        own_ref[half * LANES : (half + 1) * LANES, :] = block.astype(jnp.bfloat16)
    return centred


def near_factors(moved, live, near_ref, partner):
    row = lax.broadcasted_iota(jnp.int32, (8, LANES), 0)
    lane = lax.broadcasted_iota(jnp.int32, (8, LANES), 1)
    q1, q2, q3 = three_parts(jnp.where((row & 3) == 3, sum_of_xyz(moved * moved), moved))
    for half in range(2):
        alive = lane + half * LANES < live
        last = jnp.where(row < 3, 1.0, jnp.where((row > 3) | alive, 0.0, -1e30))
        groups = [joined(q1, q2, half), joined(q3, q1, half), joined(q2, q1, half), last]
        block = jnp.concatenate(groups, axis=0)
        near_ref[partner, :, half * LANES : (half + 1) * LANES] = block.astype(jnp.bfloat16)


def exponents(own_ref, near_ref, partner, rows):
    return jnp.dot(own_ref[rows, :], near_ref[partner], preferred_element_type=jnp.float32)


def lane_sums(acc):
    ones = jnp.ones((8, LANES), jnp.bfloat16)
    total = jnp.zeros((8, 2 * LANES), jnp.float32)
    for part in reversed(three_parts(acc)):
        total = total + lax.dot_general(
            ones, part.astype(jnp.bfloat16), (((1,), (1,)), ((), ())),
            preferred_element_type=jnp.float32,
        )
    return [total[0:1, 0:LANES], total[0:1, LANES : 2 * LANES]]


def fast_density(cells, partners, mass, box, near_ref, count_ref, table_ref, low_ref, high_ref, rho_ref,
                 own_ref, factor_ref, acc_ref):
    lengths = by_row(box + (1.0,))
    step = 64

    def one_cell(cell, carry):
        low_a, high_a = low_ref[cell], high_ref[cell]
        origin = middle(low_a, high_a)
        own_factors(table_ref[0, cell], origin, own_ref)
        for partner in range(partners):
            b = near_ref[cell * partners + partner]
            shift = image(low_a, high_a, low_ref[b], high_ref[b], lengths)
            moved = table_ref[b >> 5, b & 31] + (shift - origin)
            near_factors(moved, count_ref[b], factor_ref, partner)
        for block in range(2 * LANES // step):
            rows = slice(block * step, (block + 1) * step)
            acc = None
            for partner in range(partners):
                w = jnp.exp2(exponents(own_ref, factor_ref, partner, rows))
                both = w[:, 0:LANES] + w[:, LANES : 2 * LANES]
                acc = both if acc is None else acc + both
            acc_ref[rows, :] = acc
        h = halves_of(table_ref.at[0], cell, 3)
        for half, (part, total) in enumerate(zip(h, lane_sums(acc_ref[...]))):
            rho_ref[cell, half : half + 1] = mass * (1.0 + total) / (part * part * part)
        return carry

    lax.fori_loop(0, cells, one_cell, 0)


def fast_accel(cells, partners, mass, box, near_ref, count_ref, slot_ref, table_ref, low_ref, high_ref,
               inverse_ref, rho_ref, recv_ref, q_ref, v_ref,
               own_ref, factor_ref, moved_ref, ai_ref, acc_refs):
    lengths = by_row(box + (1.0,))
    step = 32

    def one_cell(cell, carry):
        low_a, high_a = low_ref[cell], high_ref[cell]
        origin = middle(low_a, high_a)
        centred = own_factors(table_ref[0, cell], origin, own_ref)
        store_column(ai_ref, halves_of(inverse_ref, cell, 0))
        for partner in range(partners):
            b = near_ref[cell * partners + partner]
            shift = image(low_a, high_a, low_ref[b], high_ref[b], lengths)
            moved = table_ref[b >> 5, b & 31] + (shift - origin)
            near_factors(moved, count_ref[b], factor_ref, partner)
            moved_ref[partner] = moved
            for half in range(2):
                moved_ref[partner, 4 * half + 3 : 4 * half + 4] = inverse_ref[b, half : half + 1]
        for block in range(2 * LANES // step):
            rows = slice(block * step, (block + 1) * step)
            own_inverse = ai_ref[rows, :]
            accs = [None] * 4
            for partner in range(partners):
                w = jnp.exp2(exponents(own_ref, factor_ref, partner, rows))
                for half in range(2):
                    near = [
                        jnp.broadcast_to(
                            moved_ref[partner, 4 * half + row : 4 * half + row + 1, :], (step, LANES)
                        )
                        for row in range(4)
                    ]
                    pair = w[:, half * LANES : (half + 1) * LANES] * (own_inverse + near[3])
                    terms = [pair * near[0], pair * near[1], pair * near[2], pair]
                    accs = [t if a is None else a + t for a, t in zip(accs, terms)]
            for acc_ref, acc in zip(acc_refs, accs):
                acc_ref[rows, :] = acc
        h = halves_of(table_ref.at[0], cell, 3)
        scale = [(time_step * 2.0 * mass) / (part * part * part * part * part) for part in h]
        velocity = velocity_rows(recv_ref, slot_ref[cell])
        whole = lane_sums(acc_refs[3][...])
        for component in range(3):
            sums = lane_sums(acc_refs[component][...])
            for half in range(2):
                row = slice(4 * half + component, 4 * half + component + 1)
                force = centred[row] * whole[half] - sums[half]
                kicked = velocity[half][component : component + 1] + force * scale[half]
                v_ref[cell, 3 * half + component : 3 * half + component + 1] = kicked
                q_ref[cell, row] = table_ref[0, cell, row] + time_step * kicked
        for half in range(2):
            row = slice(4 * half + 3, 4 * half + 4)
            q_ref[cell, row] = rho_ref[0, cell, half : half + 1]
        return carry

    lax.fori_loop(0, cells, one_cell, 0)


def density_kernel(partners, mass, unit, shifts, box, near_ref, count_ref, table_ref, rho_ref,
                   low_ref, high_ref, own_ref, factor_ref,
                   fixed_ref, list_ref, xi_ref, yi_ref, zi_ref, ci_ref, acc_ref):
    cells = table_ref.shape[1]
    bounds(table_ref, low_ref, high_ref)
    fits = one_image(cells, partners, box, near_ref, low_ref, high_ref)

    @pl.when(fits)
    def _():
        fast_density(cells, partners, mass, box, near_ref, count_ref, table_ref, low_ref, high_ref,
                     rho_ref, own_ref, factor_ref, acc_ref)

    @pl.when(jnp.logical_not(fits))
    def _():
        any_density(partners, mass, unit, shifts, box, near_ref, count_ref, table_ref, rho_ref,
                    fixed_ref, list_ref, xi_ref, yi_ref, zi_ref, ci_ref, acc_ref)


def any_density(partners, mass, unit, shifts, box, near_ref, count_ref, table_ref, rho_ref,
                fixed_ref, list_ref, xi_ref, yi_ref, zi_ref, ci_ref, acc_ref):
    cells, particles = table_ref.shape[1], 2 * LANES
    blocks = particles // 8
    i_refs = (xi_ref, yi_ref, zi_ref)
    lane = lax.broadcasted_iota(jnp.int32, (8, LANES), 1)
    factor = -math.log2(math.e) * unit * unit
    fixed_point(table_ref, fixed_ref, box)

    def one_cell(cell, carry):
        total = gather_live(cell, near_ref, count_ref, ((fixed_ref, list_ref),), partners)
        for component in range(3):
            store_column(i_refs[component], halves_of(fixed_ref, cell, component))
        h = halves_of(table_ref.at[0], cell, 3)
        store_column(ci_ref, [factor / (part * part) for part in h])
        last = (total - 1) >> 7

        def weights(chunk, others, block):
            rows = pl.ds(block * 8, 8)
            dx, dy, dz = offsets(i_refs, rows, others, shifts)
            return rows, jnp.exp2((dx * dx + dy * dy + dz * dz) * ci_ref[rows, :])

        others = [spread(list_ref, last, row) for row in range(3)]
        alive = lane < total - last * LANES
        for block in range(blocks):
            rows, w = weights(last, others, block)
            acc_ref[rows, :] = jnp.where(alive, w, 0.0)

        def one_chunk(chunk, inner):
            near = [spread(list_ref, chunk, row) for row in range(3)]
            for block in range(blocks):
                rows, w = weights(chunk, near, block)
                acc_ref[rows, :] += w
            return inner

        lax.fori_loop(0, last, one_chunk, 0)
        for half, (part, total_half) in enumerate(zip(h, row_sums(acc_ref[...]))):
            rho_ref[cell, half : half + 1] = mass * (1.0 + total_half) / (part * part * part)
        return carry

    lax.fori_loop(0, cells, one_cell, 0)


def accel_kernel(partners, mass, unit, shifts, box, near_ref, count_ref, slot_ref, table_ref, rho_ref,
                 recv_ref, q_ref, v_ref,
                 low_ref, high_ref, own_ref, factor_ref, moved_ref, sum_ref,
                 fixed_ref, inverse_ref, list_ref, inverse_list_ref, xi_ref, yi_ref, zi_ref, ci_ref, ai_ref,
                 ax_ref, ay_ref, az_ref):
    cells = table_ref.shape[1]
    bounds(table_ref, low_ref, high_ref)
    fits = one_image(cells, partners, box, near_ref, low_ref, high_ref)

    def invert(cell, carry):
        for block in range(rho_ref.shape[0]):
            inverse_ref[block * cells + cell] = 1.0 / rho_ref[block, cell]
        return carry

    lax.fori_loop(0, cells, invert, 0)

    @pl.when(fits)
    def _():
        fast_accel(cells, partners, mass, box, near_ref, count_ref, slot_ref, table_ref, low_ref, high_ref,
                   inverse_ref, rho_ref, recv_ref, q_ref, v_ref,
                   own_ref, factor_ref, moved_ref, ai_ref, (ax_ref, ay_ref, az_ref, sum_ref))

    @pl.when(jnp.logical_not(fits))
    def _():
        any_accel(partners, mass, unit, shifts, box, near_ref, count_ref, slot_ref, table_ref, rho_ref,
                  recv_ref, q_ref, v_ref, fixed_ref, inverse_ref, list_ref, inverse_list_ref,
                  xi_ref, yi_ref, zi_ref, ci_ref, ai_ref, ax_ref, ay_ref, az_ref)


def any_accel(partners, mass, unit, shifts, box, near_ref, count_ref, slot_ref, table_ref, rho_ref,
                 recv_ref, q_ref, v_ref,
                 fixed_ref, inverse_ref, list_ref, inverse_list_ref, xi_ref, yi_ref, zi_ref, ci_ref, ai_ref,
                 ax_ref, ay_ref, az_ref):
    cells, particles = table_ref.shape[1], 2 * LANES
    blocks = particles // 8
    i_refs = (xi_ref, yi_ref, zi_ref)
    acc_refs = (ax_ref, ay_ref, az_ref)
    lane = lax.broadcasted_iota(jnp.int32, (8, LANES), 1)
    factor = -math.log2(math.e) * unit * unit
    fixed_point(table_ref, fixed_ref, box)

    def one_cell(cell, carry):
        total = gather_live(
            cell, near_ref, count_ref,
            ((fixed_ref, list_ref), (inverse_ref, inverse_list_ref)), partners,
        )
        for component in range(3):
            store_column(i_refs[component], halves_of(fixed_ref, cell, component))
        h = halves_of(table_ref.at[0], cell, 3)
        store_column(ci_ref, [factor / (part * part) for part in h])
        store_column(ai_ref, halves_of(inverse_ref, cell, 0))
        last = (total - 1) >> 7

        def terms(others, other_inverse, block):
            rows = pl.ds(block * 8, 8)
            parts = offsets(i_refs, rows, others, shifts)
            dx, dy, dz = parts
            w = jnp.exp2((dx * dx + dy * dy + dz * dz) * ci_ref[rows, :])
            return rows, parts, w * (ai_ref[rows, :] + other_inverse)

        others = [spread(list_ref, last, row) for row in range(3)]
        other_inverse = spread(inverse_list_ref, last, 0)
        alive = lane < total - last * LANES
        for block in range(blocks):
            rows, parts, pair = terms(others, other_inverse, block)
            pair = jnp.where(alive, pair, 0.0)
            for acc_ref, part in zip(acc_refs, parts):
                acc_ref[rows, :] = pair * part

        def one_chunk(chunk, inner):
            near = [spread(list_ref, chunk, row) for row in range(3)]
            near_inverse = spread(inverse_list_ref, chunk, 0)
            for block in range(blocks):
                rows, parts, pair = terms(near, near_inverse, block)
                for acc_ref, part in zip(acc_refs, parts):
                    acc_ref[rows, :] += pair * part
            return inner

        lax.fori_loop(0, last, one_chunk, 0)
        scale = [(time_step * 2.0 * mass * unit) / (part * part * part * part * part) for part in h]
        velocity = velocity_rows(recv_ref, slot_ref[cell])
        for component, acc_ref in enumerate(acc_refs):
            sums = row_sums(acc_ref[...])
            for half in range(2):
                kicked = velocity[half][component : component + 1] + sums[half] * scale[half]
                v_ref[cell, 3 * half + component : 3 * half + component + 1] = kicked
                row = slice(4 * half + component, 4 * half + component + 1)
                q_ref[cell, row] = table_ref[0, cell, row] + time_step * kicked
        for half in range(2):
            row = slice(4 * half + 3, 4 * half + 4)
            q_ref[cell, row] = rho_ref[0, cell, half : half + 1]
        return carry

    lax.fori_loop(0, cells, one_cell, 0)


def shards(positions, smoothing, velocity, counts, plan_before, neighbours, plan_after):
    cell_count = positions.shape[0]
    particles = positions.shape[-1]
    partners = neighbours.shape[1] + 1
    sizes = tuple(lax.axis_size(axis) for axis in AXES)
    devices = sizes[0] * sizes[1] * sizes[2]
    box = (float(cell_count // 4 * sizes[0]), float(2 * sizes[1]), float(2 * sizes[2]))
    longest = max(box)
    shifts = tuple(int(round(math.log2(longest / length))) for length in box)
    unit = longest / 2.0**32
    mass = 1.0 / (partners * particles)

    smem = pl.BlockSpec(memory_space=pltpu.SMEM)
    vmem = pl.BlockSpec(memory_space=pltpu.VMEM)
    f32 = lambda *shape: jax.ShapeDtypeStruct(shape, jnp.float32)
    effects = lambda number: pltpu.CompilerParams(has_side_effects=True, collective_id=number)
    sems = lambda *count: [pltpu.SemaphoreType.DMA(count)] * 2
    blocks = (devices, 7, 4, LANES)
    cells8 = pltpu.VMEM((cell_count, 8, LANES), jnp.float32)

    keys, cells = slots_of(jnp.stack([plan_before, plan_after]), cell_count, devices)
    meta = jnp.concatenate([keys.reshape(-1), counts, jnp.zeros_like(counts)])[None, :]
    recv, metas = pl.pallas_call(
        functools.partial(first_exchange_kernel, sizes),
        out_shape=[f32(*blocks), jax.ShapeDtypeStruct((devices, 1, LANES), jnp.int32)],
        in_specs=[smem, vmem, vmem, vmem, vmem],
        out_specs=[vmem] * 2,
        scratch_shapes=[cells8, cells8, pltpu.VMEM(blocks, jnp.float32)] + sems(2),
        compiler_params=effects(0),
        name="first_exchange",
    )(cells[0], meta, jnp.transpose(positions, (1, 0, 2)), smoothing, jnp.transpose(velocity, (1, 0, 2)))

    here = [lax.axis_index(axis) for axis in AXES]
    place = flat(here, sizes) * cell_count + jnp.arange(cell_count, dtype=jnp.int32)
    metas = metas[:, 0, :]
    keys_before, keys_after = metas[:, 0:cell_count], metas[:, cell_count : 2 * cell_count]
    all_counts = metas[:, 2 * cell_count : 3 * cell_count]
    source = 2 * jnp.arange(devices, dtype=jnp.int32)[:, None]

    def pick(keys, values):
        hit = (keys >> 1)[None] == place[:, None, None]
        return jnp.sum(jnp.where(hit, values[None], 0), axis=(1, 2))

    slot_count = pick(keys_before, (keys_before & 1) + source + all_counts * (2 * devices))
    slot_before, own_count = slot_count % (2 * devices), slot_count // (2 * devices)
    slot_after = pick(keys_after, (keys_after & 1) + source)
    near = near_table(neighbours, cell_count)

    table, table_count = pl.pallas_call(
        functools.partial(cell_halo_kernel, sizes),
        out_shape=[f32(7, cell_count, 8, LANES), jax.ShapeDtypeStruct((7, 1, LANES), jnp.int32)],
        in_specs=[smem, vmem, vmem],
        out_specs=[vmem, vmem],
        scratch_shapes=sems(2, 6),
        compiler_params=effects(1),
        name="cell_halo",
    )(slot_before, jnp.pad(own_count, (0, LANES - cell_count))[None, :], recv)
    table_count = table_count[:, 0, :cell_count].reshape(-1)

    chunks = partners * particles // LANES + 1
    square = (particles, LANES)
    columns = [pltpu.VMEM(square, jnp.int32)] * 3
    extent = [pltpu.VMEM((7 * cell_count, 8, LANES), jnp.float32)] * 2 + [
        pltpu.VMEM((particles, 32), jnp.bfloat16),
        pltpu.VMEM((partners, 32, particles), jnp.bfloat16),
    ]
    fixed = pltpu.VMEM((7 * cell_count, 8, LANES), jnp.int32)
    rho = pl.pallas_call(
        functools.partial(density_kernel, partners, mass, unit, shifts, box),
        out_shape=f32(cell_count, 2, LANES),
        in_specs=[smem, smem, vmem],
        out_specs=vmem,
        scratch_shapes=extent + [fixed, pltpu.VMEM((chunks, 4, LANES), jnp.int32)] + columns
        + [pltpu.VMEM(square, jnp.float32)] * 2,
        name="density",
    )(near, table_count, table)

    table_rho = pl.pallas_call(
        functools.partial(rho_halo_kernel, sizes),
        out_shape=f32(7, cell_count, 2, LANES),
        in_specs=[vmem],
        out_specs=vmem,
        scratch_shapes=sems(1, 6),
        compiler_params=effects(2),
        name="rho_halo",
    )(rho)

    out_q, out_v = pl.pallas_call(
        functools.partial(accel_kernel, partners, mass, unit, shifts, box),
        out_shape=[f32(cell_count, 8, LANES)] * 2,
        in_specs=[smem, smem, smem, vmem, vmem, vmem],
        out_specs=[vmem, vmem],
        scratch_shapes=extent
        + [
            pltpu.VMEM((partners, 8, LANES), jnp.float32),
            pltpu.VMEM(square, jnp.float32),
            fixed,
            pltpu.VMEM((7 * cell_count, 2, LANES), jnp.float32),
            pltpu.VMEM((chunks, 4, LANES), jnp.int32),
            pltpu.VMEM((chunks, 1, LANES), jnp.float32),
        ]
        + columns
        + [pltpu.VMEM(square, jnp.float32)] * 5,
        name="accel",
    )(near, table_count, slot_before, table, table_rho, recv)

    last = pl.pallas_call(
        functools.partial(last_exchange_kernel, sizes),
        out_shape=f32(*blocks),
        in_specs=[smem, vmem, vmem],
        out_specs=vmem,
        scratch_shapes=[pltpu.VMEM(blocks, jnp.float32)] + sems(1),
        compiler_params=effects(3),
        name="last_exchange",
    )(cells[1], out_q, out_v)
    new_pos, new_vel, new_rho = pl.pallas_call(
        unpack_kernel,
        out_shape=[f32(3, cell_count, particles)] * 2 + [f32(cell_count, particles)],
        in_specs=[smem, vmem],
        out_specs=[vmem] * 3,
        name="unpack",
    )(slot_after, last)
    return jnp.transpose(new_pos, (1, 0, 2)), jnp.transpose(new_vel, (1, 0, 2)), new_rho


def solution(mesh):
    in_specs = (
        P(("gx", "gy", "gz"), None, None),
        P(("gx", "gy", "gz"), None),
        P(("gx", "gy", "gz"), None, None),
        P(("gx", "gy", "gz")),
        P(("gx", "gy", "gz")),
        P(("gx", "gy", "gz"), None),
        P(("gx", "gy", "gz")),
    )
    out_specs = (
        P(("gx", "gy", "gz"), None, None),
        P(("gx", "gy", "gz"), None, None),
        P(("gx", "gy", "gz"), None),
    )
    return jax.shard_map(shards, mesh=mesh, in_specs=in_specs, out_specs=out_specs, check_vma=False)
```

```python
import functools
import math

import jax
import jax.numpy as jnp
from jax import lax
from jax.experimental import pallas as pl
from jax.experimental.pallas import tpu as pltpu
from jax.sharding import PartitionSpec as P

time_step = 0.1
LANES = 128
AXES = ("gx", "gy", "gz")
MESH = pl.DeviceIdType.MESH

def neighbour_steps():
    return [(axis, step) for axis in AXES for step in (-1, 1)]


def slots_of(plans, cell_count, devices):
    target = plans // cell_count
    ladder = jnp.arange(cell_count, dtype=jnp.int32)
    earlier = (target[:, :, None] == target[:, None, :]) & (ladder[None, :] < ladder[:, None])
    rank = jnp.sum(earlier.astype(jnp.int32), axis=2)
    slot = target * 2 + rank
    every = jnp.arange(devices * 2, dtype=jnp.int32)
    hit = slot[:, None, :] == every[None, :, None]
    return plans * 2 + rank, jnp.sum(jnp.where(hit, ladder, 0), axis=2)


def near_table(neighbours, cell_count):
    sizes = {axis: lax.axis_size(axis) for axis in AXES}
    here = {axis: lax.axis_index(axis) for axis in AXES}
    owner = neighbours // cell_count
    block = jnp.zeros_like(owner)
    for number, (axis, step) in enumerate(neighbour_steps(), 1):
        there = dict(here)
        there[axis] = (here[axis] + step) % sizes[axis]
        device = (there["gx"] * sizes["gy"] + there["gy"]) * sizes["gz"] + there["gz"]
        block = jnp.where(owner == device, number, block)
    near = block * cell_count + neighbours % cell_count
    own = jnp.arange(cell_count, dtype=jnp.int32)[:, None]
    return jnp.concatenate([own, near], axis=1).reshape(-1)


def peer_offsets(sizes):
    count_x, count_y, count_z = sizes
    steps = [(x, y, z) for x in range(count_x) for y in range(count_y) for z in range(count_z)][1:]

    def hops(step):
        x, y, z = step
        chips = count_z // 2
        return min(x, count_x - x) + min(y, count_y - y) + min(z // 2, chips - z // 2)

    return sorted(steps, key=lambda step: -hops(step))


def shifted(here, step, sizes):
    return tuple(lax.rem(h + d, n) if d else h for h, d, n in zip(here, step, sizes))


def flat(place, sizes):
    return (place[0] * sizes[1] + place[1]) * sizes[2] + place[2]


def greet(peers):
    barrier = pltpu.get_barrier_semaphore()
    for peer in peers:
        pl.semaphore_signal(barrier, inc=1, device_id=peer, device_id_type=MESH)
    return barrier, len(peers)


def exchange(sizes, fill, pairs, send_sems, recv_sems):
    here = [lax.axis_index(axis) for axis in AXES]
    me = flat(here, sizes)
    peers = [shifted(here, step, sizes) for step in peer_offsets(sizes)]
    barrier, signals = greet(peers)
    fill()
    pl.semaphore_wait(barrier, signals)
    for number, (source, target, whole) in enumerate(pairs):
        for there in peers:
            pltpu.make_async_remote_copy(
                src_ref=source if whole else source.at[flat(there, sizes)],
                dst_ref=target.at[me],
                send_sem=send_sems.at[number],
                recv_sem=recv_sems.at[number],
                device_id=there,
                device_id_type=MESH,
            ).start()
    for source, target, whole in pairs:
        target[me] = source[...] if whole else source[me]
    for number, (source, target, whole) in enumerate(pairs):
        most = target.at[pl.ds(0, signals)]
        arrived = pltpu.make_async_remote_copy(
            src_ref=most, dst_ref=most, send_sem=send_sems.at[number],
            recv_sem=recv_sems.at[number], device_id=tuple(here), device_id_type=MESH,
        )
        arrived.wait_send()
        arrived.wait_recv()


def fill_blocks(cell_ref, q_ref, v_ref, send_ref):
    def one(d, carry):
        first, second = cell_ref[2 * d], cell_ref[2 * d + 1]
        for number, cell in enumerate((first, second)):
            rows = q_ref[cell]
            send_ref[d, 2 * number] = rows[0:4]
            send_ref[d, 2 * number + 1] = rows[4:8]
        low, high = v_ref[first], v_ref[second]
        send_ref[d, 4] = low[0:4]
        send_ref[d, 5, 0:2] = low[4:6]
        send_ref[d, 5, 2:4] = high[0:2]
        send_ref[d, 6] = high[2:6]
        return carry

    lax.fori_loop(0, send_ref.shape[0], one, 0)


def cell_rows(recv_ref, slot):
    block, odd = slot >> 1, slot & 1
    return [recv_ref[block, 2 * odd + half] for half in range(2)]


def velocity_rows(recv_ref, slot):
    block, odd = slot >> 1, (slot & 1) == 1
    first, middle, last = recv_ref[block, 4], recv_ref[block, 5], recv_ref[block, 6]
    even_rows = jnp.concatenate([first, middle[0:2]], axis=0)
    odd_rows = jnp.concatenate([middle[2:4], last], axis=0)
    rows = jnp.where(odd, odd_rows, even_rows)
    return rows[0:3], rows[3:6]


def first_exchange_kernel(sizes, cell_ref, meta_ref, pos_ref, h_ref, vel_ref, recv_ref, metas_ref,
                          q_ref, v_ref, send_ref, send_sems, recv_sems):
    def fill():
        for cell in range(pos_ref.shape[1]):
            for half in range(2):
                lanes = slice(half * LANES, (half + 1) * LANES)
                for component in range(3):
                    q_ref[cell, 4 * half + component] = pos_ref[component, cell, lanes]
                    v_ref[cell, 3 * half + component] = vel_ref[component, cell, lanes]
                q_ref[cell, 4 * half + 3] = h_ref[cell, lanes]
        fill_blocks(cell_ref, q_ref, v_ref, send_ref)

    pairs = ((meta_ref, metas_ref, True), (send_ref, recv_ref, False))
    exchange(sizes, fill, pairs, send_sems, recv_sems)


def last_exchange_kernel(sizes, cell_ref, q_ref, v_ref, recv_ref, send_ref, send_sems, recv_sems):
    def fill():
        fill_blocks(cell_ref, q_ref, v_ref, send_ref)

    exchange(sizes, fill, ((send_ref, recv_ref, False),), send_sems, recv_sems)


def halo(sizes, fill, pairs, send_sems, recv_sems):
    here = [lax.axis_index(axis) for axis in AXES]
    peers = []
    for axis, step in neighbour_steps():
        there = [0] * 3
        there[AXES.index(axis)] = (-step) % sizes[AXES.index(axis)]
        peers.append(shifted(here, there, sizes))
    barrier, signals = greet(peers)
    fill()
    pl.semaphore_wait(barrier, signals)
    copies = []
    for which, (source, target) in enumerate(pairs):
        for number, there in enumerate(peers):
            copies.append(
                pltpu.make_async_remote_copy(
                    src_ref=source, dst_ref=target.at[number + 1],
                    send_sem=send_sems.at[which, number], recv_sem=recv_sems.at[which, number],
                    device_id=there, device_id_type=MESH,
                )
            )
            copies[-1].start()
    for copy in copies:
        copy.wait()


def cell_halo_kernel(sizes, slot_ref, count_ref, recv_ref, table_ref, counts_ref, send_sems, recv_sems):
    def fill():
        counts_ref[0] = count_ref[...]
        for place in range(table_ref.shape[1]):
            low, high = cell_rows(recv_ref, slot_ref[place])
            table_ref[0, place, 0:4] = low
            table_ref[0, place, 4:8] = high

    pairs = ((count_ref, counts_ref), (table_ref.at[0], table_ref))
    halo(sizes, fill, pairs, send_sems, recv_sems)


def rho_halo_kernel(sizes, rho_ref, table_ref, send_sems, recv_sems):
    def fill():
        table_ref[0] = rho_ref[...]

    halo(sizes, fill, ((rho_ref, table_ref),), send_sems, recv_sems)


def unpack_kernel(slot_ref, recv_ref, pos_ref, vel_ref, rho_ref):
    for place in range(pos_ref.shape[1]):
        slot = slot_ref[place]
        rows = cell_rows(recv_ref, slot)
        velocity = velocity_rows(recv_ref, slot)
        for half in range(2):
            lanes = slice(half * LANES, (half + 1) * LANES)
            for component in range(3):
                pos_ref[component, place, lanes] = rows[half][component]
                vel_ref[component, place, lanes] = velocity[half][component]
            rho_ref[place, lanes] = rows[half][3]


def fixed_point(table_ref, fixed_ref, box):
    row = lax.broadcasted_iota(jnp.int32, (8, LANES), 0) & 3
    scale = jnp.full((8, LANES), 2.0**32 / box[2], jnp.float32)
    scale = jnp.where(row == 0, 2.0**32 / box[0], jnp.where(row == 1, 2.0**32 / box[1], scale))
    scale = jnp.where(row == 3, 1.0, scale)
    cells = table_ref.shape[1]

    def one(cell, carry):
        for block in range(table_ref.shape[0]):
            scaled = table_ref[block, cell] * scale
            scaled = jnp.where(scaled >= 2.0**31, scaled - 2.0**32, scaled)
            fixed_ref[block * cells + cell] = scaled.astype(jnp.int32)
        return carry

    lax.fori_loop(0, cells, one, 0)


def gather_live(cell, near_ref, count_ref, pairs, partners):
    fill = jnp.int32(0)
    for partner in range(partners):
        b = near_ref[cell * partners + partner]
        live = count_ref[b]
        shift = fill & (LANES - 1)
        chunk = fill >> 7
        for table_ref, list_ref in pairs:
            rows = list_ref.shape[1]
            kept = lax.broadcasted_iota(jnp.int32, (rows, LANES), 1) < shift
            rolled = pltpu.roll(table_ref[b], shift, 1)
            first, second = rolled[0:rows], rolled[rows : 2 * rows]
            list_ref[chunk] = jnp.where(kept, list_ref[chunk], first)
            list_ref[chunk + 1] = jnp.where(kept, first, second)
            list_ref[chunk + 2] = second
        fill = fill + live
    return fill


def store_column(ref, halves):
    for half, part in enumerate(halves):
        ref[half * LANES : (half + 1) * LANES, :] = jnp.broadcast_to(part, (LANES, LANES)).T


def halves_of(ref, cell, row):
    step = ref.shape[1] // 2
    return [ref[cell, row + half * step : row + half * step + 1, :] for half in range(2)]


def row_sums(acc):
    ones = jnp.ones((8, LANES), jnp.float32)
    sums = lax.dot_general(
        ones, acc, (((1,), (1,)), ((), ())),
        precision=lax.Precision.HIGHEST, preferred_element_type=jnp.float32,
    )
    return [sums[0:1, 0:LANES], sums[0:1, LANES : 2 * LANES]]


def spread(list_ref, chunk, row):
    return jnp.broadcast_to(list_ref[chunk, row : row + 1, :], (8, LANES))


def offsets(i_refs, rows, others, shifts):
    parts = []
    for ref, other, shift in zip(i_refs, others, shifts):
        diff = ref[rows, :] - other
        if shift:
            diff = diff >> shift
        parts.append(diff.astype(jnp.float32))
    return parts


def by_row(values):
    row = lax.broadcasted_iota(jnp.int32, (8, LANES), 0) & 3
    out = jnp.full((8, LANES), values[3], jnp.float32)
    for number in range(3):
        out = jnp.where(row == number, jnp.float32(values[number]), out)
    return out


def bounds(table_ref, low_ref, high_ref):
    blocks, cells = table_ref.shape[0], table_ref.shape[1]
    together = 4

    def some(step, carry):
        which = [(block, step * together + n) for n in range(together) for block in range(blocks)]
        lows = [jnp.min(table_ref[block, cell], axis=1, keepdims=True) for block, cell in which]
        highs = [jnp.max(table_ref[block, cell], axis=1, keepdims=True) for block, cell in which]
        for (block, cell), low, high in zip(which, lows, highs):
            low = jnp.broadcast_to(low, (8, LANES))
            high = jnp.broadcast_to(high, (8, LANES))
            low_ref[block * cells + cell] = jnp.minimum(low, pltpu.roll(low, 4, 0))
            high_ref[block * cells + cell] = jnp.maximum(high, pltpu.roll(high, 4, 0))
        return carry

    lax.fori_loop(0, cells // together, some, 0)


def middle(low, high):
    return jnp.floor(low + high + 0.5) * 0.5


def image(low_a, high_a, low_b, high_b, lengths):
    return jnp.floor((low_a - high_b) / lengths + 0.5) * lengths


def sum_of_xyz(rows):
    return pltpu.roll(rows, 1, 0) + pltpu.roll(rows, 2, 0) + pltpu.roll(rows, 3, 0)


def one_image(cells, partners, box, near_ref, low_ref, high_ref):
    lengths = by_row(box + (1.0,))
    half = lengths * (0.5 * (1.0 - 2.0**-16))
    coordinate = (lax.broadcasted_iota(jnp.int32, (8, LANES), 0) & 3) < 3
    limit = 256.0 / math.log2(math.e)

    def one(cell, good):
        low_a, high_a = low_ref[cell], high_ref[cell]
        origin = middle(low_a, high_a)
        for partner in range(partners):
            b = near_ref[cell * partners + partner]
            low_b, high_b = low_ref[b], high_ref[b]
            shift = image(low_a, high_a, low_b, high_b, lengths)
            fits = (high_a - low_b - shift < half) & (low_a - high_b - shift > -half)
            moved = shift - origin
            reach = jnp.maximum(jnp.abs(low_b + moved), jnp.abs(high_b + moved))
            small = sum_of_xyz(reach * reach) <= limit * low_a * low_a
            fine = jnp.where(coordinate, jnp.where(fits, 1.0, 0.0), jnp.where(small, 1.0, 0.0))
            good = jnp.minimum(good, fine)
        return good

    good = lax.fori_loop(0, cells, one, jnp.ones((8, LANES), jnp.float32))
    return jnp.min(good) > 0.5


def three_parts(value):
    first = value.astype(jnp.bfloat16).astype(jnp.float32)
    value = value - first
    second = value.astype(jnp.bfloat16).astype(jnp.float32)
    return first, second, value - second


def joined(upper, lower, half):
    top = lax.broadcasted_iota(jnp.int32, (8, LANES), 0) < 4
    if half == 0:
        return jnp.where(top, upper, pltpu.roll(lower, 4, 0))
    return jnp.where(top, pltpu.roll(upper, 4, 0), lower)


def own_factors(rows, origin, own_ref):
    row = lax.broadcasted_iota(jnp.int32, (8, LANES), 0)
    centred = rows - origin
    c = -math.log2(math.e) / (rows * rows)
    c = jnp.where(row < 4, jnp.broadcast_to(c[3:4], (8, LANES)), jnp.broadcast_to(c[7:8], (8, LANES)))
    p1, p2, p3 = three_parts(jnp.where((row & 3) == 3, c, -2.0 * c * centred))
    squares = three_parts(c * sum_of_xyz(centred * centred))
    for half in range(2):
        last = jnp.where(row == 3, 1.0, 0.0)
        for number, part in enumerate(squares):
            moved = pltpu.roll(part, (number + 5 - 4 * half) % 8, 0)
            last = jnp.where(row == number, moved, last)
        groups = [joined(p1, p1, half), joined(p1, p2, half), joined(p2, p3, half), last]
        block = jnp.concatenate(groups, axis=0).T
        own_ref[half * LANES : (half + 1) * LANES, :] = block.astype(jnp.bfloat16)
    return centred


def near_factors(moved, live, near_ref, partner):
    row = lax.broadcasted_iota(jnp.int32, (8, LANES), 0)
    lane = lax.broadcasted_iota(jnp.int32, (8, LANES), 1)
    q1, q2, q3 = three_parts(jnp.where((row & 3) == 3, sum_of_xyz(moved * moved), moved))
    for half in range(2):
        alive = lane + half * LANES < live
        last = jnp.where(row < 3, 1.0, jnp.where((row > 3) | alive, 0.0, -1e30))
        groups = [joined(q1, q2, half), joined(q3, q1, half), joined(q2, q1, half), last]
        block = jnp.concatenate(groups, axis=0)
        near_ref[partner, :, half * LANES : (half + 1) * LANES] = block.astype(jnp.bfloat16)


def exponents(own_ref, near_ref, partner, rows):
    return jnp.dot(own_ref[rows, :], near_ref[partner], preferred_element_type=jnp.float32)


def lane_sums(acc):
    halves = []
    for half in range(2):
        part = acc[half * LANES : (half + 1) * LANES, :].T
        eight = part[0:8]
        for row in range(8, LANES, 8):
            eight = eight + part[row : row + 8]
        halves.append(jnp.sum(eight, axis=0, keepdims=True))
    return halves


def fast_density(cells, partners, mass, box, near_ref, count_ref, table_ref, low_ref, high_ref, rho_ref,
                 own_ref, factor_ref, acc_ref):
    lengths = by_row(box + (1.0,))
    step = 64

    def one_cell(cell, own_ref, factor_ref, acc_ref):
        low_a, high_a = low_ref[cell], high_ref[cell]
        origin = middle(low_a, high_a)
        own_factors(table_ref[0, cell], origin, own_ref)
        for partner in range(partners):
            b = near_ref[cell * partners + partner]
            shift = image(low_a, high_a, low_ref[b], high_ref[b], lengths)
            moved = table_ref[b >> 5, b & 31] + (shift - origin)
            near_factors(moved, count_ref[b], factor_ref, partner)
        for block in range(2 * LANES // step):
            rows = slice(block * step, (block + 1) * step)
            acc = None
            for partner in range(partners):
                w = jnp.exp2(exponents(own_ref, factor_ref, partner, rows))
                both = w[:, 0:LANES] + w[:, LANES : 2 * LANES]
                acc = both if acc is None else acc + both
            acc_ref[rows, :] = acc
        h = halves_of(table_ref.at[0], cell, 3)
        for half, (part, total) in enumerate(zip(h, lane_sums(acc_ref[...]))):
            rho_ref[cell, half : half + 1] = mass * (1.0 + total) / (part * part * part)

    def two_cells(pair, carry):
        for number in range(2):
            one_cell(2 * pair + number, own_ref.at[number], factor_ref.at[number], acc_ref.at[number])
        return carry

    lax.fori_loop(0, cells // 2, two_cells, 0)


def fast_accel(cells, partners, mass, box, near_ref, count_ref, slot_ref, table_ref, low_ref, high_ref,
               inverse_ref, rho_ref, recv_ref, q_ref, v_ref,
               own_ref, factor_ref, moved_ref, ai_ref, acc_refs):
    lengths = by_row(box + (1.0,))
    step = 32

    def one_cell(cell, own_ref, factor_ref, moved_ref, ai_ref, acc_refs):
        low_a, high_a = low_ref[cell], high_ref[cell]
        origin = middle(low_a, high_a)
        centred = own_factors(table_ref[0, cell], origin, own_ref)
        store_column(ai_ref, halves_of(inverse_ref, cell, 0))
        for partner in range(partners):
            b = near_ref[cell * partners + partner]
            shift = image(low_a, high_a, low_ref[b], high_ref[b], lengths)
            moved = table_ref[b >> 5, b & 31] + (shift - origin)
            near_factors(moved, count_ref[b], factor_ref, partner)
            moved_ref[partner] = moved
            for half in range(2):
                moved_ref[partner, 4 * half + 3 : 4 * half + 4] = inverse_ref[b, half : half + 1]
        for block in range(2 * LANES // step):
            rows = slice(block * step, (block + 1) * step)
            own_inverse = ai_ref[rows, :]
            accs = [None] * 4
            for partner in range(partners):
                w = jnp.exp2(exponents(own_ref, factor_ref, partner, rows))
                for half in range(2):
                    near = [
                        jnp.broadcast_to(
                            moved_ref[partner, 4 * half + row : 4 * half + row + 1, :], (step, LANES)
                        )
                        for row in range(4)
                    ]
                    pair = w[:, half * LANES : (half + 1) * LANES] * (own_inverse + near[3])
                    terms = [pair * near[0], pair * near[1], pair * near[2], pair]
                    accs = [t if a is None else a + t for a, t in zip(accs, terms)]
            for acc_ref, acc in zip(acc_refs, accs):
                acc_ref[rows, :] = acc
        h = halves_of(table_ref.at[0], cell, 3)
        scale = [(time_step * 2.0 * mass) / (part * part * part * part * part) for part in h]
        velocity = velocity_rows(recv_ref, slot_ref[cell])
        whole = lane_sums(acc_refs[3][...])
        for component in range(3):
            sums = lane_sums(acc_refs[component][...])
            for half in range(2):
                row = slice(4 * half + component, 4 * half + component + 1)
                force = centred[row] * whole[half] - sums[half]
                kicked = velocity[half][component : component + 1] + force * scale[half]
                v_ref[cell, 3 * half + component : 3 * half + component + 1] = kicked
                q_ref[cell, row] = table_ref[0, cell, row] + time_step * kicked
        for half in range(2):
            row = slice(4 * half + 3, 4 * half + 4)
            q_ref[cell, row] = rho_ref[0, cell, half : half + 1]

    def two_cells(pair, carry):
        for number in range(2):
            one_cell(2 * pair + number, own_ref.at[number], factor_ref.at[number], moved_ref.at[number], ai_ref.at[number], [ref.at[number] for ref in acc_refs])
        return carry

    lax.fori_loop(0, cells // 2, two_cells, 0)


def density_kernel(partners, mass, unit, shifts, box, near_ref, count_ref, table_ref, rho_ref, fits_ref,
                   low_ref, high_ref, own_ref, factor_ref,
                   fixed_ref, list_ref, xi_ref, yi_ref, zi_ref, ci_ref, acc_ref):
    cells = table_ref.shape[1]
    bounds(table_ref, low_ref, high_ref)
    fits = one_image(cells, partners, box, near_ref, low_ref, high_ref)

    fits_ref[0] = jnp.where(fits, 1, 0)

    @pl.when(fits)
    def _():
        fast_density(cells, partners, mass, box, near_ref, count_ref, table_ref, low_ref, high_ref,
                     rho_ref, own_ref, factor_ref, acc_ref)

    @pl.when(jnp.logical_not(fits))
    def _():
        any_density(partners, mass, unit, shifts, box, near_ref, count_ref, table_ref, rho_ref,
                    fixed_ref, list_ref, xi_ref, yi_ref, zi_ref, ci_ref, acc_ref.at[0])


def any_density(partners, mass, unit, shifts, box, near_ref, count_ref, table_ref, rho_ref,
                fixed_ref, list_ref, xi_ref, yi_ref, zi_ref, ci_ref, acc_ref):
    cells, particles = table_ref.shape[1], 2 * LANES
    blocks = particles // 8
    i_refs = (xi_ref, yi_ref, zi_ref)
    lane = lax.broadcasted_iota(jnp.int32, (8, LANES), 1)
    factor = -math.log2(math.e) * unit * unit
    fixed_point(table_ref, fixed_ref, box)

    def one_cell(cell, carry):
        total = gather_live(cell, near_ref, count_ref, ((fixed_ref, list_ref),), partners)
        for component in range(3):
            store_column(i_refs[component], halves_of(fixed_ref, cell, component))
        h = halves_of(table_ref.at[0], cell, 3)
        store_column(ci_ref, [factor / (part * part) for part in h])
        last = (total - 1) >> 7

        def weights(chunk, others, block):
            rows = pl.ds(block * 8, 8)
            dx, dy, dz = offsets(i_refs, rows, others, shifts)
            return rows, jnp.exp2((dx * dx + dy * dy + dz * dz) * ci_ref[rows, :])

        others = [spread(list_ref, last, row) for row in range(3)]
        alive = lane < total - last * LANES
        for block in range(blocks):
            rows, w = weights(last, others, block)
            acc_ref[rows, :] = jnp.where(alive, w, 0.0)

        def one_chunk(chunk, inner):
            near = [spread(list_ref, chunk, row) for row in range(3)]
            for block in range(blocks):
                rows, w = weights(chunk, near, block)
                acc_ref[rows, :] += w
            return inner

        lax.fori_loop(0, last, one_chunk, 0)
        for half, (part, total_half) in enumerate(zip(h, row_sums(acc_ref[...]))):
            rho_ref[cell, half : half + 1] = mass * (1.0 + total_half) / (part * part * part)
        return carry

    lax.fori_loop(0, cells, one_cell, 0)


def accel_kernel(partners, mass, unit, shifts, box, near_ref, count_ref, slot_ref, fits_ref, table_ref, rho_ref,
                 recv_ref, q_ref, v_ref,
                 low_ref, high_ref, own_ref, factor_ref, moved_ref, sum_ref,
                 fixed_ref, inverse_ref, list_ref, inverse_list_ref, xi_ref, yi_ref, zi_ref, ci_ref, ai_ref,
                 ax_ref, ay_ref, az_ref):
    cells = table_ref.shape[1]
    bounds(table_ref, low_ref, high_ref)
    fits = fits_ref[0] > 0

    def invert(cell, carry):
        for block in range(rho_ref.shape[0]):
            inverse_ref[block * cells + cell] = 1.0 / rho_ref[block, cell]
        return carry

    lax.fori_loop(0, cells, invert, 0)

    @pl.when(fits)
    def _():
        fast_accel(cells, partners, mass, box, near_ref, count_ref, slot_ref, table_ref, low_ref, high_ref,
                   inverse_ref, rho_ref, recv_ref, q_ref, v_ref,
                   own_ref, factor_ref, moved_ref, ai_ref, (ax_ref, ay_ref, az_ref, sum_ref))

    @pl.when(jnp.logical_not(fits))
    def _():
        any_accel(partners, mass, unit, shifts, box, near_ref, count_ref, slot_ref, table_ref, rho_ref,
                  recv_ref, q_ref, v_ref, fixed_ref, inverse_ref, list_ref, inverse_list_ref,
                  xi_ref, yi_ref, zi_ref, ci_ref, ai_ref.at[0], ax_ref.at[0], ay_ref.at[0], az_ref.at[0])


def any_accel(partners, mass, unit, shifts, box, near_ref, count_ref, slot_ref, table_ref, rho_ref,
                 recv_ref, q_ref, v_ref,
                 fixed_ref, inverse_ref, list_ref, inverse_list_ref, xi_ref, yi_ref, zi_ref, ci_ref, ai_ref,
                 ax_ref, ay_ref, az_ref):
    cells, particles = table_ref.shape[1], 2 * LANES
    blocks = particles // 8
    i_refs = (xi_ref, yi_ref, zi_ref)
    acc_refs = (ax_ref, ay_ref, az_ref)
    lane = lax.broadcasted_iota(jnp.int32, (8, LANES), 1)
    factor = -math.log2(math.e) * unit * unit
    fixed_point(table_ref, fixed_ref, box)

    def one_cell(cell, carry):
        total = gather_live(
            cell, near_ref, count_ref,
            ((fixed_ref, list_ref), (inverse_ref, inverse_list_ref)), partners,
        )
        for component in range(3):
            store_column(i_refs[component], halves_of(fixed_ref, cell, component))
        h = halves_of(table_ref.at[0], cell, 3)
        store_column(ci_ref, [factor / (part * part) for part in h])
        store_column(ai_ref, halves_of(inverse_ref, cell, 0))
        last = (total - 1) >> 7

        def terms(others, other_inverse, block):
            rows = pl.ds(block * 8, 8)
            parts = offsets(i_refs, rows, others, shifts)
            dx, dy, dz = parts
            w = jnp.exp2((dx * dx + dy * dy + dz * dz) * ci_ref[rows, :])
            return rows, parts, w * (ai_ref[rows, :] + other_inverse)

        others = [spread(list_ref, last, row) for row in range(3)]
        other_inverse = spread(inverse_list_ref, last, 0)
        alive = lane < total - last * LANES
        for block in range(blocks):
            rows, parts, pair = terms(others, other_inverse, block)
            pair = jnp.where(alive, pair, 0.0)
            for acc_ref, part in zip(acc_refs, parts):
                acc_ref[rows, :] = pair * part

        def one_chunk(chunk, inner):
            near = [spread(list_ref, chunk, row) for row in range(3)]
            near_inverse = spread(inverse_list_ref, chunk, 0)
            for block in range(blocks):
                rows, parts, pair = terms(near, near_inverse, block)
                for acc_ref, part in zip(acc_refs, parts):
                    acc_ref[rows, :] += pair * part
            return inner

        lax.fori_loop(0, last, one_chunk, 0)
        scale = [(time_step * 2.0 * mass * unit) / (part * part * part * part * part) for part in h]
        velocity = velocity_rows(recv_ref, slot_ref[cell])
        for component, acc_ref in enumerate(acc_refs):
            sums = row_sums(acc_ref[...])
            for half in range(2):
                kicked = velocity[half][component : component + 1] + sums[half] * scale[half]
                v_ref[cell, 3 * half + component : 3 * half + component + 1] = kicked
                row = slice(4 * half + component, 4 * half + component + 1)
                q_ref[cell, row] = table_ref[0, cell, row] + time_step * kicked
        for half in range(2):
            row = slice(4 * half + 3, 4 * half + 4)
            q_ref[cell, row] = rho_ref[0, cell, half : half + 1]
        return carry

    lax.fori_loop(0, cells, one_cell, 0)


def shards(positions, smoothing, velocity, counts, plan_before, neighbours, plan_after):
    cell_count = positions.shape[0]
    particles = positions.shape[-1]
    partners = neighbours.shape[1] + 1
    sizes = tuple(lax.axis_size(axis) for axis in AXES)
    devices = sizes[0] * sizes[1] * sizes[2]
    box = (float(cell_count // 4 * sizes[0]), float(2 * sizes[1]), float(2 * sizes[2]))
    longest = max(box)
    shifts = tuple(int(round(math.log2(longest / length))) for length in box)
    unit = longest / 2.0**32
    mass = 1.0 / (partners * particles)

    smem = pl.BlockSpec(memory_space=pltpu.SMEM)
    vmem = pl.BlockSpec(memory_space=pltpu.VMEM)
    f32 = lambda *shape: jax.ShapeDtypeStruct(shape, jnp.float32)
    effects = lambda number: pltpu.CompilerParams(has_side_effects=True, collective_id=number)
    sems = lambda *count: [pltpu.SemaphoreType.DMA(count)] * 2
    blocks = (devices, 7, 4, LANES)
    cells8 = pltpu.VMEM((cell_count, 8, LANES), jnp.float32)

    keys, cells = slots_of(jnp.stack([plan_before, plan_after]), cell_count, devices)
    meta = jnp.concatenate([keys.reshape(-1), counts, jnp.zeros_like(counts)])[None, :]
    recv, metas = pl.pallas_call(
        functools.partial(first_exchange_kernel, sizes),
        out_shape=[f32(*blocks), jax.ShapeDtypeStruct((devices, 1, LANES), jnp.int32)],
        in_specs=[smem, vmem, vmem, vmem, vmem],
        out_specs=[vmem] * 2,
        scratch_shapes=[cells8, cells8, pltpu.VMEM(blocks, jnp.float32)] + sems(2),
        compiler_params=effects(0),
        name="first_exchange",
    )(cells[0], meta, jnp.transpose(positions, (1, 0, 2)), smoothing, jnp.transpose(velocity, (1, 0, 2)))

    here = [lax.axis_index(axis) for axis in AXES]
    place = flat(here, sizes) * cell_count + jnp.arange(cell_count, dtype=jnp.int32)
    metas = metas[:, 0, :]
    keys_before, keys_after = metas[:, 0:cell_count], metas[:, cell_count : 2 * cell_count]
    all_counts = metas[:, 2 * cell_count : 3 * cell_count]
    source = 2 * jnp.arange(devices, dtype=jnp.int32)[:, None]

    def pick(keys, values):
        hit = (keys >> 1)[None] == place[:, None, None]
        return jnp.sum(jnp.where(hit, values[None], 0), axis=(1, 2))

    slot_count = pick(keys_before, (keys_before & 1) + source + all_counts * (2 * devices))
    slot_before, own_count = slot_count % (2 * devices), slot_count // (2 * devices)
    slot_after = pick(keys_after, (keys_after & 1) + source)
    near = near_table(neighbours, cell_count)

    table, table_count = pl.pallas_call(
        functools.partial(cell_halo_kernel, sizes),
        out_shape=[f32(7, cell_count, 8, LANES), jax.ShapeDtypeStruct((7, 1, LANES), jnp.int32)],
        in_specs=[smem, vmem, vmem],
        out_specs=[vmem, vmem],
        scratch_shapes=sems(2, 6),
        compiler_params=effects(1),
        name="cell_halo",
    )(slot_before, jnp.pad(own_count, (0, LANES - cell_count))[None, :], recv)
    table_count = table_count[:, 0, :cell_count].reshape(-1)

    chunks = partners * particles // LANES + 1
    square = (particles, LANES)
    columns = [pltpu.VMEM(square, jnp.int32)] * 3
    extent = [pltpu.VMEM((7 * cell_count, 8, LANES), jnp.float32)] * 2 + [
        pltpu.VMEM((2, particles, 32), jnp.bfloat16),
        pltpu.VMEM((2, partners, 32, particles), jnp.bfloat16),
    ]
    fixed = pltpu.VMEM((7 * cell_count, 8, LANES), jnp.int32)
    rho, fits = pl.pallas_call(
        functools.partial(density_kernel, partners, mass, unit, shifts, box),
        out_shape=[f32(cell_count, 2, LANES), jax.ShapeDtypeStruct((1,), jnp.int32)],
        in_specs=[smem, smem, vmem],
        out_specs=[vmem, smem],
        scratch_shapes=extent + [fixed, pltpu.VMEM((chunks, 4, LANES), jnp.int32)] + columns
        + [pltpu.VMEM(square, jnp.float32), pltpu.VMEM((2,) + square, jnp.float32)],
        name="density",
    )(near, table_count, table)

    table_rho = pl.pallas_call(
        functools.partial(rho_halo_kernel, sizes),
        out_shape=f32(7, cell_count, 2, LANES),
        in_specs=[vmem],
        out_specs=vmem,
        scratch_shapes=sems(1, 6),
        compiler_params=effects(2),
        name="rho_halo",
    )(rho)

    out_q, out_v = pl.pallas_call(
        functools.partial(accel_kernel, partners, mass, unit, shifts, box),
        out_shape=[f32(cell_count, 8, LANES)] * 2,
        in_specs=[smem, smem, smem, smem, vmem, vmem, vmem],
        out_specs=[vmem, vmem],
        scratch_shapes=extent
        + [
            pltpu.VMEM((2, partners, 8, LANES), jnp.float32),
            pltpu.VMEM((2,) + square, jnp.float32),
            fixed,
            pltpu.VMEM((7 * cell_count, 2, LANES), jnp.float32),
            pltpu.VMEM((chunks, 4, LANES), jnp.int32),
            pltpu.VMEM((chunks, 1, LANES), jnp.float32),
        ]
        + columns
        + [pltpu.VMEM(square, jnp.float32)]
        + [pltpu.VMEM((2,) + square, jnp.float32)] * 4,
        name="accel",
    )(near, table_count, slot_before, fits, table, table_rho, recv)

    last = pl.pallas_call(
        functools.partial(last_exchange_kernel, sizes),
        out_shape=f32(*blocks),
        in_specs=[smem, vmem, vmem],
        out_specs=vmem,
        scratch_shapes=[pltpu.VMEM(blocks, jnp.float32)] + sems(1),
        compiler_params=effects(3),
        name="last_exchange",
    )(cells[1], out_q, out_v)
    new_pos, new_vel, new_rho = pl.pallas_call(
        unpack_kernel,
        out_shape=[f32(3, cell_count, particles)] * 2 + [f32(cell_count, particles)],
        in_specs=[smem, vmem],
        out_specs=[vmem] * 3,
        name="unpack",
    )(slot_after, last)
    return jnp.transpose(new_pos, (1, 0, 2)), jnp.transpose(new_vel, (1, 0, 2)), new_rho


def solution(mesh):
    in_specs = (
        P(("gx", "gy", "gz"), None, None),
        P(("gx", "gy", "gz"), None),
        P(("gx", "gy", "gz"), None, None),
        P(("gx", "gy", "gz")),
        P(("gx", "gy", "gz")),
        P(("gx", "gy", "gz"), None),
        P(("gx", "gy", "gz")),
    )
    out_specs = (
        P(("gx", "gy", "gz"), None, None),
        P(("gx", "gy", "gz"), None, None),
        P(("gx", "gy", "gz"), None),
    )
    return jax.shard_map(shards, mesh=mesh, in_specs=in_specs, out_specs=out_specs, check_vma=False)
```

```python
import functools
import math

import jax
import jax.numpy as jnp
from jax import lax
from jax.experimental import pallas as pl
from jax.experimental.pallas import tpu as pltpu
from jax.sharding import PartitionSpec as P

time_step = 0.1
LANES = 128
AXES = ("gx", "gy", "gz")
MESH = pl.DeviceIdType.MESH
VMEM = 24 * 2**20

def neighbour_steps():
    return [(axis, step) for axis in AXES for step in (-1, 1)]


def slots_of(plans, cell_count, devices):
    target = plans // cell_count
    ladder = jnp.arange(cell_count, dtype=jnp.int32)
    earlier = (target[:, :, None] == target[:, None, :]) & (ladder[None, :] < ladder[:, None])
    rank = jnp.sum(earlier.astype(jnp.int32), axis=2)
    slot = target * 2 + rank
    every = jnp.arange(devices * 2, dtype=jnp.int32)
    hit = slot[:, None, :] == every[None, :, None]
    return rank, jnp.sum(jnp.where(hit, ladder, 0), axis=2)


def near_table(neighbours, cell_count):
    sizes = {axis: lax.axis_size(axis) for axis in AXES}
    here = {axis: lax.axis_index(axis) for axis in AXES}
    owner = neighbours // cell_count
    block = jnp.zeros_like(owner)
    for number, (axis, step) in enumerate(neighbour_steps(), 1):
        there = dict(here)
        there[axis] = (here[axis] + step) % sizes[axis]
        device = (there["gx"] * sizes["gy"] + there["gy"]) * sizes["gz"] + there["gz"]
        block = jnp.where(owner == device, number, block)
    near = block * cell_count + neighbours % cell_count
    own = jnp.arange(cell_count, dtype=jnp.int32)[:, None]
    return jnp.concatenate([own, near], axis=1).reshape(-1)


def peer_offsets(sizes):
    count_x, count_y, count_z = sizes
    steps = [(x, y, z) for x in range(count_x) for y in range(count_y) for z in range(count_z)][1:]

    def hops(step):
        x, y, z = step
        chips = count_z // 2
        return min(x, count_x - x) + min(y, count_y - y) + min(z // 2, chips - z // 2)

    return sorted(steps, key=lambda step: -hops(step))


def shifted(here, step, sizes):
    return tuple(lax.rem(h + d, n) if d else h for h, d, n in zip(here, step, sizes))


def flat(place, sizes):
    return (place[0] * sizes[1] + place[1]) * sizes[2] + place[2]


def greet(peers):
    barrier = pltpu.get_barrier_semaphore()
    for peer in peers:
        pl.semaphore_signal(barrier, inc=1, device_id=peer, device_id_type=MESH)
    return barrier, len(peers)


def exchange(sizes, fill, pairs, send_sems, recv_sems):
    here = [lax.axis_index(axis) for axis in AXES]
    me = flat(here, sizes)
    peers = [shifted(here, step, sizes) for step in peer_offsets(sizes)]
    barrier, signals = greet(peers)
    fill()
    pl.semaphore_wait(barrier, signals)
    for number, (source, target, whole) in enumerate(pairs):
        for there in peers:
            pltpu.make_async_remote_copy(
                src_ref=source if whole else source.at[flat(there, sizes)],
                dst_ref=target.at[me],
                send_sem=send_sems.at[number],
                recv_sem=recv_sems.at[number],
                device_id=there,
                device_id_type=MESH,
            ).start()
    for source, target, whole in pairs:
        target[me] = source[...] if whole else source[me]
    for number, (source, target, whole) in enumerate(pairs):
        most = target.at[pl.ds(0, signals)]
        arrived = pltpu.make_async_remote_copy(
            src_ref=most, dst_ref=most, send_sem=send_sems.at[number],
            recv_sem=recv_sems.at[number], device_id=tuple(here), device_id_type=MESH,
        )
        arrived.wait_send()
        arrived.wait_recv()


def fill_blocks(cell_ref, q_ref, v_ref, send_ref):
    def one(d, carry):
        first, second = cell_ref[2 * d], cell_ref[2 * d + 1]
        for number, cell in enumerate((first, second)):
            rows = q_ref[cell]
            send_ref[d, 2 * number] = rows[0:4]
            send_ref[d, 2 * number + 1] = rows[4:8]
        low, high = v_ref[first], v_ref[second]
        send_ref[d, 4] = low[0:4]
        send_ref[d, 5, 0:2] = low[4:6]
        send_ref[d, 5, 2:4] = high[0:2]
        send_ref[d, 6] = high[2:6]
        return carry

    lax.fori_loop(0, send_ref.shape[0], one, 0)


def cell_rows(recv_ref, slot):
    block, odd = slot >> 1, slot & 1
    return [recv_ref[block, 2 * odd + half] for half in range(2)]


def velocity_rows(recv_ref, slot):
    block, odd = slot >> 1, (slot & 1) == 1
    first, middle, last = recv_ref[block, 4], recv_ref[block, 5], recv_ref[block, 6]
    even_rows = jnp.concatenate([first, middle[0:2]], axis=0)
    odd_rows = jnp.concatenate([middle[2:4], last], axis=0)
    rows = jnp.where(odd, odd_rows, even_rows)
    return rows[0:3], rows[3:6]


def first_exchange_kernel(sizes, cell_ref, meta_ref, pos_ref, h_ref, vel_ref, recv_ref, metas_ref,
                          q_ref, v_ref, send_ref, send_sems, recv_sems):
    def fill():
        for cell in range(pos_ref.shape[1]):
            for half in range(2):
                lanes = slice(half * LANES, (half + 1) * LANES)
                for component in range(3):
                    q_ref[cell, 4 * half + component] = pos_ref[component, cell, lanes]
                    v_ref[cell, 3 * half + component] = vel_ref[component, cell, lanes]
                q_ref[cell, 4 * half + 3] = h_ref[cell, lanes]
        fill_blocks(cell_ref, q_ref, v_ref, send_ref)

    pairs = ((meta_ref, metas_ref, True), (send_ref, recv_ref, False))
    exchange(sizes, fill, pairs, send_sems, recv_sems)


def last_exchange_kernel(sizes, cell_ref, q_ref, v_ref, recv_ref, send_ref, send_sems, recv_sems):
    def fill():
        fill_blocks(cell_ref, q_ref, v_ref, send_ref)

    exchange(sizes, fill, ((send_ref, recv_ref, False),), send_sems, recv_sems)


def halo(sizes, fill, pairs, send_sems, recv_sems):
    here = [lax.axis_index(axis) for axis in AXES]
    peers = []
    for axis, step in neighbour_steps():
        there = [0] * 3
        there[AXES.index(axis)] = (-step) % sizes[AXES.index(axis)]
        peers.append(shifted(here, there, sizes))
    barrier, signals = greet(peers)
    fill()
    pl.semaphore_wait(barrier, signals)
    copies = []
    for which, (source, target) in enumerate(pairs):
        for number, there in enumerate(peers):
            copies.append(
                pltpu.make_async_remote_copy(
                    src_ref=source, dst_ref=target.at[number + 1],
                    send_sem=send_sems.at[which, number], recv_sem=recv_sems.at[which, number],
                    device_id=there, device_id_type=MESH,
                )
            )
            copies[-1].start()
    for copy in copies:
        copy.wait()


def cell_halo_kernel(sizes, slot_ref, count_ref, recv_ref, table_ref, counts_ref, send_sems, recv_sems):
    def fill():
        counts_ref[0] = count_ref[...]
        for place in range(table_ref.shape[1]):
            low, high = cell_rows(recv_ref, slot_ref[place])
            table_ref[0, place, 0:4] = low
            table_ref[0, place, 4:8] = high

    pairs = ((count_ref, counts_ref), (table_ref.at[0], table_ref))
    halo(sizes, fill, pairs, send_sems, recv_sems)


def rho_halo_kernel(sizes, rho_ref, table_ref, send_sems, recv_sems):
    def fill():
        table_ref[0] = rho_ref[...]

    halo(sizes, fill, ((rho_ref, table_ref),), send_sems, recv_sems)


def unpack_kernel(slot_ref, recv_ref, pos_ref, vel_ref, rho_ref):
    for place in range(pos_ref.shape[1]):
        slot = slot_ref[place]
        rows = cell_rows(recv_ref, slot)
        velocity = velocity_rows(recv_ref, slot)
        for half in range(2):
            lanes = slice(half * LANES, (half + 1) * LANES)
            for component in range(3):
                pos_ref[component, place, lanes] = rows[half][component]
                vel_ref[component, place, lanes] = velocity[half][component]
            rho_ref[place, lanes] = rows[half][3]


def fixed_point(table_ref, fixed_ref, box):
    row = lax.broadcasted_iota(jnp.int32, (8, LANES), 0) & 3
    scale = jnp.full((8, LANES), 2.0**32 / box[2], jnp.float32)
    scale = jnp.where(row == 0, 2.0**32 / box[0], jnp.where(row == 1, 2.0**32 / box[1], scale))
    scale = jnp.where(row == 3, 1.0, scale)
    cells = table_ref.shape[1]

    def one(cell, carry):
        for block in range(table_ref.shape[0]):
            scaled = table_ref[block, cell] * scale
            scaled = jnp.where(scaled >= 2.0**31, scaled - 2.0**32, scaled)
            fixed_ref[block * cells + cell] = scaled.astype(jnp.int32)
        return carry

    lax.fori_loop(0, cells, one, 0)


def gather_live(cell, near_ref, count_ref, pairs, partners):
    fill = jnp.int32(0)
    for partner in range(partners):
        b = near_ref[cell * partners + partner]
        live = count_ref[b]
        shift = fill & (LANES - 1)
        chunk = fill >> 7
        for table_ref, list_ref in pairs:
            rows = list_ref.shape[1]
            kept = lax.broadcasted_iota(jnp.int32, (rows, LANES), 1) < shift
            rolled = pltpu.roll(table_ref[b], shift, 1)
            first, second = rolled[0:rows], rolled[rows : 2 * rows]
            list_ref[chunk] = jnp.where(kept, list_ref[chunk], first)
            list_ref[chunk + 1] = jnp.where(kept, first, second)
            list_ref[chunk + 2] = second
        fill = fill + live
    return fill


def store_column(ref, halves):
    for half, part in enumerate(halves):
        ref[half * LANES : (half + 1) * LANES, :] = jnp.broadcast_to(part, (LANES, LANES)).T


def halves_of(ref, cell, row):
    step = ref.shape[1] // 2
    return [ref[cell, row + half * step : row + half * step + 1, :] for half in range(2)]


def row_sums(acc):
    ones = jnp.ones((8, LANES), jnp.float32)
    sums = lax.dot_general(
        ones, acc, (((1,), (1,)), ((), ())),
        precision=lax.Precision.HIGHEST, preferred_element_type=jnp.float32,
    )
    return [sums[0:1, 0:LANES], sums[0:1, LANES : 2 * LANES]]


def spread(list_ref, chunk, row):
    return jnp.broadcast_to(list_ref[chunk, row : row + 1, :], (8, LANES))


def offsets(i_refs, rows, others, shifts):
    parts = []
    for ref, other, shift in zip(i_refs, others, shifts):
        diff = ref[rows, :] - other
        if shift:
            diff = diff >> shift
        parts.append(diff.astype(jnp.float32))
    return parts


def by_row(values):
    row = lax.broadcasted_iota(jnp.int32, (8, LANES), 0) & 3
    out = jnp.full((8, LANES), values[3], jnp.float32)
    for number in range(3):
        out = jnp.where(row == number, jnp.float32(values[number]), out)
    return out


def bounds(table_ref, low_ref, high_ref):
    blocks, cells = table_ref.shape[0], table_ref.shape[1]
    together = 4

    def some(step, carry):
        which = [(block, step * together + n) for n in range(together) for block in range(blocks)]
        lows = [jnp.min(table_ref[block, cell], axis=1, keepdims=True) for block, cell in which]
        highs = [jnp.max(table_ref[block, cell], axis=1, keepdims=True) for block, cell in which]
        for (block, cell), low, high in zip(which, lows, highs):
            low = jnp.broadcast_to(low, (8, LANES))
            high = jnp.broadcast_to(high, (8, LANES))
            low_ref[block * cells + cell] = jnp.minimum(low, pltpu.roll(low, 4, 0))
            high_ref[block * cells + cell] = jnp.maximum(high, pltpu.roll(high, 4, 0))
        return carry

    lax.fori_loop(0, cells // together, some, 0)


def middle(low, high):
    return jnp.floor(low + high + 0.5) * 0.5


def image(low_a, high_a, low_b, high_b, lengths):
    return jnp.floor((low_a - high_b) / lengths + 0.5) * lengths


def sum_of_xyz(rows):
    return pltpu.roll(rows, 1, 0) + pltpu.roll(rows, 2, 0) + pltpu.roll(rows, 3, 0)


def one_image(cells, partners, box, near_ref, low_ref, high_ref):
    lengths = by_row(box + (1.0,))
    half = lengths * (0.5 * (1.0 - 2.0**-16))
    coordinate = (lax.broadcasted_iota(jnp.int32, (8, LANES), 0) & 3) < 3
    limit = 256.0 / math.log2(math.e)

    def one(cell, good):
        low_a, high_a = low_ref[cell], high_ref[cell]
        origin = middle(low_a, high_a)
        for partner in range(partners):
            b = near_ref[cell * partners + partner]
            low_b, high_b = low_ref[b], high_ref[b]
            shift = image(low_a, high_a, low_b, high_b, lengths)
            fits = (high_a - low_b - shift < half) & (low_a - high_b - shift > -half)
            moved = shift - origin
            reach = jnp.maximum(jnp.abs(low_b + moved), jnp.abs(high_b + moved))
            small = sum_of_xyz(reach * reach) <= limit * low_a * low_a
            fine = jnp.where(coordinate, jnp.where(fits, 1.0, 0.0), jnp.where(small, 1.0, 0.0))
            good = jnp.minimum(good, fine)
        return good

    good = lax.fori_loop(0, cells, one, jnp.ones((8, LANES), jnp.float32))
    return jnp.min(good) > 0.5


def three_parts(value):
    first = value.astype(jnp.bfloat16).astype(jnp.float32)
    value = value - first
    second = value.astype(jnp.bfloat16).astype(jnp.float32)
    return first, second, value - second


def joined(upper, lower, half):
    top = lax.broadcasted_iota(jnp.int32, (8, LANES), 0) < 4
    if half == 0:
        return jnp.where(top, upper, pltpu.roll(lower, 4, 0))
    return jnp.where(top, pltpu.roll(upper, 4, 0), lower)


def own_factors(rows, origin, own_ref):
    row = lax.broadcasted_iota(jnp.int32, (8, LANES), 0)
    centred = rows - origin
    c = -math.log2(math.e) / (rows * rows)
    c = jnp.where(row < 4, jnp.broadcast_to(c[3:4], (8, LANES)), jnp.broadcast_to(c[7:8], (8, LANES)))
    p1, p2, p3 = three_parts(jnp.where((row & 3) == 3, c, -2.0 * c * centred))
    squares = three_parts(c * sum_of_xyz(centred * centred))
    for half in range(2):
        last = jnp.where(row == 3, 1.0, 0.0)
        for number, part in enumerate(squares):
            moved = pltpu.roll(part, (number + 5 - 4 * half) % 8, 0)
            last = jnp.where(row == number, moved, last)
        groups = [joined(p1, p1, half), joined(p1, p2, half), joined(p2, p3, half), last]
        block = jnp.concatenate(groups, axis=0).T
        own_ref[half * LANES : (half + 1) * LANES, :] = block.astype(jnp.bfloat16)
    return centred


def near_factors(moved, live, near_ref, partner):
    row = lax.broadcasted_iota(jnp.int32, (8, LANES), 0)
    lane = lax.broadcasted_iota(jnp.int32, (8, LANES), 1)
    q1, q2, q3 = three_parts(jnp.where((row & 3) == 3, sum_of_xyz(moved * moved), moved))
    for half in range(2):
        alive = lane + half * LANES < live
        last = jnp.where(row < 3, 1.0, jnp.where((row > 3) | alive, 0.0, -1e30))
        groups = [joined(q1, q2, half), joined(q3, q1, half), joined(q2, q1, half), last]
        block = jnp.concatenate(groups, axis=0)
        near_ref[partner, :, half * LANES : (half + 1) * LANES] = block.astype(jnp.bfloat16)


def exponents(own_ref, near_ref, partner, rows):
    return jnp.dot(own_ref[rows, :], near_ref[partner], preferred_element_type=jnp.float32)


def lane_sums(acc):
    halves = []
    for half in range(2):
        part = acc[half * LANES : (half + 1) * LANES, :].T
        eight = part[0:8]
        for row in range(8, LANES, 8):
            eight = eight + part[row : row + 8]
        halves.append(jnp.sum(eight, axis=0, keepdims=True))
    return halves


def fast_density(cells, partners, mass, box, near_ref, count_ref, table_ref, low_ref, high_ref, rho_ref,
                 own_ref, factor_ref, acc_ref):
    lengths = by_row(box + (1.0,))
    step = 64

    def one_cell(cell, own_ref, factor_ref, acc_ref):
        low_a, high_a = low_ref[cell], high_ref[cell]
        origin = middle(low_a, high_a)
        own_factors(table_ref[0, cell], origin, own_ref)
        for partner in range(partners):
            b = near_ref[cell * partners + partner]
            shift = image(low_a, high_a, low_ref[b], high_ref[b], lengths)
            moved = table_ref[b >> 5, b & 31] + (shift - origin)
            near_factors(moved, count_ref[b], factor_ref, partner)
        for block in range(2 * LANES // step):
            rows = slice(block * step, (block + 1) * step)
            acc = None
            for partner in range(partners):
                w = jnp.exp2(exponents(own_ref, factor_ref, partner, rows))
                both = w[:, 0:LANES] + w[:, LANES : 2 * LANES]
                acc = both if acc is None else acc + both
            acc_ref[rows, :] = acc
        h = halves_of(table_ref.at[0], cell, 3)
        for half, (part, total) in enumerate(zip(h, lane_sums(acc_ref[...]))):
            rho_ref[cell, half : half + 1] = mass * (1.0 + total) / (part * part * part)

    def two_cells(pair, carry):
        for number in range(2):
            one_cell(2 * pair + number, own_ref.at[number], factor_ref.at[number], acc_ref.at[number])
        return carry

    lax.fori_loop(0, cells // 2, two_cells, 0)


def fast_accel(cells, partners, mass, box, near_ref, count_ref, slot_ref, table_ref, low_ref, high_ref,
               inverse_ref, rho_ref, recv_ref, q_ref, v_ref,
               own_ref, factor_ref, moved_ref, ai_ref, acc_refs):
    lengths = by_row(box + (1.0,))
    step = 32

    def one_cell(cell, own_ref, factor_ref, moved_ref, ai_ref, acc_refs):
        low_a, high_a = low_ref[cell], high_ref[cell]
        origin = middle(low_a, high_a)
        centred = own_factors(table_ref[0, cell], origin, own_ref)
        store_column(ai_ref, halves_of(inverse_ref, cell, 0))
        for partner in range(partners):
            b = near_ref[cell * partners + partner]
            shift = image(low_a, high_a, low_ref[b], high_ref[b], lengths)
            moved = table_ref[b >> 5, b & 31] + (shift - origin)
            near_factors(moved, count_ref[b], factor_ref, partner)
            moved_ref[partner] = moved
            for half in range(2):
                moved_ref[partner, 4 * half + 3 : 4 * half + 4] = inverse_ref[b, half : half + 1]
        for block in range(2 * LANES // step):
            rows = slice(block * step, (block + 1) * step)
            own_inverse = ai_ref[rows, :]
            accs = [None] * 4
            for partner in range(partners):
                w = jnp.exp2(exponents(own_ref, factor_ref, partner, rows))
                for half in range(2):
                    near = [
                        jnp.broadcast_to(
                            moved_ref[partner, 4 * half + row : 4 * half + row + 1, :], (step, LANES)
                        )
                        for row in range(4)
                    ]
                    pair = w[:, half * LANES : (half + 1) * LANES] * (own_inverse + near[3])
                    terms = [pair * near[0], pair * near[1], pair * near[2], pair]
                    accs = [t if a is None else a + t for a, t in zip(accs, terms)]
            for acc_ref, acc in zip(acc_refs, accs):
                acc_ref[rows, :] = acc
        h = halves_of(table_ref.at[0], cell, 3)
        scale = [(time_step * 2.0 * mass) / (part * part * part * part * part) for part in h]
        velocity = velocity_rows(recv_ref, slot_ref[cell])
        whole = lane_sums(acc_refs[3][...])
        for component in range(3):
            sums = lane_sums(acc_refs[component][...])
            for half in range(2):
                row = slice(4 * half + component, 4 * half + component + 1)
                force = centred[row] * whole[half] - sums[half]
                kicked = velocity[half][component : component + 1] + force * scale[half]
                v_ref[cell, 3 * half + component : 3 * half + component + 1] = kicked
                q_ref[cell, row] = table_ref[0, cell, row] + time_step * kicked
        for half in range(2):
            row = slice(4 * half + 3, 4 * half + 4)
            q_ref[cell, row] = rho_ref[0, cell, half : half + 1]

    def two_cells(pair, carry):
        for number in range(2):
            one_cell(2 * pair + number, own_ref.at[number], factor_ref.at[number], moved_ref.at[number], ai_ref.at[number], [ref.at[number] for ref in acc_refs])
        return carry

    lax.fori_loop(0, cells // 2, two_cells, 0)


def density_kernel(partners, mass, unit, shifts, box, near_ref, count_ref, table_ref, rho_ref, fits_ref,
                   low_ref, high_ref, own_ref, factor_ref,
                   fixed_ref, list_ref, xi_ref, yi_ref, zi_ref, ci_ref, acc_ref):
    cells = table_ref.shape[1]
    bounds(table_ref, low_ref, high_ref)
    fits = one_image(cells, partners, box, near_ref, low_ref, high_ref)

    fits_ref[0] = jnp.where(fits, 1, 0)

    @pl.when(fits)
    def _():
        fast_density(cells, partners, mass, box, near_ref, count_ref, table_ref, low_ref, high_ref,
                     rho_ref, own_ref, factor_ref, acc_ref)

    @pl.when(jnp.logical_not(fits))
    def _():
        any_density(partners, mass, unit, shifts, box, near_ref, count_ref, table_ref, rho_ref,
                    fixed_ref, list_ref, xi_ref, yi_ref, zi_ref, ci_ref, acc_ref.at[0])


def any_density(partners, mass, unit, shifts, box, near_ref, count_ref, table_ref, rho_ref,
                fixed_ref, list_ref, xi_ref, yi_ref, zi_ref, ci_ref, acc_ref):
    cells, particles = table_ref.shape[1], 2 * LANES
    blocks = particles // 8
    i_refs = (xi_ref, yi_ref, zi_ref)
    lane = lax.broadcasted_iota(jnp.int32, (8, LANES), 1)
    factor = -math.log2(math.e) * unit * unit
    fixed_point(table_ref, fixed_ref, box)

    def one_cell(cell, carry):
        total = gather_live(cell, near_ref, count_ref, ((fixed_ref, list_ref),), partners)
        for component in range(3):
            store_column(i_refs[component], halves_of(fixed_ref, cell, component))
        h = halves_of(table_ref.at[0], cell, 3)
        store_column(ci_ref, [factor / (part * part) for part in h])
        last = (total - 1) >> 7

        def weights(chunk, others, block):
            rows = pl.ds(block * 8, 8)
            dx, dy, dz = offsets(i_refs, rows, others, shifts)
            return rows, jnp.exp2((dx * dx + dy * dy + dz * dz) * ci_ref[rows, :])

        others = [spread(list_ref, last, row) for row in range(3)]
        alive = lane < total - last * LANES
        for block in range(blocks):
            rows, w = weights(last, others, block)
            acc_ref[rows, :] = jnp.where(alive, w, 0.0)

        def one_chunk(chunk, inner):
            near = [spread(list_ref, chunk, row) for row in range(3)]
            for block in range(blocks):
                rows, w = weights(chunk, near, block)
                acc_ref[rows, :] += w
            return inner

        lax.fori_loop(0, last, one_chunk, 0)
        for half, (part, total_half) in enumerate(zip(h, row_sums(acc_ref[...]))):
            rho_ref[cell, half : half + 1] = mass * (1.0 + total_half) / (part * part * part)
        return carry

    lax.fori_loop(0, cells, one_cell, 0)


def accel_kernel(partners, mass, unit, shifts, box, near_ref, count_ref, slot_ref, fits_ref, table_ref, rho_ref,
                 recv_ref, q_ref, v_ref,
                 low_ref, high_ref, own_ref, factor_ref, moved_ref, sum_ref,
                 fixed_ref, inverse_ref, list_ref, inverse_list_ref, xi_ref, yi_ref, zi_ref, ci_ref, ai_ref,
                 ax_ref, ay_ref, az_ref):
    cells = table_ref.shape[1]
    bounds(table_ref, low_ref, high_ref)
    fits = fits_ref[0] > 0

    def invert(cell, carry):
        for block in range(rho_ref.shape[0]):
            inverse_ref[block * cells + cell] = 1.0 / rho_ref[block, cell]
        return carry

    lax.fori_loop(0, cells, invert, 0)

    @pl.when(fits)
    def _():
        fast_accel(cells, partners, mass, box, near_ref, count_ref, slot_ref, table_ref, low_ref, high_ref,
                   inverse_ref, rho_ref, recv_ref, q_ref, v_ref,
                   own_ref, factor_ref, moved_ref, ai_ref, (ax_ref, ay_ref, az_ref, sum_ref))

    @pl.when(jnp.logical_not(fits))
    def _():
        any_accel(partners, mass, unit, shifts, box, near_ref, count_ref, slot_ref, table_ref, rho_ref,
                  recv_ref, q_ref, v_ref, fixed_ref, inverse_ref, list_ref, inverse_list_ref,
                  xi_ref, yi_ref, zi_ref, ci_ref, ai_ref.at[0], ax_ref.at[0], ay_ref.at[0], az_ref.at[0])


def any_accel(partners, mass, unit, shifts, box, near_ref, count_ref, slot_ref, table_ref, rho_ref,
                 recv_ref, q_ref, v_ref,
                 fixed_ref, inverse_ref, list_ref, inverse_list_ref, xi_ref, yi_ref, zi_ref, ci_ref, ai_ref,
                 ax_ref, ay_ref, az_ref):
    cells, particles = table_ref.shape[1], 2 * LANES
    blocks = particles // 8
    i_refs = (xi_ref, yi_ref, zi_ref)
    acc_refs = (ax_ref, ay_ref, az_ref)
    lane = lax.broadcasted_iota(jnp.int32, (8, LANES), 1)
    factor = -math.log2(math.e) * unit * unit
    fixed_point(table_ref, fixed_ref, box)

    def one_cell(cell, carry):
        total = gather_live(
            cell, near_ref, count_ref,
            ((fixed_ref, list_ref), (inverse_ref, inverse_list_ref)), partners,
        )
        for component in range(3):
            store_column(i_refs[component], halves_of(fixed_ref, cell, component))
        h = halves_of(table_ref.at[0], cell, 3)
        store_column(ci_ref, [factor / (part * part) for part in h])
        store_column(ai_ref, halves_of(inverse_ref, cell, 0))
        last = (total - 1) >> 7

        def terms(others, other_inverse, block):
            rows = pl.ds(block * 8, 8)
            parts = offsets(i_refs, rows, others, shifts)
            dx, dy, dz = parts
            w = jnp.exp2((dx * dx + dy * dy + dz * dz) * ci_ref[rows, :])
            return rows, parts, w * (ai_ref[rows, :] + other_inverse)

        others = [spread(list_ref, last, row) for row in range(3)]
        other_inverse = spread(inverse_list_ref, last, 0)
        alive = lane < total - last * LANES
        for block in range(blocks):
            rows, parts, pair = terms(others, other_inverse, block)
            pair = jnp.where(alive, pair, 0.0)
            for acc_ref, part in zip(acc_refs, parts):
                acc_ref[rows, :] = pair * part

        def one_chunk(chunk, inner):
            near = [spread(list_ref, chunk, row) for row in range(3)]
            near_inverse = spread(inverse_list_ref, chunk, 0)
            for block in range(blocks):
                rows, parts, pair = terms(near, near_inverse, block)
                for acc_ref, part in zip(acc_refs, parts):
                    acc_ref[rows, :] += pair * part
            return inner

        lax.fori_loop(0, last, one_chunk, 0)
        scale = [(time_step * 2.0 * mass * unit) / (part * part * part * part * part) for part in h]
        velocity = velocity_rows(recv_ref, slot_ref[cell])
        for component, acc_ref in enumerate(acc_refs):
            sums = row_sums(acc_ref[...])
            for half in range(2):
                kicked = velocity[half][component : component + 1] + sums[half] * scale[half]
                v_ref[cell, 3 * half + component : 3 * half + component + 1] = kicked
                row = slice(4 * half + component, 4 * half + component + 1)
                q_ref[cell, row] = table_ref[0, cell, row] + time_step * kicked
        for half in range(2):
            row = slice(4 * half + 3, 4 * half + 4)
            q_ref[cell, row] = rho_ref[0, cell, half : half + 1]
        return carry

    lax.fori_loop(0, cells, one_cell, 0)


def shards(positions, smoothing, velocity, counts, plan_before, neighbours, plan_after):
    cell_count = positions.shape[0]
    particles = positions.shape[-1]
    partners = neighbours.shape[1] + 1
    sizes = tuple(lax.axis_size(axis) for axis in AXES)
    devices = sizes[0] * sizes[1] * sizes[2]
    box = (float(cell_count // 4 * sizes[0]), float(2 * sizes[1]), float(2 * sizes[2]))
    longest = max(box)
    shifts = tuple(int(round(math.log2(longest / length))) for length in box)
    unit = longest / 2.0**32
    mass = 1.0 / (partners * particles)

    smem = pl.BlockSpec(memory_space=pltpu.SMEM)
    vmem = pl.BlockSpec(memory_space=pltpu.VMEM)
    f32 = lambda *shape: jax.ShapeDtypeStruct(shape, jnp.float32)
    effects = lambda number: pltpu.CompilerParams(has_side_effects=True, collective_id=number, vmem_limit_bytes=VMEM)
    sems = lambda *count: [pltpu.SemaphoreType.DMA(count)] * 2
    blocks = (devices, 7, 4, LANES)
    cells8 = pltpu.VMEM((cell_count, 8, LANES), jnp.float32)

    ranks, cells = slots_of(jnp.stack([plan_before, plan_after]), cell_count, devices)
    meta = jnp.concatenate([plan_before, plan_after, ranks.reshape(-1), counts, jnp.zeros((96,), jnp.int32)])[None, :]
    recv, metas = pl.pallas_call(
        functools.partial(first_exchange_kernel, sizes),
        out_shape=[f32(*blocks), jax.ShapeDtypeStruct((devices, 1, 2 * LANES), jnp.int32)],
        in_specs=[smem, vmem, vmem, vmem, vmem],
        out_specs=[vmem] * 2,
        scratch_shapes=[cells8, cells8, pltpu.VMEM(blocks, jnp.float32)] + sems(2),
        compiler_params=effects(0),
        name="first_exchange",
    )(cells[0], meta, jnp.transpose(positions, (1, 0, 2)), smoothing, jnp.transpose(velocity, (1, 0, 2)))

    here = [lax.axis_index(axis) for axis in AXES]
    place = flat(here, sizes) * cell_count + jnp.arange(cell_count, dtype=jnp.int32)
    metas = metas[:, 0, :]
    fields = [metas[:, n * cell_count : (n + 1) * cell_count] for n in range(5)]
    placed_before, placed_after, rank_before, rank_after, all_counts = fields
    source = 2 * jnp.arange(devices, dtype=jnp.int32)[:, None]

    def pick(placed, values):
        hit = placed[None] == place[:, None, None]
        return jnp.sum(jnp.where(hit, values[None], 0), axis=(1, 2))

    slot_count = pick(placed_before, rank_before + source + all_counts * (2 * devices))
    slot_before, own_count = slot_count % (2 * devices), slot_count // (2 * devices)
    slot_after = pick(placed_after, rank_after + source)
    near = near_table(neighbours, cell_count)

    table, table_count = pl.pallas_call(
        functools.partial(cell_halo_kernel, sizes),
        out_shape=[f32(7, cell_count, 8, LANES), jax.ShapeDtypeStruct((7, 1, LANES), jnp.int32)],
        in_specs=[smem, vmem, vmem],
        out_specs=[vmem, vmem],
        scratch_shapes=sems(2, 6),
        compiler_params=effects(1),
        name="cell_halo",
    )(slot_before, jnp.pad(own_count, (0, LANES - cell_count))[None, :], recv)
    table_count = table_count[:, 0, :cell_count].reshape(-1)

    chunks = partners * particles // LANES + 1
    square = (particles, LANES)
    columns = [pltpu.VMEM(square, jnp.int32)] * 3
    extent = [pltpu.VMEM((7 * cell_count, 8, LANES), jnp.float32)] * 2 + [
        pltpu.VMEM((2, particles, 32), jnp.bfloat16),
        pltpu.VMEM((2, partners, 32, particles), jnp.bfloat16),
    ]
    fixed = pltpu.VMEM((7 * cell_count, 8, LANES), jnp.int32)
    rho, fits = pl.pallas_call(
        functools.partial(density_kernel, partners, mass, unit, shifts, box),
        out_shape=[f32(cell_count, 2, LANES), jax.ShapeDtypeStruct((1,), jnp.int32)],
        in_specs=[smem, smem, vmem],
        out_specs=[vmem, smem],
        scratch_shapes=extent + [fixed, pltpu.VMEM((chunks, 4, LANES), jnp.int32)] + columns
        + [pltpu.VMEM(square, jnp.float32), pltpu.VMEM((2,) + square, jnp.float32)],
        compiler_params=pltpu.CompilerParams(vmem_limit_bytes=VMEM),
        name="density",
    )(near, table_count, table)

    table_rho = pl.pallas_call(
        functools.partial(rho_halo_kernel, sizes),
        out_shape=f32(7, cell_count, 2, LANES),
        in_specs=[vmem],
        out_specs=vmem,
        scratch_shapes=sems(1, 6),
        compiler_params=effects(2),
        name="rho_halo",
    )(rho)

    out_q, out_v = pl.pallas_call(
        functools.partial(accel_kernel, partners, mass, unit, shifts, box),
        out_shape=[f32(cell_count, 8, LANES)] * 2,
        in_specs=[smem, smem, smem, smem, vmem, vmem, vmem],
        out_specs=[vmem, vmem],
        scratch_shapes=extent
        + [
            pltpu.VMEM((2, partners, 8, LANES), jnp.float32),
            pltpu.VMEM((2,) + square, jnp.float32),
            fixed,
            pltpu.VMEM((7 * cell_count, 2, LANES), jnp.float32),
            pltpu.VMEM((chunks, 4, LANES), jnp.int32),
            pltpu.VMEM((chunks, 1, LANES), jnp.float32),
        ]
        + columns
        + [pltpu.VMEM(square, jnp.float32)]
        + [pltpu.VMEM((2,) + square, jnp.float32)] * 4,
        compiler_params=pltpu.CompilerParams(vmem_limit_bytes=VMEM),
        name="accel",
    )(near, table_count, slot_before, fits, table, table_rho, recv)

    last = pl.pallas_call(
        functools.partial(last_exchange_kernel, sizes),
        out_shape=f32(*blocks),
        in_specs=[smem, vmem, vmem],
        out_specs=vmem,
        scratch_shapes=[pltpu.VMEM(blocks, jnp.float32)] + sems(1),
        compiler_params=effects(3),
        name="last_exchange",
    )(cells[1], out_q, out_v)
    new_pos, new_vel, new_rho = pl.pallas_call(
        unpack_kernel,
        out_shape=[f32(3, cell_count, particles)] * 2 + [f32(cell_count, particles)],
        in_specs=[smem, vmem],
        out_specs=[vmem] * 3,
        compiler_params=pltpu.CompilerParams(vmem_limit_bytes=VMEM),
        name="unpack",
    )(slot_after, last)
    return jnp.transpose(new_pos, (1, 0, 2)), jnp.transpose(new_vel, (1, 0, 2)), new_rho


def solution(mesh):
    in_specs = (
        P(("gx", "gy", "gz"), None, None),
        P(("gx", "gy", "gz"), None),
        P(("gx", "gy", "gz"), None, None),
        P(("gx", "gy", "gz")),
        P(("gx", "gy", "gz")),
        P(("gx", "gy", "gz"), None),
        P(("gx", "gy", "gz")),
    )
    out_specs = (
        P(("gx", "gy", "gz"), None, None),
        P(("gx", "gy", "gz"), None, None),
        P(("gx", "gy", "gz"), None),
    )
    return jax.shard_map(shards, mesh=mesh, in_specs=in_specs, out_specs=out_specs, check_vma=False)
```

```python
import functools
import math

import jax
import jax.numpy as jnp
from jax import lax
from jax.experimental import pallas as pl
from jax.experimental.pallas import tpu as pltpu
from jax.sharding import PartitionSpec as P

time_step = 0.1
LANES = 128
AXES = ("gx", "gy", "gz")
MESH = pl.DeviceIdType.MESH
VMEM = 24 * 2**20

def neighbour_steps():
    return [(axis, step) for axis in AXES for step in (-1, 1)]


def slots_of(plans, cell_count, devices):
    target = plans // cell_count
    ladder = jnp.arange(cell_count, dtype=jnp.int32)
    earlier = (target[:, :, None] == target[:, None, :]) & (ladder[None, :] < ladder[:, None])
    rank = jnp.sum(earlier.astype(jnp.int32), axis=2)
    slot = target * 2 + rank
    every = jnp.arange(devices * 2, dtype=jnp.int32)
    hit = slot[:, None, :] == every[None, :, None]
    return rank, jnp.sum(jnp.where(hit, ladder, 0), axis=2)


def near_table(neighbours, cell_count):
    sizes = {axis: lax.axis_size(axis) for axis in AXES}
    here = {axis: lax.axis_index(axis) for axis in AXES}
    owner = neighbours // cell_count
    block = jnp.zeros_like(owner)
    for number, (axis, step) in enumerate(neighbour_steps(), 1):
        there = dict(here)
        there[axis] = (here[axis] + step) % sizes[axis]
        device = (there["gx"] * sizes["gy"] + there["gy"]) * sizes["gz"] + there["gz"]
        block = jnp.where(owner == device, number, block)
    near = block * cell_count + neighbours % cell_count
    own = jnp.arange(cell_count, dtype=jnp.int32)[:, None]
    return jnp.concatenate([own, near], axis=1).reshape(-1)


def peer_offsets(sizes):
    count_x, count_y, count_z = sizes
    steps = [(x, y, z) for x in range(count_x) for y in range(count_y) for z in range(count_z)][1:]

    def hops(step):
        x, y, z = step
        chips = count_z // 2
        return min(x, count_x - x) + min(y, count_y - y) + min(z // 2, chips - z // 2)

    return sorted(steps, key=lambda step: -hops(step))


def shifted(here, step, sizes):
    return tuple(lax.rem(h + d, n) if d else h for h, d, n in zip(here, step, sizes))


def flat(place, sizes):
    return (place[0] * sizes[1] + place[1]) * sizes[2] + place[2]


def greet(peers):
    barrier = pltpu.get_barrier_semaphore()
    for peer in peers:
        pl.semaphore_signal(barrier, inc=1, device_id=peer, device_id_type=MESH)
    return barrier, len(peers)


def exchange(sizes, fill, pairs, send_sems, recv_sems):
    here = [lax.axis_index(axis) for axis in AXES]
    me = flat(here, sizes)
    peers = [shifted(here, step, sizes) for step in peer_offsets(sizes)]
    barrier, signals = greet(peers)
    fill()
    pl.semaphore_wait(barrier, signals)
    for number, (source, target, whole) in enumerate(pairs):
        for there in peers:
            pltpu.make_async_remote_copy(
                src_ref=source if whole else source.at[flat(there, sizes)],
                dst_ref=target.at[me],
                send_sem=send_sems.at[number],
                recv_sem=recv_sems.at[number],
                device_id=there,
                device_id_type=MESH,
            ).start()
    for source, target, whole in pairs:
        target[me] = source[...] if whole else source[me]
    for number, (source, target, whole) in enumerate(pairs):
        most = target.at[pl.ds(0, signals)]
        arrived = pltpu.make_async_remote_copy(
            src_ref=most, dst_ref=most, send_sem=send_sems.at[number],
            recv_sem=recv_sems.at[number], device_id=tuple(here), device_id_type=MESH,
        )
        arrived.wait_send()
        arrived.wait_recv()


def fill_blocks(cell_ref, q_ref, v_ref, send_ref):
    def one(d, carry):
        first, second = cell_ref[2 * d], cell_ref[2 * d + 1]
        for number, cell in enumerate((first, second)):
            rows = q_ref[cell]
            send_ref[d, 2 * number] = rows[0:4]
            send_ref[d, 2 * number + 1] = rows[4:8]
        low, high = v_ref[first], v_ref[second]
        send_ref[d, 4] = low[0:4]
        send_ref[d, 5, 0:2] = low[4:6]
        send_ref[d, 5, 2:4] = high[0:2]
        send_ref[d, 6] = high[2:6]
        return carry

    lax.fori_loop(0, send_ref.shape[0], one, 0)


def cell_rows(recv_ref, slot):
    block, odd = slot >> 1, slot & 1
    return [recv_ref[block, 2 * odd + half] for half in range(2)]


def velocity_rows(recv_ref, slot):
    block, odd = slot >> 1, (slot & 1) == 1
    first, middle, last = recv_ref[block, 4], recv_ref[block, 5], recv_ref[block, 6]
    even_rows = jnp.concatenate([first, middle[0:2]], axis=0)
    odd_rows = jnp.concatenate([middle[2:4], last], axis=0)
    rows = jnp.where(odd, odd_rows, even_rows)
    return rows[0:3], rows[3:6]


def first_exchange_kernel(sizes, cell_ref, meta_ref, pos_ref, h_ref, vel_ref, recv_ref, metas_ref,
                          q_ref, v_ref, send_ref, send_sems, recv_sems):
    def fill():
        for cell in range(pos_ref.shape[1]):
            for half in range(2):
                lanes = slice(half * LANES, (half + 1) * LANES)
                for component in range(3):
                    q_ref[cell, 4 * half + component] = pos_ref[component, cell, lanes]
                    v_ref[cell, 3 * half + component] = vel_ref[component, cell, lanes]
                q_ref[cell, 4 * half + 3] = h_ref[cell, lanes]
        fill_blocks(cell_ref, q_ref, v_ref, send_ref)

    pairs = ((send_ref, recv_ref, False), (meta_ref, metas_ref, True))
    exchange(sizes, fill, pairs, send_sems, recv_sems)


def last_exchange_kernel(sizes, cell_ref, q_ref, v_ref, recv_ref, send_ref, send_sems, recv_sems):
    def fill():
        fill_blocks(cell_ref, q_ref, v_ref, send_ref)

    exchange(sizes, fill, ((send_ref, recv_ref, False),), send_sems, recv_sems)


def halo(sizes, fill, pairs, send_sems, recv_sems):
    here = [lax.axis_index(axis) for axis in AXES]
    peers = []
    for axis, step in neighbour_steps():
        there = [0] * 3
        there[AXES.index(axis)] = (-step) % sizes[AXES.index(axis)]
        peers.append(shifted(here, there, sizes))
    barrier, signals = greet(peers)
    fill()
    pl.semaphore_wait(barrier, signals)
    copies = []
    for which, (source, target) in enumerate(pairs):
        for number, there in enumerate(peers):
            copies.append(
                pltpu.make_async_remote_copy(
                    src_ref=source, dst_ref=target.at[number + 1],
                    send_sem=send_sems.at[which, number], recv_sem=recv_sems.at[which, number],
                    device_id=there, device_id_type=MESH,
                )
            )
            copies[-1].start()
    for copy in copies:
        copy.wait()


def cell_halo_kernel(sizes, slot_ref, count_ref, recv_ref, table_ref, counts_ref, send_sems, recv_sems):
    def fill():
        counts_ref[0] = count_ref[...]
        for place in range(table_ref.shape[1]):
            low, high = cell_rows(recv_ref, slot_ref[place])
            table_ref[0, place, 0:4] = low
            table_ref[0, place, 4:8] = high

    pairs = ((count_ref, counts_ref), (table_ref.at[0], table_ref))
    halo(sizes, fill, pairs, send_sems, recv_sems)


def rho_halo_kernel(sizes, rho_ref, table_ref, send_sems, recv_sems):
    def fill():
        table_ref[0] = rho_ref[...]

    halo(sizes, fill, ((rho_ref, table_ref),), send_sems, recv_sems)


def unpack_kernel(slot_ref, recv_ref, pos_ref, vel_ref, rho_ref):
    for place in range(pos_ref.shape[1]):
        slot = slot_ref[place]
        rows = cell_rows(recv_ref, slot)
        velocity = velocity_rows(recv_ref, slot)
        for half in range(2):
            lanes = slice(half * LANES, (half + 1) * LANES)
            for component in range(3):
                pos_ref[component, place, lanes] = rows[half][component]
                vel_ref[component, place, lanes] = velocity[half][component]
            rho_ref[place, lanes] = rows[half][3]


def fixed_point(table_ref, fixed_ref, box):
    row = lax.broadcasted_iota(jnp.int32, (8, LANES), 0) & 3
    scale = jnp.full((8, LANES), 2.0**32 / box[2], jnp.float32)
    scale = jnp.where(row == 0, 2.0**32 / box[0], jnp.where(row == 1, 2.0**32 / box[1], scale))
    scale = jnp.where(row == 3, 1.0, scale)
    cells = table_ref.shape[1]

    def one(cell, carry):
        for block in range(table_ref.shape[0]):
            scaled = table_ref[block, cell] * scale
            scaled = jnp.where(scaled >= 2.0**31, scaled - 2.0**32, scaled)
            fixed_ref[block * cells + cell] = scaled.astype(jnp.int32)
        return carry

    lax.fori_loop(0, cells, one, 0)


def gather_live(cell, near_ref, count_ref, pairs, partners):
    fill = jnp.int32(0)
    for partner in range(partners):
        b = near_ref[cell * partners + partner]
        live = count_ref[b]
        shift = fill & (LANES - 1)
        chunk = fill >> 7
        for table_ref, list_ref in pairs:
            rows = list_ref.shape[1]
            kept = lax.broadcasted_iota(jnp.int32, (rows, LANES), 1) < shift
            rolled = pltpu.roll(table_ref[b], shift, 1)
            first, second = rolled[0:rows], rolled[rows : 2 * rows]
            list_ref[chunk] = jnp.where(kept, list_ref[chunk], first)
            list_ref[chunk + 1] = jnp.where(kept, first, second)
            list_ref[chunk + 2] = second
        fill = fill + live
    return fill


def store_column(ref, halves):
    for half, part in enumerate(halves):
        ref[half * LANES : (half + 1) * LANES, :] = jnp.broadcast_to(part, (LANES, LANES)).T


def halves_of(ref, cell, row):
    step = ref.shape[1] // 2
    return [ref[cell, row + half * step : row + half * step + 1, :] for half in range(2)]


def row_sums(acc):
    ones = jnp.ones((8, LANES), jnp.float32)
    sums = lax.dot_general(
        ones, acc, (((1,), (1,)), ((), ())),
        precision=lax.Precision.HIGHEST, preferred_element_type=jnp.float32,
    )
    return [sums[0:1, 0:LANES], sums[0:1, LANES : 2 * LANES]]


def spread(list_ref, chunk, row):
    return jnp.broadcast_to(list_ref[chunk, row : row + 1, :], (8, LANES))


def offsets(i_refs, rows, others, shifts):
    parts = []
    for ref, other, shift in zip(i_refs, others, shifts):
        diff = ref[rows, :] - other
        if shift:
            diff = diff >> shift
        parts.append(diff.astype(jnp.float32))
    return parts


def by_row(values):
    row = lax.broadcasted_iota(jnp.int32, (8, LANES), 0) & 3
    out = jnp.full((8, LANES), values[3], jnp.float32)
    for number in range(3):
        out = jnp.where(row == number, jnp.float32(values[number]), out)
    return out


def bounds(table_ref, low_ref, high_ref):
    blocks, cells = table_ref.shape[0], table_ref.shape[1]
    together = 4

    def some(step, carry):
        which = [(block, step * together + n) for n in range(together) for block in range(blocks)]
        lows = [jnp.min(table_ref[block, cell], axis=1, keepdims=True) for block, cell in which]
        highs = [jnp.max(table_ref[block, cell], axis=1, keepdims=True) for block, cell in which]
        for (block, cell), low, high in zip(which, lows, highs):
            low = jnp.broadcast_to(low, (8, LANES))
            high = jnp.broadcast_to(high, (8, LANES))
            low_ref[block * cells + cell] = jnp.minimum(low, pltpu.roll(low, 4, 0))
            high_ref[block * cells + cell] = jnp.maximum(high, pltpu.roll(high, 4, 0))
        return carry

    lax.fori_loop(0, cells // together, some, 0)


def middle(low, high):
    return jnp.floor(low + high + 0.5) * 0.5


def image(low_a, high_a, low_b, high_b, lengths):
    return jnp.floor((low_a - high_b) / lengths + 0.5) * lengths


def sum_of_xyz(rows):
    return pltpu.roll(rows, 1, 0) + pltpu.roll(rows, 2, 0) + pltpu.roll(rows, 3, 0)


def one_image(cells, partners, box, near_ref, low_ref, high_ref):
    lengths = by_row(box + (1.0,))
    half = lengths * (0.5 * (1.0 - 2.0**-16))
    coordinate = (lax.broadcasted_iota(jnp.int32, (8, LANES), 0) & 3) < 3
    limit = 256.0 / math.log2(math.e)

    def one(cell, good):
        low_a, high_a = low_ref[cell], high_ref[cell]
        origin = middle(low_a, high_a)
        for partner in range(partners):
            b = near_ref[cell * partners + partner]
            low_b, high_b = low_ref[b], high_ref[b]
            shift = image(low_a, high_a, low_b, high_b, lengths)
            fits = (high_a - low_b - shift < half) & (low_a - high_b - shift > -half)
            moved = shift - origin
            reach = jnp.maximum(jnp.abs(low_b + moved), jnp.abs(high_b + moved))
            small = sum_of_xyz(reach * reach) <= limit * low_a * low_a
            fine = jnp.where(coordinate, jnp.where(fits, 1.0, 0.0), jnp.where(small, 1.0, 0.0))
            good = jnp.minimum(good, fine)
        return good

    good = lax.fori_loop(0, cells, one, jnp.ones((8, LANES), jnp.float32), unroll=4)
    return jnp.min(good) > 0.5


def three_parts(value):
    first = value.astype(jnp.bfloat16).astype(jnp.float32)
    value = value - first
    second = value.astype(jnp.bfloat16).astype(jnp.float32)
    return first, second, value - second


def joined(upper, lower, half):
    top = lax.broadcasted_iota(jnp.int32, (8, LANES), 0) < 4
    if half == 0:
        return jnp.where(top, upper, pltpu.roll(lower, 4, 0))
    return jnp.where(top, pltpu.roll(upper, 4, 0), lower)


def own_factors(rows, origin, own_ref):
    row = lax.broadcasted_iota(jnp.int32, (8, LANES), 0)
    centred = rows - origin
    c = -math.log2(math.e) / (rows * rows)
    c = jnp.where(row < 4, jnp.broadcast_to(c[3:4], (8, LANES)), jnp.broadcast_to(c[7:8], (8, LANES)))
    p1, p2, p3 = three_parts(jnp.where((row & 3) == 3, c, -2.0 * c * centred))
    squares = three_parts(c * sum_of_xyz(centred * centred))
    for half in range(2):
        last = jnp.where(row == 3, 1.0, 0.0)
        for number, part in enumerate(squares):
            moved = pltpu.roll(part, (number + 5 - 4 * half) % 8, 0)
            last = jnp.where(row == number, moved, last)
        groups = [joined(p1, p1, half), joined(p1, p2, half), joined(p2, p3, half), last]
        block = jnp.concatenate(groups, axis=0).T
        own_ref[half * LANES : (half + 1) * LANES, :] = block.astype(jnp.bfloat16)
    return centred


def near_factors(moved, live, near_ref, partner):
    row = lax.broadcasted_iota(jnp.int32, (8, LANES), 0)
    lane = lax.broadcasted_iota(jnp.int32, (8, LANES), 1)
    q1, q2, q3 = three_parts(jnp.where((row & 3) == 3, sum_of_xyz(moved * moved), moved))
    for half in range(2):
        alive = lane + half * LANES < live
        last = jnp.where(row < 3, 1.0, jnp.where((row > 3) | alive, 0.0, -1e30))
        groups = [joined(q1, q2, half), joined(q3, q1, half), joined(q2, q1, half), last]
        block = jnp.concatenate(groups, axis=0)
        near_ref[partner, :, half * LANES : (half + 1) * LANES] = block.astype(jnp.bfloat16)


def exponents(own_ref, near_ref, partner, rows):
    return jnp.dot(own_ref[rows, :], near_ref[partner], preferred_element_type=jnp.float32)


def lane_sums(acc):
    halves = []
    for half in range(2):
        part = acc[half * LANES : (half + 1) * LANES, :].T
        eight = part[0:8]
        for row in range(8, LANES, 8):
            eight = eight + part[row : row + 8]
        halves.append(jnp.sum(eight, axis=0, keepdims=True))
    return halves


def fast_density(cells, partners, mass, box, near_ref, count_ref, table_ref, low_ref, high_ref, rho_ref,
                 own_ref, factor_ref, acc_ref):
    lengths = by_row(box + (1.0,))
    step = 64

    def one_cell(cell, own_ref, factor_ref, acc_ref):
        low_a, high_a = low_ref[cell], high_ref[cell]
        origin = middle(low_a, high_a)
        own_factors(table_ref[0, cell], origin, own_ref)
        for partner in range(partners):
            b = near_ref[cell * partners + partner]
            shift = image(low_a, high_a, low_ref[b], high_ref[b], lengths)
            moved = table_ref[b >> 5, b & 31] + (shift - origin)
            near_factors(moved, count_ref[b], factor_ref, partner)
        for block in range(2 * LANES // step):
            rows = slice(block * step, (block + 1) * step)
            acc = None
            for partner in range(partners):
                w = jnp.exp2(exponents(own_ref, factor_ref, partner, rows))
                both = w[:, 0:LANES] + w[:, LANES : 2 * LANES]
                acc = both if acc is None else acc + both
            acc_ref[rows, :] = acc
        h = halves_of(table_ref.at[0], cell, 3)
        for half, (part, total) in enumerate(zip(h, lane_sums(acc_ref[...]))):
            rho_ref[cell, half : half + 1] = mass * (1.0 + total) / (part * part * part)

    def four_cells(group, carry):
        for number in range(4):
            one_cell(4 * group + number, own_ref.at[number], factor_ref.at[number], acc_ref.at[number])
        return carry

    lax.fori_loop(0, cells // 4, four_cells, 0)


def fast_accel(cells, partners, mass, box, near_ref, count_ref, slot_ref, table_ref, low_ref, high_ref,
               inverse_ref, rho_ref, recv_ref, q_ref, v_ref,
               own_ref, factor_ref, moved_ref, ai_ref, acc_refs):
    lengths = by_row(box + (1.0,))
    step = 32

    def one_cell(cell, own_ref, factor_ref, moved_ref, ai_ref, acc_refs):
        low_a, high_a = low_ref[cell], high_ref[cell]
        origin = middle(low_a, high_a)
        centred = own_factors(table_ref[0, cell], origin, own_ref)
        store_column(ai_ref, halves_of(inverse_ref, cell, 0))
        for partner in range(partners):
            b = near_ref[cell * partners + partner]
            shift = image(low_a, high_a, low_ref[b], high_ref[b], lengths)
            moved = table_ref[b >> 5, b & 31] + (shift - origin)
            near_factors(moved, count_ref[b], factor_ref, partner)
            moved_ref[partner] = moved
            for half in range(2):
                moved_ref[partner, 4 * half + 3 : 4 * half + 4] = inverse_ref[b, half : half + 1]
        for block in range(2 * LANES // step):
            rows = slice(block * step, (block + 1) * step)
            own_inverse = ai_ref[rows, :]
            accs = [None] * 4
            for partner in range(partners):
                w = jnp.exp2(exponents(own_ref, factor_ref, partner, rows))
                for half in range(2):
                    near = [
                        jnp.broadcast_to(
                            moved_ref[partner, 4 * half + row : 4 * half + row + 1, :], (step, LANES)
                        )
                        for row in range(4)
                    ]
                    pair = w[:, half * LANES : (half + 1) * LANES] * (own_inverse + near[3])
                    terms = [pair * near[0], pair * near[1], pair * near[2], pair]
                    accs = [t if a is None else a + t for a, t in zip(accs, terms)]
            for acc_ref, acc in zip(acc_refs, accs):
                acc_ref[rows, :] = acc
        h = halves_of(table_ref.at[0], cell, 3)
        scale = [(time_step * 2.0 * mass) / (part * part * part * part * part) for part in h]
        velocity = velocity_rows(recv_ref, slot_ref[cell])
        whole = lane_sums(acc_refs[3][...])
        for component in range(3):
            sums = lane_sums(acc_refs[component][...])
            for half in range(2):
                row = slice(4 * half + component, 4 * half + component + 1)
                force = centred[row] * whole[half] - sums[half]
                kicked = velocity[half][component : component + 1] + force * scale[half]
                v_ref[cell, 3 * half + component : 3 * half + component + 1] = kicked
                q_ref[cell, row] = table_ref[0, cell, row] + time_step * kicked
        for half in range(2):
            row = slice(4 * half + 3, 4 * half + 4)
            q_ref[cell, row] = rho_ref[0, cell, half : half + 1]

    def two_cells(pair, carry):
        for number in range(2):
            one_cell(2 * pair + number, own_ref.at[number], factor_ref.at[number], moved_ref.at[number], ai_ref.at[number], [ref.at[number] for ref in acc_refs])
        return carry

    lax.fori_loop(0, cells // 2, two_cells, 0)


def density_kernel(partners, mass, unit, shifts, box, near_ref, count_ref, table_ref, rho_ref, fits_ref,
                   low_ref, high_ref, own_ref, factor_ref,
                   fixed_ref, list_ref, xi_ref, yi_ref, zi_ref, ci_ref, acc_ref):
    cells = table_ref.shape[1]
    bounds(table_ref, low_ref, high_ref)
    fits = one_image(cells, partners, box, near_ref, low_ref, high_ref)

    fits_ref[0] = jnp.where(fits, 1, 0)

    @pl.when(fits)
    def _():
        fast_density(cells, partners, mass, box, near_ref, count_ref, table_ref, low_ref, high_ref,
                     rho_ref, own_ref, factor_ref, acc_ref)

    @pl.when(jnp.logical_not(fits))
    def _():
        any_density(partners, mass, unit, shifts, box, near_ref, count_ref, table_ref, rho_ref,
                    fixed_ref, list_ref, xi_ref, yi_ref, zi_ref, ci_ref, acc_ref.at[0])


def any_density(partners, mass, unit, shifts, box, near_ref, count_ref, table_ref, rho_ref,
                fixed_ref, list_ref, xi_ref, yi_ref, zi_ref, ci_ref, acc_ref):
    cells, particles = table_ref.shape[1], 2 * LANES
    blocks = particles // 8
    i_refs = (xi_ref, yi_ref, zi_ref)
    lane = lax.broadcasted_iota(jnp.int32, (8, LANES), 1)
    factor = -math.log2(math.e) * unit * unit
    fixed_point(table_ref, fixed_ref, box)

    def one_cell(cell, carry):
        total = gather_live(cell, near_ref, count_ref, ((fixed_ref, list_ref),), partners)
        for component in range(3):
            store_column(i_refs[component], halves_of(fixed_ref, cell, component))
        h = halves_of(table_ref.at[0], cell, 3)
        store_column(ci_ref, [factor / (part * part) for part in h])
        last = (total - 1) >> 7

        def weights(chunk, others, block):
            rows = pl.ds(block * 8, 8)
            dx, dy, dz = offsets(i_refs, rows, others, shifts)
            return rows, jnp.exp2((dx * dx + dy * dy + dz * dz) * ci_ref[rows, :])

        others = [spread(list_ref, last, row) for row in range(3)]
        alive = lane < total - last * LANES
        for block in range(blocks):
            rows, w = weights(last, others, block)
            acc_ref[rows, :] = jnp.where(alive, w, 0.0)

        def one_chunk(chunk, inner):
            near = [spread(list_ref, chunk, row) for row in range(3)]
            for block in range(blocks):
                rows, w = weights(chunk, near, block)
                acc_ref[rows, :] += w
            return inner

        lax.fori_loop(0, last, one_chunk, 0)
        for half, (part, total_half) in enumerate(zip(h, row_sums(acc_ref[...]))):
            rho_ref[cell, half : half + 1] = mass * (1.0 + total_half) / (part * part * part)
        return carry

    lax.fori_loop(0, cells, one_cell, 0)


def accel_kernel(partners, mass, unit, shifts, box, near_ref, count_ref, slot_ref, fits_ref, table_ref, rho_ref,
                 recv_ref, q_ref, v_ref,
                 low_ref, high_ref, own_ref, factor_ref, moved_ref, sum_ref,
                 fixed_ref, inverse_ref, list_ref, inverse_list_ref, xi_ref, yi_ref, zi_ref, ci_ref, ai_ref,
                 ax_ref, ay_ref, az_ref):
    cells = table_ref.shape[1]
    bounds(table_ref, low_ref, high_ref)
    fits = fits_ref[0] > 0

    def invert(cell, carry):
        for block in range(rho_ref.shape[0]):
            inverse_ref[block * cells + cell] = 1.0 / rho_ref[block, cell]
        return carry

    lax.fori_loop(0, cells, invert, 0)

    @pl.when(fits)
    def _():
        fast_accel(cells, partners, mass, box, near_ref, count_ref, slot_ref, table_ref, low_ref, high_ref,
                   inverse_ref, rho_ref, recv_ref, q_ref, v_ref,
                   own_ref, factor_ref, moved_ref, ai_ref, (ax_ref, ay_ref, az_ref, sum_ref))

    @pl.when(jnp.logical_not(fits))
    def _():
        any_accel(partners, mass, unit, shifts, box, near_ref, count_ref, slot_ref, table_ref, rho_ref,
                  recv_ref, q_ref, v_ref, fixed_ref, inverse_ref, list_ref, inverse_list_ref,
                  xi_ref, yi_ref, zi_ref, ci_ref, ai_ref.at[0], ax_ref.at[0], ay_ref.at[0], az_ref.at[0])


def any_accel(partners, mass, unit, shifts, box, near_ref, count_ref, slot_ref, table_ref, rho_ref,
                 recv_ref, q_ref, v_ref,
                 fixed_ref, inverse_ref, list_ref, inverse_list_ref, xi_ref, yi_ref, zi_ref, ci_ref, ai_ref,
                 ax_ref, ay_ref, az_ref):
    cells, particles = table_ref.shape[1], 2 * LANES
    blocks = particles // 8
    i_refs = (xi_ref, yi_ref, zi_ref)
    acc_refs = (ax_ref, ay_ref, az_ref)
    lane = lax.broadcasted_iota(jnp.int32, (8, LANES), 1)
    factor = -math.log2(math.e) * unit * unit
    fixed_point(table_ref, fixed_ref, box)

    def one_cell(cell, carry):
        total = gather_live(
            cell, near_ref, count_ref,
            ((fixed_ref, list_ref), (inverse_ref, inverse_list_ref)), partners,
        )
        for component in range(3):
            store_column(i_refs[component], halves_of(fixed_ref, cell, component))
        h = halves_of(table_ref.at[0], cell, 3)
        store_column(ci_ref, [factor / (part * part) for part in h])
        store_column(ai_ref, halves_of(inverse_ref, cell, 0))
        last = (total - 1) >> 7

        def terms(others, other_inverse, block):
            rows = pl.ds(block * 8, 8)
            parts = offsets(i_refs, rows, others, shifts)
            dx, dy, dz = parts
            w = jnp.exp2((dx * dx + dy * dy + dz * dz) * ci_ref[rows, :])
            return rows, parts, w * (ai_ref[rows, :] + other_inverse)

        others = [spread(list_ref, last, row) for row in range(3)]
        other_inverse = spread(inverse_list_ref, last, 0)
        alive = lane < total - last * LANES
        for block in range(blocks):
            rows, parts, pair = terms(others, other_inverse, block)
            pair = jnp.where(alive, pair, 0.0)
            for acc_ref, part in zip(acc_refs, parts):
                acc_ref[rows, :] = pair * part

        def one_chunk(chunk, inner):
            near = [spread(list_ref, chunk, row) for row in range(3)]
            near_inverse = spread(inverse_list_ref, chunk, 0)
            for block in range(blocks):
                rows, parts, pair = terms(near, near_inverse, block)
                for acc_ref, part in zip(acc_refs, parts):
                    acc_ref[rows, :] += pair * part
            return inner

        lax.fori_loop(0, last, one_chunk, 0)
        scale = [(time_step * 2.0 * mass * unit) / (part * part * part * part * part) for part in h]
        velocity = velocity_rows(recv_ref, slot_ref[cell])
        for component, acc_ref in enumerate(acc_refs):
            sums = row_sums(acc_ref[...])
            for half in range(2):
                kicked = velocity[half][component : component + 1] + sums[half] * scale[half]
                v_ref[cell, 3 * half + component : 3 * half + component + 1] = kicked
                row = slice(4 * half + component, 4 * half + component + 1)
                q_ref[cell, row] = table_ref[0, cell, row] + time_step * kicked
        for half in range(2):
            row = slice(4 * half + 3, 4 * half + 4)
            q_ref[cell, row] = rho_ref[0, cell, half : half + 1]
        return carry

    lax.fori_loop(0, cells, one_cell, 0)


def shards(positions, smoothing, velocity, counts, plan_before, neighbours, plan_after):
    cell_count = positions.shape[0]
    particles = positions.shape[-1]
    partners = neighbours.shape[1] + 1
    sizes = tuple(lax.axis_size(axis) for axis in AXES)
    devices = sizes[0] * sizes[1] * sizes[2]
    box = (float(cell_count // 4 * sizes[0]), float(2 * sizes[1]), float(2 * sizes[2]))
    longest = max(box)
    shifts = tuple(int(round(math.log2(longest / length))) for length in box)
    unit = longest / 2.0**32
    mass = 1.0 / (partners * particles)

    smem = pl.BlockSpec(memory_space=pltpu.SMEM)
    vmem = pl.BlockSpec(memory_space=pltpu.VMEM)
    f32 = lambda *shape: jax.ShapeDtypeStruct(shape, jnp.float32)
    effects = lambda number: pltpu.CompilerParams(has_side_effects=True, collective_id=number, vmem_limit_bytes=VMEM)
    sems = lambda *count: [pltpu.SemaphoreType.DMA(count)] * 2
    blocks = (devices, 7, 4, LANES)
    cells8 = pltpu.VMEM((cell_count, 8, LANES), jnp.float32)

    ranks, cells = slots_of(jnp.stack([plan_before, plan_after]), cell_count, devices)
    meta = jnp.concatenate([plan_before, plan_after, ranks.reshape(-1), counts, jnp.zeros((96,), jnp.int32)])[None, :]
    recv, metas = pl.pallas_call(
        functools.partial(first_exchange_kernel, sizes),
        out_shape=[f32(*blocks), jax.ShapeDtypeStruct((devices, 1, 2 * LANES), jnp.int32)],
        in_specs=[smem, vmem, vmem, vmem, vmem],
        out_specs=[vmem] * 2,
        scratch_shapes=[cells8, cells8, pltpu.VMEM(blocks, jnp.float32)] + sems(2),
        compiler_params=effects(0),
        name="first_exchange",
    )(cells[0], meta, jnp.transpose(positions, (1, 0, 2)), smoothing, jnp.transpose(velocity, (1, 0, 2)))

    here = [lax.axis_index(axis) for axis in AXES]
    place = flat(here, sizes) * cell_count + jnp.arange(cell_count, dtype=jnp.int32)
    metas = metas[:, 0, :]
    fields = [metas[:, n * cell_count : (n + 1) * cell_count] for n in range(5)]
    placed_before, placed_after, rank_before, rank_after, all_counts = fields
    source = 2 * jnp.arange(devices, dtype=jnp.int32)[:, None]

    def pick(placed, values):
        hit = placed[None] == place[:, None, None]
        return jnp.sum(jnp.where(hit, values[None], 0), axis=(1, 2))

    slot_count = pick(placed_before, rank_before + source + all_counts * (2 * devices))
    slot_before, own_count = slot_count % (2 * devices), slot_count // (2 * devices)
    slot_after = pick(placed_after, rank_after + source)
    near = near_table(neighbours, cell_count)

    table, table_count = pl.pallas_call(
        functools.partial(cell_halo_kernel, sizes),
        out_shape=[f32(7, cell_count, 8, LANES), jax.ShapeDtypeStruct((7, 1, LANES), jnp.int32)],
        in_specs=[smem, vmem, vmem],
        out_specs=[vmem, vmem],
        scratch_shapes=sems(2, 6),
        compiler_params=effects(1),
        name="cell_halo",
    )(slot_before, jnp.pad(own_count, (0, LANES - cell_count))[None, :], recv)
    table_count = table_count[:, 0, :cell_count].reshape(-1)

    chunks = partners * particles // LANES + 1
    square = (particles, LANES)
    columns = [pltpu.VMEM(square, jnp.int32)] * 3
    extent = [pltpu.VMEM((7 * cell_count, 8, LANES), jnp.float32)] * 2 + [
        pltpu.VMEM((4, particles, 32), jnp.bfloat16),
        pltpu.VMEM((4, partners, 32, particles), jnp.bfloat16),
    ]
    fixed = pltpu.VMEM((7 * cell_count, 8, LANES), jnp.int32)
    rho, fits = pl.pallas_call(
        functools.partial(density_kernel, partners, mass, unit, shifts, box),
        out_shape=[f32(cell_count, 2, LANES), jax.ShapeDtypeStruct((1,), jnp.int32)],
        in_specs=[smem, smem, vmem],
        out_specs=[vmem, smem],
        scratch_shapes=extent + [fixed, pltpu.VMEM((chunks, 4, LANES), jnp.int32)] + columns
        + [pltpu.VMEM(square, jnp.float32), pltpu.VMEM((4,) + square, jnp.float32)],
        compiler_params=pltpu.CompilerParams(vmem_limit_bytes=VMEM),
        name="density",
    )(near, table_count, table)

    table_rho = pl.pallas_call(
        functools.partial(rho_halo_kernel, sizes),
        out_shape=f32(7, cell_count, 2, LANES),
        in_specs=[vmem],
        out_specs=vmem,
        scratch_shapes=sems(1, 6),
        compiler_params=effects(2),
        name="rho_halo",
    )(rho)

    out_q, out_v = pl.pallas_call(
        functools.partial(accel_kernel, partners, mass, unit, shifts, box),
        out_shape=[f32(cell_count, 8, LANES)] * 2,
        in_specs=[smem, smem, smem, smem, vmem, vmem, vmem],
        out_specs=[vmem, vmem],
        scratch_shapes=extent
        + [
            pltpu.VMEM((2, partners, 8, LANES), jnp.float32),
            pltpu.VMEM((2,) + square, jnp.float32),
            fixed,
            pltpu.VMEM((7 * cell_count, 2, LANES), jnp.float32),
            pltpu.VMEM((chunks, 4, LANES), jnp.int32),
            pltpu.VMEM((chunks, 1, LANES), jnp.float32),
        ]
        + columns
        + [pltpu.VMEM(square, jnp.float32)]
        + [pltpu.VMEM((2,) + square, jnp.float32)] * 4,
        compiler_params=pltpu.CompilerParams(vmem_limit_bytes=VMEM),
        name="accel",
    )(near, table_count, slot_before, fits, table, table_rho, recv)

    last = pl.pallas_call(
        functools.partial(last_exchange_kernel, sizes),
        out_shape=f32(*blocks),
        in_specs=[smem, vmem, vmem],
        out_specs=vmem,
        scratch_shapes=[pltpu.VMEM(blocks, jnp.float32)] + sems(1),
        compiler_params=effects(3),
        name="last_exchange",
    )(cells[1], out_q, out_v)
    new_pos, new_vel, new_rho = pl.pallas_call(
        unpack_kernel,
        out_shape=[f32(3, cell_count, particles)] * 2 + [f32(cell_count, particles)],
        in_specs=[smem, vmem],
        out_specs=[vmem] * 3,
        compiler_params=pltpu.CompilerParams(vmem_limit_bytes=VMEM),
        name="unpack",
    )(slot_after, last)
    return jnp.transpose(new_pos, (1, 0, 2)), jnp.transpose(new_vel, (1, 0, 2)), new_rho


def solution(mesh):
    in_specs = (
        P(("gx", "gy", "gz"), None, None),
        P(("gx", "gy", "gz"), None),
        P(("gx", "gy", "gz"), None, None),
        P(("gx", "gy", "gz")),
        P(("gx", "gy", "gz")),
        P(("gx", "gy", "gz"), None),
        P(("gx", "gy", "gz")),
    )
    out_specs = (
        P(("gx", "gy", "gz"), None, None),
        P(("gx", "gy", "gz"), None, None),
        P(("gx", "gy", "gz"), None),
    )
    return jax.shard_map(shards, mesh=mesh, in_specs=in_specs, out_specs=out_specs, check_vma=False)
```
